128 devices in a mesh: tp: 1, cp: 128 (over z, y, x, core).
Axes of the slice: x: 4, y: 4, z: 4, core: 2. Of those that a mesh axis runs over, the one named last changes fastest.
Arguments:
- query: bfloat16 [6, 1024, 16, 128], P(None, 'cp', 'tp')
- out_act: bfloat16 [6, 1024, 16, 128], P(None, 'cp', 'tp')
- out_grad: bfloat16 [6, 1024, 16, 128], P(None, 'cp', 'tp')
- row_lse: float32 [6, 1024, 16], P(None, 'cp', 'tp')
- key_act: bfloat16 [38912, 1, 128], P('cp', 'tp')
- value_act: bfloat16 [38912, 1, 128], P('cp', 'tp')
- doc_ids: int32 [38912], replicated
Outputs:
- output 1: bfloat16 [6, 1024, 16, 128], P(None, 'cp', 'tp')
- output 2: float32 [38912, 1, 128], P('cp', 'tp')
- output 3: float32 [38912, 1, 128], P('cp', 'tp')
All inputs are finite; a program needn't handle non-finite values.
Results may differ from the reference program's by a relative error of at most 0.001.
Values are sent between devices in bfloat16 or wider.
A program may use at most 1 GiB of HBM per device.

```python
import jax
import jax.numpy as jnp
from jax import lax

SLICES = 6
SUB_LEN = 1024
PRE_LEN = 32768
Q_HEADS = 16
KV_HEADS = 1
HEAD_DIM = 128
SPLITS = 128

PREFIX = PRE_LEN + SLICES * SUB_LEN
GROUP_SIZE = Q_HEADS // KV_HEADS
BLOCK_LEN = SUB_LEN // SPLITS
SCORE_SCALE = HEAD_DIM ** -0.5
GRAD_SCALE = (PREFIX // 8) ** 0.5
DOC_MEAN = PREFIX // 8


def masked_scores(q_blk, key_act, doc_ids, first_pos):
    block_len = q_blk.shape[0]
    scores = jnp.einsum('qhgd,khd->qhgk', q_blk.astype(jnp.float32), key_act.astype(jnp.float32)) * SCORE_SCALE
    q_pos = first_pos + jnp.arange(block_len)
    k_pos = jnp.arange(key_act.shape[0])
    q_doc = lax.dynamic_slice(doc_ids, (first_pos,), (block_len,))
    allowed = (k_pos[None, :] <= q_pos[:, None]) & (doc_ids[None, :] == q_doc[:, None])
    return scores, allowed[:, None, None, :]


def forward_lse(query, key_act, doc_ids):
    n_blocks = SLICES * SPLITS
    q_blocks = query.reshape(n_blocks, BLOCK_LEN, KV_HEADS, GROUP_SIZE, HEAD_DIM)
    firsts = PRE_LEN + jnp.arange(n_blocks) * BLOCK_LEN

    def block_lse(xs_blk):
        q_blk, first_pos = xs_blk
        scores, allowed = masked_scores(q_blk, key_act, doc_ids, first_pos)
        return jax.nn.logsumexp(jnp.where(allowed, scores, -1e30), axis=-1)

    return lax.map(block_lse, (q_blocks, firsts)).reshape(SLICES, SUB_LEN, Q_HEADS)


def setup_inputs(seed: int = 0, part: int = 0) -> dict:
    root_key = jax.random.key(seed)
    part_keys = jax.random.split(jax.random.fold_in(root_key, part), 5)
    doc_key = jax.random.key(seed + 17)
    starts = (jax.random.randint(doc_key, (PREFIX,), 0, DOC_MEAN) == 0) & (jnp.arange(PREFIX) > 0)
    doc_ids = jnp.cumsum(starts.astype(jnp.int32)).astype(jnp.int32)
    q_shape = (SLICES, SUB_LEN, Q_HEADS, HEAD_DIM)
    query = jax.random.normal(part_keys[0], q_shape, jnp.float32).astype(jnp.bfloat16)
    key_act = jax.random.normal(part_keys[1], (PREFIX, KV_HEADS, HEAD_DIM), jnp.float32).astype(jnp.bfloat16)
    value_act = jax.random.normal(part_keys[2], (PREFIX, KV_HEADS, HEAD_DIM), jnp.float32).astype(jnp.bfloat16)
    grad_dir = jax.random.normal(part_keys[3], q_shape, jnp.float32)
    out_noise = jax.random.normal(part_keys[4], q_shape, jnp.float32)
    out_grad = (GRAD_SCALE * grad_dir).astype(jnp.bfloat16)
    out_act = (0.125 * (grad_dir + out_noise)).astype(jnp.bfloat16)
    row_lse = forward_lse(query, key_act, doc_ids)
    return {'query': query, 'out_act': out_act, 'out_grad': out_grad, 'row_lse': row_lse, 'key_act': key_act, 'value_act': value_act, 'doc_ids': doc_ids}


def reference(query, out_act, out_grad, row_lse, key_act, value_act, doc_ids):
    n_blocks = SLICES * SPLITS
    blk_shape = (n_blocks, BLOCK_LEN, KV_HEADS, GROUP_SIZE, HEAD_DIM)
    key_f32 = key_act.astype(jnp.float32)
    value_f32 = value_act.astype(jnp.float32)
    xs_all = (query.reshape(blk_shape), out_act.reshape(blk_shape), out_grad.reshape(blk_shape), row_lse.reshape(n_blocks, BLOCK_LEN, KV_HEADS, GROUP_SIZE), PRE_LEN + jnp.arange(n_blocks) * BLOCK_LEN)

    def block_step(carry_in, xs_blk):
        dk_acc, dv_acc = carry_in
        q_blk, o_blk, do_blk, lse_blk, first_pos = xs_blk
        scores, allowed = masked_scores(q_blk, key_act, doc_ids, first_pos)
        p_full = jnp.where(allowed, jnp.exp(scores - lse_blk[..., None]), 0.0)
        p_half = p_full.astype(jnp.bfloat16).astype(jnp.float32)
        grad_f32 = do_blk.astype(jnp.float32)
        row_delta = jnp.sum(grad_f32 * o_blk.astype(jnp.float32), axis=-1)
        dv_acc = dv_acc + jnp.einsum('qhgk,qhgd->khd', p_half, grad_f32)
        d_prob = jnp.einsum('qhgd,khd->qhgk', grad_f32, value_f32)
        d_score = (p_full * (d_prob - row_delta[..., None])).astype(jnp.bfloat16).astype(jnp.float32)
        dq_blk = (jnp.einsum('qhgk,khd->qhgd', d_score, key_f32) * SCORE_SCALE).astype(jnp.bfloat16)
        dk_acc = dk_acc + jnp.einsum('qhgk,qhgd->khd', d_score, q_blk.astype(jnp.float32)) * SCORE_SCALE
        return (dk_acc, dv_acc), dq_blk

    zero_acc = jnp.zeros((PREFIX, KV_HEADS, HEAD_DIM), jnp.float32)
    (d_key, d_value), dq_blocks = lax.scan(block_step, (zero_acc, zero_acc), xs_all)
    return dq_blocks.reshape(SLICES, SUB_LEN, Q_HEADS, HEAD_DIM), d_key, d_value
```

```python
import functools

import jax
import jax.numpy as jnp
from jax import lax
from jax.experimental import pallas as pl
from jax.experimental.pallas import tpu as pltpu
from jax.sharding import PartitionSpec as P

MESH = pl.DeviceIdType.MESH
TK = 256
LOG2E = 1.4426950408889634
F32, BF16 = jnp.float32, jnp.bfloat16


def place():
    me = lax.axis_index('cp')
    return me // 32, lax.rem(me // 8, 4), lax.rem(me // 2, 4), lax.rem(me, 2)


def at(z, y, x, c):
    return ((z * 4 + y) * 4 + x) * 2 + c


def up(v):
    return lax.rem(v + 1, 4)


def down(v):
    return lax.rem(v + 3, 4)


def far(v):
    return lax.rem(v + 2, 4)


class Wire:
    def __init__(self, ssem, rsem):
        self.ssem, self.rsem, self.n, self.sent = ssem, rsem, 0, []

    def send(self, src, dst, dev):
        cp = pltpu.make_async_remote_copy(
            src_ref=src, dst_ref=dst, send_sem=self.ssem.at[self.n], recv_sem=self.rsem.at[self.n],
            device_id={'cp': dev}, device_id_type=MESH)
        self.n += 1
        cp.start()
        self.sent.append(cp)
        return cp

    def finish(self):
        for cp in self.sent:
            cp.wait_send()


def greet(partners):
    barrier = pltpu.get_barrier_semaphore()
    for dev in partners:
        pl.semaphore_signal(barrier, inc=1, device_id={'cp': dev}, device_id_type=MESH)
    pl.semaphore_wait(barrier, len(partners))


def gather_body(q, do, st, k, v, qg, dg, sg, kg, vg, ssem, rsem):
    z, y, x, c = place()
    xu, xd, sib = at(z, y, up(x), c), at(z, y, down(x), c), at(z, y, x, 1 - c)
    yu, yd = at(z, up(y), x, c), at(z, down(y), x, c)
    zu, zd = at(up(z), y, x, c), at(down(z), y, x, c)
    greet([xu, xd, sib, yu, yd, zu, zd])
    w = Wire(ssem, rsem)
    lane = lambda xx: xx * 2 + c
    own = lane(x)
    ha, hb = slice(0, 3), slice(3, 6)
    pairs = ((q, qg), (do, dg))
    ru_a, rd_b, ru_b, rd_a = [], [], [], []
    k_u = w.send(k, kg.at[z, y], yu)
    k_d = w.send(k, kg.at[z, y], yd)
    v_u = w.send(v, vg.at[z, y], zu)
    v_d = w.send(v, vg.at[z, y], zd)
    for src, dst in pairs:
        ru_a.append(w.send(src.at[ha], dst.at[ha, own], xu))
        rd_b.append(w.send(src.at[hb], dst.at[hb, own], xd))
    su = w.send(st, sg.at[own], xu)
    sd = w.send(st, sg.at[own], xd)
    for src, dst in pairs:
        ru_b.append(w.send(src.at[hb], dst.at[hb, own], xu))
        rd_a.append(w.send(src.at[ha], dst.at[ha, own], xd))
    sibs = [w.send(st, sg.at[own], sib)]
    for src, dst in pairs:
        sibs.append(w.send(src, dst.at[:, own], sib))
    kz, vy = {}, {}
    kz['u', 0] = w.send(k, kg.at[z, y], zu)
    kz['d', 0] = w.send(k, kg.at[z, y], zd)
    vy['u', 0] = w.send(v, vg.at[z, y], yu)
    vy['d', 0] = w.send(v, vg.at[z, y], yd)
    kg[z, y] = k[...]
    vg[z, y] = v[...]
    sg[own] = st[...]
    for j in range(q.shape[0]):
        qg[j, own] = q[j]
        dg[j, own] = do[j]
    lo_rows, hi_rows = pl.ds(0, 160), pl.ds(160, 144)
    k_u.wait_recv()
    kf_a = w.send(kg.at[z, down(y), lo_rows], kg.at[z, down(y), lo_rows], yu)
    k_d.wait_recv()
    kf_b = w.send(kg.at[z, up(y), hi_rows], kg.at[z, up(y), hi_rows], yd)
    v_u.wait_recv()
    vf_a = w.send(vg.at[down(z), y, lo_rows], vg.at[down(z), y, lo_rows], zu)
    v_d.wait_recv()
    vf_b = w.send(vg.at[up(z), y, hi_rows], vg.at[up(z), y, hi_rows], zd)
    for r, yy, zz in ((3, down(y), down(z)), (1, up(y), up(z))):
        for name, dev in (('u', zu), ('d', zd)):
            kz[name, r] = w.send(kg.at[z, yy], kg.at[z, yy], dev)
        for name, dev in (('u', yu), ('d', yd)):
            vy[name, r] = w.send(vg.at[zz, y], vg.at[zz, y], dev)
    kf_a.wait_recv()
    kf_b.wait_recv()
    for name, dev in (('u', zu), ('d', zd)):
        kz[name, 2] = w.send(kg.at[z, far(y)], kg.at[z, far(y)], dev)
    vf_a.wait_recv()
    vf_b.wait_recv()
    for name, dev in (('u', yu), ('d', yd)):
        vy[name, 2] = w.send(vg.at[far(z), y], vg.at[far(z), y], dev)
    ld, lu, lf = lane(down(x)), lane(up(x)), lane(far(x))
    fu, fd = [], []
    for i, (_, g) in enumerate(pairs):
        ru_a[i].wait_recv()
        fu.append(w.send(g.at[ha, ld], g.at[ha, ld], xu))
        rd_b[i].wait_recv()
        fd.append(w.send(g.at[hb, lu], g.at[hb, lu], xd))
    su.wait_recv()
    sf = w.send(sg.at[ld], sg.at[ld], xu)
    sd.wait_recv()
    for i, (_, g) in enumerate(pairs):
        sibs.append(w.send(g.at[ha, ld], g.at[ha, ld], sib))
        sibs.append(w.send(g.at[hb, lu], g.at[hb, lu], sib))
    sibs.append(w.send(sg.at[ld], sg.at[ld], sib))
    sibs.append(w.send(sg.at[lu], sg.at[lu], sib))
    slot = lambda r, v_: lax.rem(v_ + r, 4)
    kzf, vyf = [], []
    for r in (0, 3, 1, 2):
        yy, zz = slot(r, y), slot(r, z)
        kz['u', r].wait_recv()
        if r in (0, 1):
            kzf.append(w.send(kg.at[down(z), yy], kg.at[down(z), yy], zu))
        kz['d', r].wait_recv()
        if r in (2, 3):
            kzf.append(w.send(kg.at[up(z), yy], kg.at[up(z), yy], zd))
        vy['u', r].wait_recv()
        if r in (0, 1):
            vyf.append(w.send(vg.at[zz, down(y)], vg.at[zz, down(y)], yu))
        vy['d', r].wait_recv()
        if r in (2, 3):
            vyf.append(w.send(vg.at[zz, up(y)], vg.at[zz, up(y)], yd))
    for i, (_, g) in enumerate(pairs):
        ru_b[i].wait_recv()
        sibs.append(w.send(g.at[hb, ld], g.at[hb, ld], sib))
        rd_a[i].wait_recv()
        sibs.append(w.send(g.at[ha, lu], g.at[ha, lu], sib))
    sf.wait_recv()
    sibs.append(w.send(sg.at[lf], sg.at[lf], sib))
    for i, (_, g) in enumerate(pairs):
        fu[i].wait_recv()
        sibs.append(w.send(g.at[ha, lf], g.at[ha, lf], sib))
        fd[i].wait_recv()
        sibs.append(w.send(g.at[hb, lf], g.at[hb, lf], sib))
    for cp in kzf + vyf + sibs:
        cp.wait_recv()
    w.finish()


def gather(q, do, st, k, v):
    n_sub = q.shape[0]
    vm = pl.BlockSpec(memory_space=pltpu.VMEM)
    return pl.pallas_call(
        gather_body,
        in_specs=[vm] * 5,
        out_specs=[vm] * 5,
        out_shape=[
            jax.ShapeDtypeStruct((n_sub, 8, 128, 128), BF16),
            jax.ShapeDtypeStruct((n_sub, 8, 128, 128), BF16),
            jax.ShapeDtypeStruct((8,) + st.shape, F32),
            jax.ShapeDtypeStruct((4, 4) + k.shape, BF16),
            jax.ShapeDtypeStruct((4, 4) + k.shape, BF16),
        ],
        scratch_shapes=[pltpu.SemaphoreType.DMA((80,)), pltpu.SemaphoreType.DMA((80,))],
        compiler_params=pltpu.CompilerParams(collective_id=0, has_side_effects=True, vmem_limit_bytes=8 * 2**20),
        name='gather',
    )(q, do, st, k, v)


def attend_body(scale, bnd, kg, vg, q, do, st, lim, dq, dk, dv, acc):
    j = pl.program_id(0)
    n_keys = kg.shape[0]
    n_lane = q.shape[1]

    @pl.when(j == 0)
    def _():
        def clear(i, _):
            rows = pl.ds(pl.multiple_of(i * 64, 64), 64)
            dk[rows, :] = jnp.zeros((64, 128), F32)
            dv[rows, :] = jnp.zeros((64, 128), F32)
            return 0
        lax.fori_loop(0, n_keys // 64, clear, 0)

    acc[...] = jnp.zeros_like(acc)
    start, tiles = bnd[j, 0], bnd[j, 1]

    def tile(i, _):
        nominal = start + i * TK
        first = pl.multiple_of(jnp.minimum(nominal, n_keys - TK), 16)
        rows = pl.ds(first, TK)
        kt, vt = kg[rows, :], vg[rows, :]
        ktt = kt.T
        index = lax.broadcasted_iota(jnp.int32, (TK, 128), 0) + first
        ak = jnp.zeros((TK, 128), F32)
        av = jnp.zeros((TK, 128), F32)
        for m in range(n_lane // 2):
            qc = q[0, 2 * m:2 * m + 2].reshape(256, 128)
            dc = do[0, 2 * m:2 * m + 2].reshape(256, 128)
            s = lax.dot_general(kt, qc, (((1,), (1,)), ((), ())), preferred_element_type=F32)
            dp = lax.dot_general(vt, dc, (((1,), (1,)), ((), ())), preferred_element_type=F32)
            ps, dss = [], []
            for h in range(2):
                l = 2 * m + h
                cols = slice(128 * h, 128 * h + 128)
                lse, delta = st[l, pl.ds(j, 1), :], st[l, pl.ds(j + 8, 1), :]
                low, high = lim[l, pl.ds(j, 1), :], lim[l, pl.ds(j + 8, 1), :]
                e = jnp.exp2(s[:, cols] * (scale * LOG2E) - lse)
                p = jnp.where((index >= jnp.maximum(low, nominal)) & (index < high), e, 0.0)
                ps.append(p.astype(BF16))
                dss.append((p * (dp[:, cols] - delta)).astype(BF16))
            pb, db = jnp.concatenate(ps, axis=1), jnp.concatenate(dss, axis=1)
            av += jnp.dot(pb, dc, preferred_element_type=F32)
            ak += jnp.dot(db, qc, preferred_element_type=F32)
            acc[:, 256 * m:256 * m + 256] += jnp.dot(ktt, db, preferred_element_type=F32)
        dk[rows, :] += ak * scale
        dv[rows, :] += av
        return 0

    lax.fori_loop(0, tiles, tile, 0)
    for l in range(n_lane):
        dq[0, l] = acc[:, 128 * l:128 * l + 128].T * scale


def attend(bnd, kg, vg, q, do, st, lim):
    n_sub, n_lane = q.shape[0], q.shape[1]
    whole = lambda a: pl.BlockSpec(a.shape, lambda j, *_: (0,) * a.ndim)
    one = lambda a: pl.BlockSpec((1,) + a.shape[1:], lambda j, *_: (j,) + (0,) * (a.ndim - 1))
    return pl.pallas_call(
        functools.partial(attend_body, 128 ** -0.5),
        grid_spec=pltpu.PrefetchScalarGridSpec(
            num_scalar_prefetch=1, grid=(n_sub,),
            in_specs=[whole(kg), whole(vg), one(q), one(do), whole(st), whole(lim)],
            out_specs=[one(q), whole(kg), whole(kg)],
            scratch_shapes=[pltpu.VMEM((128, n_lane * 128), F32)]),
        out_shape=[jax.ShapeDtypeStruct(q.shape, F32), jax.ShapeDtypeStruct(kg.shape, F32),
                   jax.ShapeDtypeStruct(kg.shape, F32)],
        compiler_params=pltpu.CompilerParams(vmem_limit_bytes=40 * 2**20, dimension_semantics=('arbitrary',)),
        name='attend',
    )(bnd, kg, vg, q, do, st, lim)


class Ring:
    def __init__(self, w, place_, dev_up, dev_down, block, via, got):
        self.w, self.p, self.up, self.dn = w, place_, dev_up, dev_down
        self.block, self.via, self.got = block, via, got

    def start(self):
        w, p = self.w, self.p
        self.fu = w.send(self.block(far(p), 0), self.via(0), self.up)
        self.fd = w.send(self.block(far(p), 1), self.via(1), self.dn)
        self.du = w.send(self.block(up(p), 1), self.got(0, 1), self.up)
        self.dd = w.send(self.block(down(p), 0), self.got(1, 0), self.dn)

    def middle(self, add):
        w, p = self.w, self.p
        self.fu.wait_recv()
        add(self.via(0), self.block(up(p), 0))
        self.mu = w.send(self.via(0), self.got(0, 0), self.up)
        self.fd.wait_recv()
        add(self.via(1), self.block(down(p), 1))
        self.md = w.send(self.via(1), self.got(1, 1), self.dn)

    def wait(self):
        for cp in (self.du, self.dd, self.mu, self.md):
            cp.wait_recv()


def scatter_body(dq, dk, dv, oq, ok, ov, sq, sv, sg, kv_, kg_, ks, k2v, k2g, vv_, vg_, vs, v2v, v2g, ssem, rsem):
    z, y, x, c = place()
    xu, xd, sib = at(z, y, up(x), c), at(z, y, down(x), c), at(z, y, x, 1 - c)
    yu, yd = at(z, up(y), x, c), at(z, down(y), x, c)
    zu, zd = at(up(z), y, x, c), at(down(z), y, x, c)
    greet([xu, xd, sib, yu, yd, zu, zd])
    w = Wire(ssem, rsem)
    n_sub = dq.shape[0]
    hn = n_sub // 2

    def add(dst, src):
        dst[...] = dst[...] + src[...]

    order = (far(x), up(x), down(x), x)
    cross = [w.send(dq.at[:, xx * 2 + 1 - c], sq.at[xx], sib) for xx in order]
    hz = (pl.ds(0, 2), pl.ds(2, 2))
    kr = Ring(w, z, zu, zd, lambda b, h: dk.at[b, hz[h]], lambda h: kv_.at[h], lambda s, h: kg_.at[s, hz[h]])
    vr = Ring(w, y, yu, yd, lambda b, h: dv.at[hz[h], b], lambda h: vv_.at[h], lambda s, h: vg_.at[s, hz[h]])
    kr.start()
    vr.start()
    for cp, xx in zip(cross, order):
        cp.wait_recv()
        for j in range(n_sub):
            sq[xx, j] = sq[xx, j] + dq[j, xx * 2 + c]
    hj = (pl.ds(0, hn), pl.ds(hn, n_sub - hn))
    qr = Ring(w, x, xu, xd, lambda b, h: sq.at[b, hj[h]], lambda h: sv.at[h], lambda s, h: sg.at[s, hj[h]])
    qr.start()
    qr.middle(add)
    kr.middle(add)
    vr.middle(add)
    qr.wait()
    oq[...] = (sq[x] + sg[0] + sg[1]).astype(BF16)
    hr = (pl.ds(0, 160), pl.ds(160, 144))
    k2 = Ring(w, y, yu, yd, lambda b, h: ks.at[b, hr[h]], lambda h: k2v.at[h, pl.ds(0, (160, 144)[h])],
              lambda s, h: k2g.at[s, hr[h]])
    v2 = Ring(w, z, zu, zd, lambda b, h: vs.at[b, hr[h]], lambda h: v2v.at[h, pl.ds(0, (160, 144)[h])],
              lambda s, h: v2g.at[s, hr[h]])
    kr.wait()
    for b in range(4):
        ks[b] = dk[z, b] + kg_[0, b] + kg_[1, b]
    vr.wait()
    for b in range(4):
        vs[b] = dv[b, y] + vg_[0, b] + vg_[1, b]
    k2.start()
    v2.start()
    k2.middle(add)
    v2.middle(add)
    k2.wait()
    ok[...] = ks[y] + k2g[0] + k2g[1]
    v2.wait()
    ov[...] = vs[z] + v2g[0] + v2g[1]
    w.finish()


def scatter(dq, dk, dv):
    n_sub = dq.shape[0]
    rows = dk.shape[2]
    vm = pl.BlockSpec(memory_space=pltpu.VMEM)
    stage = [
        pltpu.VMEM((2, 2, rows, 128), F32),
        pltpu.VMEM((2, 4, rows, 128), F32),
        pltpu.VMEM((4, rows, 128), F32),
        pltpu.VMEM((2, 160, 128), F32),
        pltpu.VMEM((2, rows, 128), F32),
    ]
    return pl.pallas_call(
        scatter_body,
        in_specs=[vm] * 3,
        out_specs=[vm] * 3,
        out_shape=[
            jax.ShapeDtypeStruct((n_sub, 128, 128), BF16),
            jax.ShapeDtypeStruct((rows, 128), F32),
            jax.ShapeDtypeStruct((rows, 128), F32),
        ],
        scratch_shapes=[
            pltpu.VMEM((4, n_sub, 128, 128), F32),
            pltpu.VMEM((2, n_sub // 2, 128, 128), F32),
            pltpu.VMEM((2, n_sub, 128, 128), F32),
        ] + stage + stage + [pltpu.SemaphoreType.DMA((40,)), pltpu.SemaphoreType.DMA((40,))],
        compiler_params=pltpu.CompilerParams(collective_id=1, has_side_effects=True, vmem_limit_bytes=20 * 2**20),
        name='scatter',
    )(dq, dk, dv)


def limits(doc_ids, n_sub, sub_len, keys_local):
    z, y, x, c = place()
    lane = x * 2 + c
    n_pos = doc_ids.shape[0]
    sub_start = n_pos - n_sub * sub_len
    period = 8 * keys_local

    def flat(pos):
        return (pos // period) * keys_local + jnp.clip(pos % period - lane * keys_local, 0, keys_local)

    tok = 8 * (sub_len // 128)
    grp = z * 4 + y
    docs = lax.dynamic_index_in_dim(doc_ids[sub_start:].reshape(n_sub, 16, tok), grp, axis=1, keepdims=False)
    pos = sub_start + jnp.arange(n_sub)[:, None] * sub_len + grp * tok + jnp.arange(tok)[None, :]
    head = docs[:, :1]
    before = jnp.sum((doc_ids[None, :] < head).astype(jnp.int32), axis=1, keepdims=True)
    inside = jnp.sum((docs[:, :, None] > docs[:, None, :]).astype(jnp.int32), axis=2)
    begin = jnp.where(docs == head, before, pos[:, :1] + inside)
    low, high = flat(begin), flat(pos + 1)
    start = flat(before[:, 0]) // 16 * 16
    tiles = (flat(pos[:, -1] + 1) - start + TK - 1) // TK
    bnd = jnp.stack([start, tiles], axis=1)
    spread = lambda a: jnp.broadcast_to(a.reshape(n_sub, 8, tok // 8, 1), (n_sub, 8, tok // 8, 16)).reshape(n_sub, 8, 128)
    pad = ((0, 8 - n_sub), (0, 0), (0, 0))
    lim = jnp.concatenate([jnp.pad(spread(low), pad), jnp.pad(spread(high), pad)], axis=0)
    return bnd, lim.transpose(1, 0, 2)


def solution(mesh):
    q_spec = P(None, 'cp', 'tp', None)
    lse_spec = P(None, 'cp', 'tp')
    kv_spec = P('cp', 'tp', None)

    def local_backward(query, out_act, out_grad, row_lse, key_act, value_act, doc_ids):
        n_sub, local_len, n_heads, head_dim = query.shape
        keys_local = key_act.shape[0]
        rows = local_len * n_heads
        q = query.reshape(n_sub, rows, head_dim)
        do = out_grad.reshape(n_sub, rows, head_dim)
        delta = jnp.sum(out_grad.astype(F32) * out_act.astype(F32), axis=-1).reshape(n_sub, rows)
        lse = (row_lse * LOG2E).reshape(n_sub, rows)
        pad = ((0, 8 - n_sub), (0, 0))
        st = jnp.concatenate([jnp.pad(lse, pad), jnp.pad(delta, pad)], axis=0)
        bnd, lim = limits(doc_ids, n_sub, local_len * 128, keys_local)
        k, v = key_act.reshape(keys_local, head_dim), value_act.reshape(keys_local, head_dim)
        qg, dg, sg, kg, vg = gather(q, do, st, k, v)
        flat = (16 * keys_local, head_dim)
        dq, dk, dv = attend(bnd, kg.reshape(flat), vg.reshape(flat), qg, dg, sg, lim)
        blocks = (4, 4, keys_local, head_dim)
        oq, ok, ov = scatter(dq, dk.reshape(blocks), dv.reshape(blocks))
        return (oq.reshape(query.shape), ok.reshape(keys_local, 1, head_dim), ov.reshape(keys_local, 1, head_dim))

    return jax.shard_map(local_backward, mesh=mesh, in_specs=(q_spec, q_spec, q_spec, lse_spec, kv_spec, kv_spec, P()), out_specs=(q_spec, kv_spec, kv_spec), check_vma=False)
```

```python
import functools

import jax
import jax.numpy as jnp
from jax import lax
from jax.experimental import pallas as pl
from jax.experimental.pallas import tpu as pltpu
from jax.sharding import PartitionSpec as P

MESH = pl.DeviceIdType.MESH
TK = 256
LANES = 128
LOG2E = 1.4426950408889634
F32, BF16 = jnp.float32, jnp.bfloat16


def place():
    me = lax.axis_index('cp')
    return me // 32, lax.rem(me // 8, 4), lax.rem(me // 2, 4), lax.rem(me, 2)


def at(z, y, x, c):
    return ((z * 4 + y) * 4 + x) * 2 + c


def up(v):
    return lax.rem(v + 1, 4)


def down(v):
    return lax.rem(v + 3, 4)


def far(v):
    return lax.rem(v + 2, 4)


class Wire:
    def __init__(self, ssem, rsem):
        self.ssem, self.rsem, self.n, self.sent = ssem, rsem, 0, []

    def copy(self, src, dst, dev):
        cp = pltpu.make_async_remote_copy(
            src_ref=src, dst_ref=dst, send_sem=self.ssem.at[self.n], recv_sem=self.rsem.at[self.n],
            device_id={'cp': dev}, device_id_type=MESH)
        self.n += 1
        return cp

    def send(self, src, dst, dev):
        cp = self.copy(src, dst, dev)
        cp.start()
        self.sent.append(cp)
        return cp

    def finish(self):
        for cp in self.sent:
            cp.wait_send()


def greet(partners):
    barrier = pltpu.get_barrier_semaphore()
    for dev in partners:
        pl.semaphore_signal(barrier, inc=1, device_id={'cp': dev}, device_id_type=MESH)
    pl.semaphore_wait(barrier, len(partners))


def row_stats(do, o, lse, st):
    st[...] = jnp.zeros_like(st)
    tok = lax.broadcasted_iota(jnp.int32, (8, LANES), 0)
    lane = lax.broadcasted_iota(jnp.int32, (8, LANES), 1)
    for j in range(do.shape[0]):
        wide = jnp.concatenate([lse[j]] * 8, axis=1)
        st[j:j + 1, :] = jnp.sum(jnp.where((lane >> 4) == tok, wide, 0.0), axis=0, keepdims=True) * LOG2E
        prod = do[j].astype(F32) * o[j].astype(F32)
        st[8 + j:9 + j, :] = jnp.sum(prod.T, axis=0, keepdims=True)


def limits(doc, n_sub, sub_len, keys_local, lim, bnd):
    z, y, x, c = place()
    grp, lane = z * 4 + y, x * 2 + c
    n_pos = doc.shape[0] * LANES
    sub_start = n_pos - n_sub * sub_len
    period = 8 * keys_local

    def flat(pos):
        b = jnp.zeros_like(pos)
        for i in range(1, n_pos // period):
            b += jnp.where(pos >= i * period, 1, 0)
        return b * keys_local + jnp.clip(pos - b * period - lane * keys_local, 0, keys_local)

    sub = lax.broadcasted_iota(jnp.int32, (8, LANES), 0)
    tok = lax.broadcasted_iota(jnp.int32, (8, LANES), 1)
    docs = jnp.zeros((8, LANES), jnp.int32)
    for j in range(n_sub):
        row = doc[pl.ds((sub_start + j * sub_len) // LANES + grp // 2, 1), :]
        docs = jnp.where(sub == j, row, docs)
    docs = jnp.where(lax.rem(grp, 2) == 1, pltpu.roll(docs, 64, 1), docs)
    before = jnp.zeros((8, LANES), jnp.int32)
    for j in range(n_sub):
        head = docs[j:j + 1, 0:1]
        count = jnp.zeros((8, LANES), jnp.int32)
        for r in range(0, doc.shape[0], 8):
            count += jnp.where(doc[r:r + 8, :] < head, 1, 0)
        count = jnp.sum(jnp.sum(count.astype(F32), axis=0, keepdims=True), axis=1, keepdims=True)
        before = jnp.where(sub == j, count.astype(jnp.int32), before)
    base = sub_start + sub * sub_len + grp * 64
    pos = base + tok
    begin = jnp.where((tok > 0) & (docs != pltpu.roll(docs, 1, 1)), pos, before)
    for shift in (1, 2, 4, 8, 16, 32):
        begin = jnp.maximum(begin, jnp.where(tok >= shift, pltpu.roll(begin, shift, 1), 0))
    pick = jnp.where(
        lax.broadcasted_iota(jnp.int32, (LANES, 1024), 0) == lax.broadcasted_iota(jnp.int32, (LANES, 1024), 1) >> 4, 1.0, 0.0)
    for first, value in ((0, flat(begin)), (8, flat(pos + 1))):
        wide = jnp.dot(value.astype(F32), pick, precision=lax.Precision.HIGHEST, preferred_element_type=F32)
        for l in range(8):
            lim[l, first:first + 8, :] = wide[:, LANES * l:LANES * l + LANES].astype(jnp.int32)
    start = flat(before) & -16
    tiles = jnp.maximum((flat(base + 64) - start + (TK - 1)) // TK, 1)
    first = doc[pl.ds(sub_start // LANES, 1), :][:, 0:1]
    edge = lambda planes: doc[pl.ds((n_pos - planes * n_pos // 4 - 1) // LANES, 1), :][:, 127:LANES] >= first
    which = jnp.where(edge(1), jnp.where(edge(2), 2, 1), 0)
    bnd[...] = jnp.where(tok == 0, start, jnp.where(tok == 1, tiles, which))


def clear(zq, zk, zv):
    def rows(i, _):
        for r in range(4):
            at_ = pl.ds(pl.multiple_of((i * 4 + r) * 16, 16), 16)
            zk[at_, :] = jnp.zeros((16, LANES), F32)
            zv[at_, :] = jnp.zeros((16, LANES), F32)
        return 0

    lax.fori_loop(0, zk.shape[0] // 64, rows, 0)

    def block(i, _):
        zq[i // 8, lax.rem(i, 8)] = jnp.zeros((LANES, LANES), F32)
        return 0

    lax.fori_loop(0, zq.shape[0] * 8, block, 0)


def gather_body(sub_len, q, do, o, lse, doc, k, v, qg, dg, sg, kg, vg, lim, bnd, zq, zk, zv, st, ov, lv, cv, lsem, ssem, rsem):
    z, y, x, c = place()
    xu, xd, sib = at(z, y, up(x), c), at(z, y, down(x), c), at(z, y, x, 1 - c)
    yu, yd = at(z, up(y), x, c), at(z, down(y), x, c)
    zu, zd = at(up(z), y, x, c), at(down(z), y, x, c)
    lane = lambda xx: xx * 2 + c
    own = lane(x)
    loads = []
    for i, (src, dst) in enumerate((
            (k, kg.at[z, y]), (v, vg.at[z, y]), (q, qg.at[:, own]), (do, dg.at[:, own]), (o, ov), (lse, lv), (doc, cv))):
        loads.append(pltpu.make_async_copy(src, dst, lsem.at[i]))
        loads[i].start()
    greet([xu, xd, sib, yu, yd, zu, zd])
    w = Wire(ssem, rsem)
    ha, hb = slice(0, 3), slice(3, 6)
    pairs = (qg, dg)
    k, v = kg.at[z, y], vg.at[z, y]
    ru_a, rd_b, ru_b, rd_a = [], [], [], []
    loads[0].wait()
    k_u = w.send(k, k, yu)
    k_d = w.send(k, k, yd)
    loads[1].wait()
    v_u = w.send(v, v, zu)
    v_d = w.send(v, v, zd)
    for i, g in enumerate(pairs):
        loads[2 + i].wait()
        ru_a.append(w.send(g.at[ha, own], g.at[ha, own], xu))
        rd_b.append(w.send(g.at[hb, own], g.at[hb, own], xd))
    for g in pairs:
        ru_b.append(w.send(g.at[hb, own], g.at[hb, own], xu))
        rd_a.append(w.send(g.at[ha, own], g.at[ha, own], xd))
    sibs = [w.send(g.at[:, own], g.at[:, own], sib) for g in pairs]
    kz, vy = {}, {}
    kz['u', 0] = w.send(k, k, zu)
    kz['d', 0] = w.send(k, k, zd)
    vy['u', 0] = w.send(v, v, yu)
    vy['d', 0] = w.send(v, v, yd)
    for cp in loads[4:]:
        cp.wait()
    row_stats(dg.at[:, own], ov, lv, st)
    sg[own] = st[...]
    limits(cv, qg.shape[0], sub_len, kg.shape[2], lim, bnd)
    su = w.send(st, sg.at[own], xu)
    sd = w.send(st, sg.at[own], xd)
    sibs.append(w.send(st, sg.at[own], sib))
    lo_rows, hi_rows = pl.ds(0, 160), pl.ds(160, 144)
    clear(zq, zk, zv)
    k_u.wait_recv()
    kf_a = w.send(kg.at[z, down(y), lo_rows], kg.at[z, down(y), lo_rows], yu)
    k_d.wait_recv()
    kf_b = w.send(kg.at[z, up(y), hi_rows], kg.at[z, up(y), hi_rows], yd)
    v_u.wait_recv()
    vf_a = w.send(vg.at[down(z), y, lo_rows], vg.at[down(z), y, lo_rows], zu)
    v_d.wait_recv()
    vf_b = w.send(vg.at[up(z), y, hi_rows], vg.at[up(z), y, hi_rows], zd)
    for r, yy, zz in ((3, down(y), down(z)), (1, up(y), up(z))):
        for name, dev in (('u', zu), ('d', zd)):
            kz[name, r] = w.send(kg.at[z, yy], kg.at[z, yy], dev)
        for name, dev in (('u', yu), ('d', yd)):
            vy[name, r] = w.send(vg.at[zz, y], vg.at[zz, y], dev)
    kf_a.wait_recv()
    kf_b.wait_recv()
    for name, dev in (('u', zu), ('d', zd)):
        kz[name, 2] = w.send(kg.at[z, far(y)], kg.at[z, far(y)], dev)
    vf_a.wait_recv()
    vf_b.wait_recv()
    for name, dev in (('u', yu), ('d', yd)):
        vy[name, 2] = w.send(vg.at[far(z), y], vg.at[far(z), y], dev)
    ld, lu, lf = lane(down(x)), lane(up(x)), lane(far(x))
    fu, fd = [], []
    for i, g in enumerate(pairs):
        ru_a[i].wait_recv()
        fu.append(w.send(g.at[ha, ld], g.at[ha, ld], xu))
        rd_b[i].wait_recv()
        fd.append(w.send(g.at[hb, lu], g.at[hb, lu], xd))
    su.wait_recv()
    sf = w.send(sg.at[ld], sg.at[ld], xu)
    sd.wait_recv()
    for i, g in enumerate(pairs):
        sibs.append(w.send(g.at[ha, ld], g.at[ha, ld], sib))
        sibs.append(w.send(g.at[hb, lu], g.at[hb, lu], sib))
    sibs.append(w.send(sg.at[ld], sg.at[ld], sib))
    sibs.append(w.send(sg.at[lu], sg.at[lu], sib))
    slot = lambda r, v_: lax.rem(v_ + r, 4)
    kzf, vyf = [], []
    for r in (0, 3, 1, 2):
        if r == 2:
            for i, g in enumerate(pairs):
                ru_b[i].wait_recv()
                sibs.append(w.send(g.at[hb, ld], g.at[hb, ld], sib))
                rd_a[i].wait_recv()
                sibs.append(w.send(g.at[ha, lu], g.at[ha, lu], sib))
        yy, zz = slot(r, y), slot(r, z)
        kz['u', r].wait_recv()
        if r in (0, 1):
            kzf.append(w.send(kg.at[down(z), yy], kg.at[down(z), yy], zu))
        kz['d', r].wait_recv()
        if r in (2, 3):
            kzf.append(w.send(kg.at[up(z), yy], kg.at[up(z), yy], zd))
        vy['u', r].wait_recv()
        if r in (0, 1):
            vyf.append(w.send(vg.at[zz, down(y)], vg.at[zz, down(y)], yu))
        vy['d', r].wait_recv()
        if r in (2, 3):
            vyf.append(w.send(vg.at[zz, up(y)], vg.at[zz, up(y)], yd))
    sf.wait_recv()
    sibs.append(w.send(sg.at[lf], sg.at[lf], sib))
    for i, g in enumerate(pairs):
        fu[i].wait_recv()
        sibs.append(w.send(g.at[ha, lf], g.at[ha, lf], sib))
        fd[i].wait_recv()
        sibs.append(w.send(g.at[hb, lf], g.at[hb, lf], sib))
    for cp in kzf + vyf + sibs:
        cp.wait_recv()
    w.finish()


def gather(sub_len, q, do, o, lse, doc, k, v):
    n_sub = q.shape[0]
    vm = pl.BlockSpec(memory_space=pltpu.VMEM)
    return pl.pallas_call(
        functools.partial(gather_body, sub_len),
        in_specs=[pl.BlockSpec(memory_space=pltpu.HBM)] * 7,
        out_specs=[vm] * 10,
        out_shape=[
            jax.ShapeDtypeStruct((n_sub, 8, LANES, LANES), BF16),
            jax.ShapeDtypeStruct((n_sub, 8, LANES, LANES), BF16),
            jax.ShapeDtypeStruct((8, 16, LANES), F32),
            jax.ShapeDtypeStruct((4, 4) + k.shape, BF16),
            jax.ShapeDtypeStruct((4, 4) + k.shape, BF16),
            jax.ShapeDtypeStruct((8, 16, LANES), jnp.int32),
            jax.ShapeDtypeStruct((8, LANES), jnp.int32),
            jax.ShapeDtypeStruct((n_sub, 8, LANES, LANES), F32),
            jax.ShapeDtypeStruct((16 * k.shape[0], LANES), F32),
            jax.ShapeDtypeStruct((16 * k.shape[0], LANES), F32),
        ],
        scratch_shapes=[
            pltpu.VMEM((16, LANES), F32), pltpu.VMEM(o.shape, BF16), pltpu.VMEM(lse.shape, F32), pltpu.VMEM(doc.shape, jnp.int32),
            pltpu.SemaphoreType.DMA((7,)), pltpu.SemaphoreType.DMA((80,)), pltpu.SemaphoreType.DMA((80,))],
        compiler_params=pltpu.CompilerParams(collective_id=0, has_side_effects=True, vmem_limit_bytes=8 * 2**20),
        name='gather',
    )(*[pltpu.with_memory_space_constraint(a, pltpu.HBM) for a in (q, do, o, lse, doc, k, v)])


def attend_body(scale, bnd, kg, vg, q, do, st, lim, zq, zk, zv, dq, dk, dv, which, p0, d0, p1, d1):
    n_keys, n_sub, n_lane = kg.shape[0], q.shape[0], q.shape[1]

    p1[...] = jnp.zeros_like(p1)
    d1[...] = jnp.zeros_like(d1)
    which[0] = bnd[0, 2]
    total = bnd[0, 1]
    for j in range(1, n_sub):
        total = total + bnd[j, 1]

    def tile_of(j, i):
        nominal = bnd[j, 0] + i * TK
        return nominal, pl.multiple_of(jnp.minimum(nominal, n_keys - TK), 16)

    def front(j, i, pr, dr):
        nominal, first = tile_of(j, i)
        rows = pl.ds(first, TK)
        kt, vt = kg[rows, :], vg[rows, :]
        index = lax.broadcasted_iota(jnp.int32, (TK, LANES), 0) + first
        for m in range(n_lane // 2):
            qc = q[j, 2 * m:2 * m + 2].reshape(256, LANES)
            dc = do[j, 2 * m:2 * m + 2].reshape(256, LANES)
            s = lax.dot_general(kt, qc, (((1,), (1,)), ((), ())), preferred_element_type=F32)
            dp = lax.dot_general(vt, dc, (((1,), (1,)), ((), ())), preferred_element_type=F32)
            for h in range(2):
                l = 2 * m + h
                cols = slice(LANES * h, LANES * h + LANES)
                lse, delta = st[l, pl.ds(j, 1), :], st[l, pl.ds(j + 8, 1), :]
                low, high = lim[l, pl.ds(j, 1), :], lim[l, pl.ds(j + 8, 1), :]
                e = jnp.exp2(s[:, cols] * (scale * LOG2E) - lse)
                p = jnp.where((index >= jnp.maximum(low, nominal)) & (index < high), e, 0.0)
                pr[l] = p.astype(BF16)
                dr[l] = (p * (dp[:, cols] - delta)).astype(BF16)

    def back(j, i, pr, dr):
        rows = pl.ds(tile_of(j, i)[1], TK)
        ktt = kg[rows, :].T
        pa = jnp.concatenate([pr[l] for l in range(n_lane)], axis=1)
        da = jnp.concatenate([dr[l] for l in range(n_lane)], axis=1)
        dv[rows, :] += jnp.dot(pa, do[j].reshape(n_lane * LANES, LANES), preferred_element_type=F32)
        dk[rows, :] += jnp.dot(da, q[j].reshape(n_lane * LANES, LANES), preferred_element_type=F32)
        for m in range(n_lane // 2):
            t = jnp.dot(ktt, da[:, 256 * m:256 * m + 256], preferred_element_type=F32)
            dq[j, 2 * m] += t[:, :LANES]
            dq[j, 2 * m + 1] += t[:, LANES:]

    def after(j, i):
        turn = (i + 1 >= bnd[j, 1]) & (j < n_sub - 1)
        return jnp.where(turn, j + 1, j), jnp.where(turn, 0, i + 1)

    def two(_, at_):
        hj, hi, j, i = at_
        front(j, i, p0, d0)
        back(hj, hi, p1, d1)
        nj, ni = after(j, i)
        front(nj, ni, p1, d1)
        back(j, i, p0, d0)
        return (nj, ni) + after(nj, ni)

    zero = jnp.int32(0)
    lax.fori_loop(0, (total + 2) // 2, two, (zero, zero, zero, zero))


def attend(bnd, kg, vg, q, do, st, lim, zq, zk, zv):
    n_lane = q.shape[1]
    vm = pl.BlockSpec(memory_space=pltpu.VMEM)
    return pl.pallas_call(
        functools.partial(attend_body, LANES ** -0.5),
        in_specs=[pl.BlockSpec(memory_space=pltpu.SMEM)] + [vm] * 9,
        out_specs=[vm] * 3 + [pl.BlockSpec(memory_space=pltpu.SMEM)],
        out_shape=[jax.ShapeDtypeStruct(q.shape, F32), jax.ShapeDtypeStruct(kg.shape, F32),
                   jax.ShapeDtypeStruct(kg.shape, F32), jax.ShapeDtypeStruct((1,), jnp.int32)],
        input_output_aliases={7: 0, 8: 1, 9: 2},
        scratch_shapes=[pltpu.VMEM((n_lane, TK, LANES), BF16)] * 4,
        compiler_params=pltpu.CompilerParams(vmem_limit_bytes=16 * 2**20),
        name='attend',
    )(bnd, kg, vg, q, do, st, lim, zq, zk, zv)


class Split:
    def __init__(self, planes, keys):
        self.planes, self.keys, self.parts = planes, keys, 4 // planes
        self.rows = -(-keys // self.parts // 16) * 16 if planes == 1 else keys // self.parts
        self.low = self.rows // 2 if self.rows % 16 == 0 else self.rows // 16 * 8
        self.last = keys - self.rows
        self.half = {4: (2, keys, LANES), 2: (keys, LANES), 1: (2 * self.rows, LANES)}[planes]

    def slot(self, z):
        if self.planes == 4:
            return z, 0
        if self.planes == 2:
            return jnp.where(lax.rem(z, 3) == 0, 3, 2), jnp.where(z < 2, self.rows, 0)
        return 3, jnp.minimum(lax.rem(z + 1, 4) * self.rows, self.last)

    def rows_at(self, first):
        return pl.ds(first if isinstance(first, int) else pl.multiple_of(first, 8), self.rows)

    def keys_of(self, dk, z, ys):
        owner, first = self.slot(z)
        return dk.at[owner, ys, self.rows_at(first)]

    def values_of(self, dv, y, h):
        if self.planes == 4:
            return dv.at[pl.ds(2 * h, 2), y]
        if self.planes == 2:
            return dv.at[2 + h, y]
        return dv.at[3, y, pl.ds(h * (self.keys - 2 * self.rows), 2 * self.rows)]

    def value_slot(self, vs, z):
        owner, first = self.slot(z)
        if self.planes == 4:
            return vs.at[z // 2, lax.rem(z, 2)]
        if self.planes == 2:
            return vs.at[owner - 2, self.rows_at(first)]
        h = jnp.where(first >= 2 * self.rows, 1, 0)
        return vs.at[h, self.rows_at(first - h * (self.keys - 2 * self.rows))]

    def shares(self):
        if self.planes == 4:
            return []
        if self.planes == 2:
            return [(3, 1, 0), (2, 1, 1)]
        return [(3, h, (3 + h) % 4) for h in (1, 2, 3)]


class Ring:
    def __init__(self, w, place_, dev_up, dev_down, block, via, got):
        self.w, self.p, self.up, self.dn = w, place_, dev_up, dev_down
        self.block, self.via, self.got = block, via, got

    def first(self):
        w, p = self.w, self.p
        self.fu = w.send(self.block(far(p), 0), self.via(0), self.up)
        self.fd = w.send(self.block(far(p), 1), self.via(1), self.dn)

    def direct_up(self):
        self.du = self.w.send(self.block(up(self.p), 1), self.got(0, 1), self.up)

    def direct_down(self):
        self.dd = self.w.send(self.block(down(self.p), 0), self.got(1, 0), self.dn)

    def start(self):
        self.first()
        self.direct_up()
        self.direct_down()

    def middle(self):
        w, p = self.w, self.p
        self.fu.wait_recv()
        add(self.via(0), self.block(up(p), 0))
        self.mu = w.send(self.via(0), self.got(0, 0), self.up)
        self.fd.wait_recv()
        add(self.via(1), self.block(down(p), 1))
        self.md = w.send(self.via(1), self.got(1, 1), self.dn)

    def wait(self):
        for cp in (self.du, self.dd, self.mu, self.md):
            cp.wait_recv()


def add(dst, src):
    dst[...] = dst[...] + src[...]


def scatter_body(scale, sp, dq, dk, dv, oq, ok, ov, sq, sv, sg, k1v, k1g, ks, k2v, k2g, kr, v1v, v1g, vs, v2v, v2g, vr, ssem, rsem):
    z, y, x, c = place()
    xu, xd, sib = at(z, y, up(x), c), at(z, y, down(x), c), at(z, y, x, 1 - c)
    yu, yd = at(z, up(y), x, c), at(z, down(y), x, c)
    zu, zd = at(up(z), y, x, c), at(down(z), y, x, c)
    greet([xu, xd, sib, yu, yd, zu, zd] + ([at(far(z), y, x, c)] if sp.planes == 1 else []))
    w = Wire(ssem, rsem)
    n_sub = dq.shape[0]
    hn = n_sub // 2
    order = (far(x), up(x), down(x), x)
    cross = [w.send(dq.at[:, xx * 2 + 1 - c], sq.at[xx], sib) for xx in order]
    hy = (pl.ds(0, 2), pl.ds(2, 2))
    kone = Ring(w, z, zu, zd, lambda b, h: sp.keys_of(dk, b, hy[h]), lambda h: k1v.at[h], lambda s, h: k1g.at[s, hy[h]])
    vone = Ring(w, y, yu, yd, lambda b, h: sp.values_of(dv, b, h), lambda h: v1v.at[h], lambda s, h: v1g.at[s, h])
    kone.start()
    vone.start()
    hj = (pl.ds(0, hn), pl.ds(hn, n_sub - hn))
    qring = Ring(w, x, xu, xd, lambda b, h: sq.at[b, hj[h]], lambda h: sv.at[h], lambda s, h: sg.at[s, hj[h]])
    for cp, xx, then in zip(cross, order, (qring.first, qring.direct_up, qring.direct_down, None)):
        cp.wait_recv()
        for j in range(n_sub):
            sq[xx, j] = sq[xx, j] + dq[j, xx * 2 + c]
        if then is not None:
            then()
    kone.middle()
    vone.middle()
    qring.middle()
    nr = (sp.low, sp.rows - sp.low)
    hr = (pl.ds(0, nr[0]), pl.ds(nr[0], nr[1]))
    ktwo = Ring(w, y, yu, yd, lambda b, h: ks.at[b, hr[h]], lambda h: k2v.at[h, pl.ds(0, nr[h])], lambda s, h: k2g.at[s, hr[h]])
    vtwo = Ring(w, z, zu, zd, lambda b, h: sp.value_slot(vs, b).at[hr[h]], lambda h: v2v.at[h, pl.ds(0, nr[h])],
                lambda s, h: v2g.at[s, hr[h]])
    kone.wait()
    for b in range(4):
        ks[b] = sp.keys_of(dk, z, b)[...] + k1g[0, b] + k1g[1, b]
    ktwo.start()
    vone.wait()
    for h in range(2):
        vs[h] = sp.values_of(dv, y, h)[...] + v1g[0, h] + v1g[1, h]
    vtwo.start()
    ktwo.middle()
    vtwo.middle()
    ktwo.wait()
    kr[0] = (ks[y] + k2g[0] + k2g[1]) * scale
    vtwo.wait()
    vr[0] = sp.value_slot(vs, z)[...] + v2g[0] + v2g[1]
    home = []
    for owner, h, taker in sp.shares():
        for buf, out in ((kr, ok), (vr, ov)):
            cp = w.copy(buf.at[0], buf.at[h], at(owner, y, x, c))
            home.append((owner, h, taker, buf, out, cp))
            pl.when(z == taker)(cp.start)
    qring.wait()
    for j in range(n_sub):
        oq[j] = ((sq[x, j] + sg[0, j] + sg[1, j]).T * scale).astype(BF16)
    if sp.planes == 4:
        ok[...] = kr[0]
        ov[...] = vr[0]
    else:
        @pl.when(z < 4 - sp.planes)
        def _():
            ok[...] = jnp.zeros_like(ok)
            ov[...] = jnp.zeros_like(ov)

        @pl.when(z >= 4 - sp.planes)
        def _():
            ok[0:sp.rows, :] = kr[0]
            ov[0:sp.rows, :] = vr[0]

        for owner, h, taker, buf, out, cp in home:
            first = min(h * sp.rows, sp.last)

            @pl.when(z == owner)
            def _():
                cp.wait_recv()
                out[first:first + sp.rows, :] = buf[h]

            pl.when(z == taker)(cp.wait_send)
    w.finish()


def scatter(planes, dq, dk, dv):
    n_sub = dq.shape[0]
    sp = Split(planes, dk.shape[2])
    rows = sp.rows
    vm = pl.BlockSpec(memory_space=pltpu.VMEM)
    two = [
        pltpu.VMEM((2, sp.low + sp.low % 16, LANES), F32),
        pltpu.VMEM((2, rows, LANES), F32),
        pltpu.VMEM((sp.parts, rows, LANES), F32),
    ]
    return pl.pallas_call(
        functools.partial(scatter_body, LANES ** -0.5, sp),
        in_specs=[vm] * 3,
        out_specs=[vm] * 3,
        out_shape=[
            jax.ShapeDtypeStruct((n_sub, LANES, LANES), BF16),
            jax.ShapeDtypeStruct((sp.keys, LANES), F32),
            jax.ShapeDtypeStruct((sp.keys, LANES), F32),
        ],
        scratch_shapes=[
            pltpu.VMEM((4, n_sub, LANES, LANES), F32),
            pltpu.VMEM((2, n_sub // 2, LANES, LANES), F32),
            pltpu.VMEM((2, n_sub, LANES, LANES), F32),
            pltpu.VMEM((2, 2, rows, LANES), F32), pltpu.VMEM((2, 4, rows, LANES), F32), pltpu.VMEM((4, rows, LANES), F32), *two,
            pltpu.VMEM((2,) + sp.half, F32), pltpu.VMEM((2, 2) + sp.half, F32), pltpu.VMEM((2,) + sp.half, F32), *two,
            pltpu.SemaphoreType.DMA((44,)), pltpu.SemaphoreType.DMA((44,))],
        compiler_params=pltpu.CompilerParams(collective_id=planes, has_side_effects=True, vmem_limit_bytes=20 * 2**20),
        name='scatter',
    )(dq, dk, dv)


def solution(mesh):
    q_spec = P(None, 'cp', 'tp', None)
    lse_spec = P(None, 'cp', 'tp')
    kv_spec = P('cp', 'tp', None)

    def local_backward(query, out_act, out_grad, row_lse, key_act, value_act, doc_ids):
        n_sub, local_len, n_heads, head_dim = query.shape
        keys_local = key_act.shape[0]
        rows = local_len * n_heads
        q = query.reshape(n_sub, rows, head_dim)
        do = out_grad.reshape(n_sub, rows, head_dim)
        o = out_act.reshape(n_sub, rows, head_dim)
        doc = doc_ids.reshape(-1, LANES)
        k, v = key_act.reshape(keys_local, head_dim), value_act.reshape(keys_local, head_dim)
        qg, dg, sg, kg, vg, lim, bnd, zq, zk, zv = gather(local_len * LANES, q, do, o, row_lse, doc, k, v)
        flat = (16 * keys_local, head_dim)
        dq, dk, dv, which = attend(bnd, kg.reshape(flat), vg.reshape(flat), qg, dg, sg, lim, zq, zk, zv)
        blocks = (4, 4, keys_local, head_dim)
        oq, ok, ov = lax.switch(which[0], [functools.partial(scatter, n) for n in (1, 2, 4)], dq, dk.reshape(blocks), dv.reshape(blocks))
        return (oq.reshape(query.shape), ok.reshape(keys_local, 1, head_dim), ov.reshape(keys_local, 1, head_dim))

    return jax.shard_map(local_backward, mesh=mesh, in_specs=(q_spec, q_spec, q_spec, lse_spec, kv_spec, kv_spec, P()), out_specs=(q_spec, kv_spec, kv_spec), check_vma=False)
```

```python
import functools

import jax
import jax.numpy as jnp
from jax import lax
from jax.experimental import pallas as pl
from jax.experimental.pallas import tpu as pltpu
from jax.sharding import PartitionSpec as P

MESH = pl.DeviceIdType.MESH
TK = 256
LANES = 128
LOG2E = 1.4426950408889634
F32, BF16 = jnp.float32, jnp.bfloat16


def place():
    me = lax.axis_index('cp')
    return me // 32, lax.rem(me // 8, 4), lax.rem(me // 2, 4), lax.rem(me, 2)


def at(z, y, x, c):
    return ((z * 4 + y) * 4 + x) * 2 + c


def up(v):
    return lax.rem(v + 1, 4)


def down(v):
    return lax.rem(v + 3, 4)


def far(v):
    return lax.rem(v + 2, 4)


class Wire:
    def __init__(self, ssem, rsem):
        self.ssem, self.rsem, self.n, self.sent = ssem, rsem, 0, []

    def copy(self, src, dst, dev):
        cp = pltpu.make_async_remote_copy(
            src_ref=src, dst_ref=dst, send_sem=self.ssem.at[self.n], recv_sem=self.rsem.at[self.n],
            device_id={'cp': dev}, device_id_type=MESH)
        self.n += 1
        return cp

    def send(self, src, dst, dev):
        cp = self.copy(src, dst, dev)
        cp.start()
        self.sent.append(cp)
        return cp

    def finish(self):
        for cp in self.sent:
            cp.wait_send()


def greet(partners):
    barrier = pltpu.get_barrier_semaphore()
    for dev in partners:
        pl.semaphore_signal(barrier, inc=1, device_id={'cp': dev}, device_id_type=MESH)
    pl.semaphore_wait(barrier, len(partners))


def row_stats(do, o, lse, st):
    st[...] = jnp.zeros_like(st)
    tok = lax.broadcasted_iota(jnp.int32, (8, LANES), 0)
    lane = lax.broadcasted_iota(jnp.int32, (8, LANES), 1)
    for j in range(do.shape[0]):
        wide = jnp.concatenate([lse[j]] * 8, axis=1)
        st[j:j + 1, :] = jnp.sum(jnp.where((lane >> 4) == tok, wide, 0.0), axis=0, keepdims=True) * LOG2E
        prod = do[j].astype(F32) * o[j].astype(F32)
        st[8 + j:9 + j, :] = jnp.sum(prod.T, axis=0, keepdims=True)


def limits(doc, n_sub, sub_len, keys_local, lim, bnd):
    z, y, x, c = place()
    grp, lane = z * 4 + y, x * 2 + c
    n_pos = doc.shape[0] * LANES
    sub_start = n_pos - n_sub * sub_len
    period = 8 * keys_local

    def flat(pos):
        b = jnp.zeros_like(pos)
        for i in range(1, n_pos // period):
            b += jnp.where(pos >= i * period, 1, 0)
        return b * keys_local + jnp.clip(pos - b * period - lane * keys_local, 0, keys_local)

    sub = lax.broadcasted_iota(jnp.int32, (8, LANES), 0)
    tok = lax.broadcasted_iota(jnp.int32, (8, LANES), 1)
    docs = jnp.zeros((8, LANES), jnp.int32)
    for j in range(n_sub):
        row = doc[pl.ds((sub_start + j * sub_len) // LANES + grp // 2, 1), :]
        docs = jnp.where(sub == j, row, docs)
    docs = jnp.where(lax.rem(grp, 2) == 1, pltpu.roll(docs, 64, 1), docs)
    before = jnp.zeros((8, LANES), jnp.int32)
    for j in range(n_sub):
        head = docs[j:j + 1, 0:1]
        count = jnp.zeros((8, LANES), jnp.int32)
        for r in range(0, doc.shape[0], 8):
            count += jnp.where(doc[r:r + 8, :] < head, 1, 0)
        count = jnp.sum(jnp.sum(count.astype(F32), axis=0, keepdims=True), axis=1, keepdims=True)
        before = jnp.where(sub == j, count.astype(jnp.int32), before)
    base = sub_start + sub * sub_len + grp * 64
    pos = base + tok
    begin = jnp.where((tok > 0) & (docs != pltpu.roll(docs, 1, 1)), pos, before)
    for shift in (1, 2, 4, 8, 16, 32):
        begin = jnp.maximum(begin, jnp.where(tok >= shift, pltpu.roll(begin, shift, 1), 0))
    pick = jnp.where(
        lax.broadcasted_iota(jnp.int32, (LANES, 1024), 0) == lax.broadcasted_iota(jnp.int32, (LANES, 1024), 1) >> 4, 1.0, 0.0)
    for first, value in ((0, flat(begin)), (8, flat(pos + 1))):
        wide = jnp.dot(value.astype(F32), pick, precision=lax.Precision.HIGHEST, preferred_element_type=F32)
        for l in range(8):
            lim[l, first:first + 8, :] = wide[:, LANES * l:LANES * l + LANES].astype(jnp.int32)
    start = flat(before) & -16
    tiles = jnp.maximum((flat(base + 64) - start + (TK - 1)) // TK, jnp.where(sub == 0, 1, 0))
    first = doc[pl.ds(sub_start // LANES, 1), :][:, 0:1]
    edge = lambda planes: doc[pl.ds((n_pos - planes * n_pos // 4 - 1) // LANES, 1), :][:, 127:LANES] >= first
    which = jnp.where(edge(1), jnp.where(edge(2), 2, 1), 0)
    bnd[...] = jnp.where(tok == 0, start, jnp.where(tok == 1, tiles, which))


def clear(zq, zk, zv):
    def rows(i, _):
        for r in range(4):
            at_ = pl.ds(pl.multiple_of((i * 4 + r) * 16, 16), 16)
            zk[at_, :] = jnp.zeros((16, LANES), F32)
            zv[at_, :] = jnp.zeros((16, LANES), F32)
        return 0

    lax.fori_loop(0, zk.shape[0] // 64, rows, 0)

    def block(i, _):
        zq[i // 8, lax.rem(i, 8)] = jnp.zeros((LANES, LANES), F32)
        return 0

    lax.fori_loop(0, zq.shape[0] * 8, block, 0)


def gather_body(sub_len, q, do, o, lse, doc, k, v, qg, dg, sg, kg, vg, lim, bnd, zq, zk, zv, st, ov, lv, cv, lsem, ssem, rsem):
    z, y, x, c = place()
    xu, xd, sib = at(z, y, up(x), c), at(z, y, down(x), c), at(z, y, x, 1 - c)
    yu, yd = at(z, up(y), x, c), at(z, down(y), x, c)
    zu, zd = at(up(z), y, x, c), at(down(z), y, x, c)
    lane = lambda xx: xx * 2 + c
    own = lane(x)
    loads = []
    for i, (src, dst) in enumerate((
            (k, kg.at[z, y]), (v, vg.at[z, y]), (q, qg.at[:, own]), (do, dg.at[:, own]), (o, ov), (lse, lv), (doc, cv))):
        loads.append(pltpu.make_async_copy(src, dst, lsem.at[i]))
        loads[i].start()
    greet([xu, xd, sib, yu, yd, zu, zd])
    w = Wire(ssem, rsem)
    ha, hb = slice(0, 3), slice(3, 6)
    pairs = (qg, dg)
    k, v = kg.at[z, y], vg.at[z, y]
    ru_a, rd_b, ru_b, rd_a = [], [], [], []
    loads[0].wait()
    k_u = w.send(k, k, yu)
    k_d = w.send(k, k, yd)
    loads[1].wait()
    v_u = w.send(v, v, zu)
    v_d = w.send(v, v, zd)
    for i, g in enumerate(pairs):
        loads[2 + i].wait()
        ru_a.append(w.send(g.at[ha, own], g.at[ha, own], xu))
        rd_b.append(w.send(g.at[hb, own], g.at[hb, own], xd))
    for g in pairs:
        ru_b.append(w.send(g.at[hb, own], g.at[hb, own], xu))
        rd_a.append(w.send(g.at[ha, own], g.at[ha, own], xd))
    sibs = [w.send(g.at[:, own], g.at[:, own], sib) for g in pairs]
    kz, vy = {}, {}
    kz['u', 0] = w.send(k, k, zu)
    kz['d', 0] = w.send(k, k, zd)
    vy['u', 0] = w.send(v, v, yu)
    vy['d', 0] = w.send(v, v, yd)
    for cp in loads[4:]:
        cp.wait()
    row_stats(dg.at[:, own], ov, lv, st)
    sg[own] = st[...]
    limits(cv, qg.shape[0], sub_len, kg.shape[2], lim, bnd)
    su = w.send(st, sg.at[own], xu)
    sd = w.send(st, sg.at[own], xd)
    sibs.append(w.send(st, sg.at[own], sib))
    lo_rows, hi_rows = pl.ds(0, 160), pl.ds(160, 144)
    clear(zq, zk, zv)
    k_u.wait_recv()
    kf_a = w.send(kg.at[z, down(y), lo_rows], kg.at[z, down(y), lo_rows], yu)
    k_d.wait_recv()
    kf_b = w.send(kg.at[z, up(y), hi_rows], kg.at[z, up(y), hi_rows], yd)
    v_u.wait_recv()
    vf_a = w.send(vg.at[down(z), y, lo_rows], vg.at[down(z), y, lo_rows], zu)
    v_d.wait_recv()
    vf_b = w.send(vg.at[up(z), y, hi_rows], vg.at[up(z), y, hi_rows], zd)
    for r, yy, zz in ((3, down(y), down(z)), (1, up(y), up(z))):
        for name, dev in (('u', zu), ('d', zd)):
            kz[name, r] = w.send(kg.at[z, yy], kg.at[z, yy], dev)
        for name, dev in (('u', yu), ('d', yd)):
            vy[name, r] = w.send(vg.at[zz, y], vg.at[zz, y], dev)
    kf_a.wait_recv()
    kf_b.wait_recv()
    for name, dev in (('u', zu), ('d', zd)):
        kz[name, 2] = w.send(kg.at[z, far(y)], kg.at[z, far(y)], dev)
    vf_a.wait_recv()
    vf_b.wait_recv()
    for name, dev in (('u', yu), ('d', yd)):
        vy[name, 2] = w.send(vg.at[far(z), y], vg.at[far(z), y], dev)
    ld, lu, lf = lane(down(x)), lane(up(x)), lane(far(x))
    fu, fd = [], []
    for i, g in enumerate(pairs):
        ru_a[i].wait_recv()
        fu.append(w.send(g.at[ha, ld], g.at[ha, ld], xu))
        rd_b[i].wait_recv()
        fd.append(w.send(g.at[hb, lu], g.at[hb, lu], xd))
    su.wait_recv()
    sf = w.send(sg.at[ld], sg.at[ld], xu)
    sd.wait_recv()
    for i, g in enumerate(pairs):
        sibs.append(w.send(g.at[ha, ld], g.at[ha, ld], sib))
        sibs.append(w.send(g.at[hb, lu], g.at[hb, lu], sib))
    sibs.append(w.send(sg.at[ld], sg.at[ld], sib))
    sibs.append(w.send(sg.at[lu], sg.at[lu], sib))
    slot = lambda r, v_: lax.rem(v_ + r, 4)
    kzf, vyf = [], []
    for r in (0, 3, 1, 2):
        if r == 2:
            for i, g in enumerate(pairs):
                ru_b[i].wait_recv()
                sibs.append(w.send(g.at[hb, ld], g.at[hb, ld], sib))
                rd_a[i].wait_recv()
                sibs.append(w.send(g.at[ha, lu], g.at[ha, lu], sib))
        yy, zz = slot(r, y), slot(r, z)
        kz['u', r].wait_recv()
        if r in (0, 1):
            kzf.append(w.send(kg.at[down(z), yy], kg.at[down(z), yy], zu))
        kz['d', r].wait_recv()
        if r in (2, 3):
            kzf.append(w.send(kg.at[up(z), yy], kg.at[up(z), yy], zd))
        vy['u', r].wait_recv()
        if r in (0, 1):
            vyf.append(w.send(vg.at[zz, down(y)], vg.at[zz, down(y)], yu))
        vy['d', r].wait_recv()
        if r in (2, 3):
            vyf.append(w.send(vg.at[zz, up(y)], vg.at[zz, up(y)], yd))
    sf.wait_recv()
    sibs.append(w.send(sg.at[lf], sg.at[lf], sib))
    for i, g in enumerate(pairs):
        fu[i].wait_recv()
        sibs.append(w.send(g.at[ha, lf], g.at[ha, lf], sib))
        fd[i].wait_recv()
        sibs.append(w.send(g.at[hb, lf], g.at[hb, lf], sib))
    for cp in kzf + vyf + sibs:
        cp.wait_recv()
    w.finish()


def gather(sub_len, q, do, o, lse, doc, k, v):
    n_sub = q.shape[0]
    vm = pl.BlockSpec(memory_space=pltpu.VMEM)
    return pl.pallas_call(
        functools.partial(gather_body, sub_len),
        in_specs=[pl.BlockSpec(memory_space=pltpu.HBM)] * 7,
        out_specs=[vm] * 10,
        out_shape=[
            jax.ShapeDtypeStruct((n_sub, 8, LANES, LANES), BF16),
            jax.ShapeDtypeStruct((n_sub, 8, LANES, LANES), BF16),
            jax.ShapeDtypeStruct((8, 16, LANES), F32),
            jax.ShapeDtypeStruct((4, 4) + k.shape, BF16),
            jax.ShapeDtypeStruct((4, 4) + k.shape, BF16),
            jax.ShapeDtypeStruct((8, 16, LANES), jnp.int32),
            jax.ShapeDtypeStruct((8, LANES), jnp.int32),
            jax.ShapeDtypeStruct((n_sub, 8, LANES, LANES), F32),
            jax.ShapeDtypeStruct((16 * k.shape[0], LANES), F32),
            jax.ShapeDtypeStruct((16 * k.shape[0], LANES), F32),
        ],
        scratch_shapes=[
            pltpu.VMEM((16, LANES), F32), pltpu.VMEM(o.shape, BF16), pltpu.VMEM(lse.shape, F32), pltpu.VMEM(doc.shape, jnp.int32),
            pltpu.SemaphoreType.DMA((7,)), pltpu.SemaphoreType.DMA((80,)), pltpu.SemaphoreType.DMA((80,))],
        compiler_params=pltpu.CompilerParams(collective_id=0, has_side_effects=True, vmem_limit_bytes=8 * 2**20),
        name='gather',
    )(*[pltpu.with_memory_space_constraint(a, pltpu.HBM) for a in (q, do, o, lse, doc, k, v)])


def attend_body(scale, bnd, kg, vg, q, do, st, lim, zq, zk, zv, dq, dk, dv, which, p0, d0, p1, d1):
    n_keys, n_sub, n_lane = kg.shape[0], q.shape[0], q.shape[1]

    which[0] = bnd[0, 2]
    total = bnd[0, 1]
    for j in range(1, n_sub):
        total = total + bnd[j, 1]

    def tile_of(j, i):
        nominal = bnd[j, 0] + i * TK
        return nominal, pl.multiple_of(jnp.minimum(nominal, n_keys - TK), 16)

    def front(j, i, pr, dr):
        nominal, first = tile_of(j, i)
        rows = pl.ds(first, TK)
        kt, vt = kg[rows, :], vg[rows, :]
        index = lax.broadcasted_iota(jnp.int32, (TK, LANES), 0) + first

        def chunk(m):
            qc = q[j, 2 * m:2 * m + 2].reshape(256, LANES)
            dc = do[j, 2 * m:2 * m + 2].reshape(256, LANES)
            s = lax.dot_general(kt, qc, (((1,), (1,)), ((), ())), preferred_element_type=F32)
            dp = lax.dot_general(vt, dc, (((1,), (1,)), ((), ())), preferred_element_type=F32)
            for h in range(2):
                l = 2 * m + h
                cols = slice(LANES * h, LANES * h + LANES)
                lse, delta = st[l, pl.ds(j, 1), :], st[l, pl.ds(j + 8, 1), :]
                low, high = lim[l, pl.ds(j, 1), :], lim[l, pl.ds(j + 8, 1), :]
                e = jnp.exp2(s[:, cols] * (scale * LOG2E) - lse)
                p = jnp.where((index >= jnp.maximum(low, nominal)) & (index < high), e, 0.0)
                pr[l] = p.astype(BF16)
                dr[l] = (p * (dp[:, cols] - delta)).astype(BF16)

        return [functools.partial(chunk, m) for m in range(n_lane // 2)]

    def back(j, i, pr, dr):
        rows = pl.ds(tile_of(j, i)[1], TK)
        wide = lambda ref, ls: jnp.concatenate([ref[l] for l in ls], axis=1)

        def values():
            dv[rows, :] += jnp.dot(wide(pr, range(n_lane)), do[j].reshape(n_lane * LANES, LANES), preferred_element_type=F32)

        def keys():
            t = lax.dot_general(q[j].reshape(n_lane * LANES, LANES).T, wide(dr, range(n_lane)), (((1,), (1,)), ((), ())), preferred_element_type=F32)
            dk[rows, :] += t.T

        def queries():
            ktt = kg[rows, :].T
            for m in range(n_lane // 2):
                t = jnp.dot(ktt, wide(dr, (2 * m, 2 * m + 1)), preferred_element_type=F32)
                dq[j, 2 * m] += t[:, :LANES]
                dq[j, 2 * m + 1] += t[:, LANES:]

        return [values, keys, queries]

    def do_all(*parts):
        for part in parts:
            part()

    def beyond(j):
        nxt = n_sub - 1
        for jj in reversed(range(n_sub - 1)):
            nxt = jnp.where((jj > j) & (bnd[jj, 1] > 0), jj, nxt)
        return nxt

    def after(j, i):
        turn = i + 1 >= bnd[j, 1]
        return jnp.where(turn, beyond(j), j), jnp.where(turn, 0, i + 1)

    def step(now, have, want):
        nxt = after(*now)
        b, f = back(*now, *have), front(*nxt, *want)
        do_all(b[0], f[0], f[1], b[1], f[2], f[3], b[2])
        return nxt

    def four(_, now):
        for _ in range(2):
            now = step(step(now, (p0, d0), (p1, d1)), (p1, d1), (p0, d0))
        return now

    def one(_, now):
        nxt = after(*now)
        do_all(*back(*now, p0, d0), *front(*nxt, p0, d0))
        return nxt

    first = (beyond(jnp.int32(-1)), jnp.int32(0))
    do_all(*front(*first, p0, d0))
    more = total - 1
    now = lax.fori_loop(0, more // 4, four, first)
    now = lax.fori_loop(0, lax.rem(more, 4), one, now)
    do_all(*back(*now, p0, d0))


def attend(bnd, kg, vg, q, do, st, lim, zq, zk, zv):
    n_lane = q.shape[1]
    vm = pl.BlockSpec(memory_space=pltpu.VMEM)
    return pl.pallas_call(
        functools.partial(attend_body, LANES ** -0.5),
        in_specs=[pl.BlockSpec(memory_space=pltpu.SMEM)] + [vm] * 9,
        out_specs=[vm] * 3 + [pl.BlockSpec(memory_space=pltpu.SMEM)],
        out_shape=[jax.ShapeDtypeStruct(q.shape, F32), jax.ShapeDtypeStruct(kg.shape, F32),
                   jax.ShapeDtypeStruct(kg.shape, F32), jax.ShapeDtypeStruct((1,), jnp.int32)],
        input_output_aliases={7: 0, 8: 1, 9: 2},
        scratch_shapes=[pltpu.VMEM((n_lane, TK, LANES), BF16)] * 4,
        compiler_params=pltpu.CompilerParams(vmem_limit_bytes=16 * 2**20),
        name='attend',
    )(bnd, kg, vg, q, do, st, lim, zq, zk, zv)


class Split:
    def __init__(self, planes, keys):
        self.planes, self.keys, self.parts = planes, keys, 4 // planes
        self.rows = -(-keys // self.parts // 16) * 16 if planes == 1 else keys // self.parts
        self.low = self.rows // 2 if self.rows % 16 == 0 else self.rows // 16 * 8
        self.last = keys - self.rows
        self.half = {4: (2, keys, LANES), 2: (keys, LANES), 1: (2 * self.rows, LANES)}[planes]

    def slot(self, z):
        if self.planes == 4:
            return z, 0
        if self.planes == 2:
            return jnp.where(lax.rem(z, 3) == 0, 3, 2), jnp.where(z < 2, self.rows, 0)
        return 3, jnp.minimum(lax.rem(z + 1, 4) * self.rows, self.last)

    def rows_at(self, first):
        return pl.ds(first if isinstance(first, int) else pl.multiple_of(first, 8), self.rows)

    def keys_of(self, dk, z, ys):
        owner, first = self.slot(z)
        return dk.at[owner, ys, self.rows_at(first)]

    def values_of(self, dv, y, h):
        if self.planes == 4:
            return dv.at[pl.ds(2 * h, 2), y]
        if self.planes == 2:
            return dv.at[2 + h, y]
        return dv.at[3, y, pl.ds(h * (self.keys - 2 * self.rows), 2 * self.rows)]

    def value_slot(self, vs, z):
        owner, first = self.slot(z)
        if self.planes == 4:
            return vs.at[z // 2, lax.rem(z, 2)]
        if self.planes == 2:
            return vs.at[owner - 2, self.rows_at(first)]
        h = jnp.where(first >= 2 * self.rows, 1, 0)
        return vs.at[h, self.rows_at(first - h * (self.keys - 2 * self.rows))]

    def shares(self):
        if self.planes == 4:
            return []
        if self.planes == 2:
            return [(3, 1, 0), (2, 1, 1)]
        return [(3, h, (3 + h) % 4) for h in (1, 2, 3)]


class Ring:
    def __init__(self, w, place_, dev_up, dev_down, block, via, got):
        self.w, self.p, self.up, self.dn = w, place_, dev_up, dev_down
        self.block, self.via, self.got = block, via, got

    def first_up(self):
        self.fu = self.w.send(self.block(far(self.p), 0), self.via(0), self.up)

    def first_down(self):
        self.fd = self.w.send(self.block(far(self.p), 1), self.via(1), self.dn)

    def direct_up(self):
        self.du = self.w.send(self.block(up(self.p), 1), self.got(0, 1), self.up)

    def direct_down(self):
        self.dd = self.w.send(self.block(down(self.p), 0), self.got(1, 0), self.dn)

    def start(self):
        self.first_up()
        self.first_down()
        self.direct_up()
        self.direct_down()

    def middle(self):
        w, p = self.w, self.p
        self.fu.wait_recv()
        add(self.via(0), self.block(up(p), 0))
        self.mu = w.send(self.via(0), self.got(0, 0), self.up)
        self.fd.wait_recv()
        add(self.via(1), self.block(down(p), 1))
        self.md = w.send(self.via(1), self.got(1, 1), self.dn)

    def wait(self):
        for cp in (self.du, self.dd, self.mu, self.md):
            cp.wait_recv()


def add(dst, src):
    dst[...] = dst[...] + src[...]


def scatter_body(scale, sp, dq, dk, dv, oq, ok, ov, sq, sv, sg, k1v, k1g, ks, k2v, k2g, kr, v1v, v1g, vs, v2v, v2g, vr, ssem, rsem):
    z, y, x, c = place()
    xu, xd, sib = at(z, y, up(x), c), at(z, y, down(x), c), at(z, y, x, 1 - c)
    yu, yd = at(z, up(y), x, c), at(z, down(y), x, c)
    zu, zd = at(up(z), y, x, c), at(down(z), y, x, c)
    greet([xu, xd, sib, yu, yd, zu, zd] + ([at(far(z), y, x, c)] if sp.planes == 1 else []))
    w = Wire(ssem, rsem)
    n_sub = dq.shape[0]
    hn = n_sub // 2
    halves = (range(hn), range(hn, n_sub))
    order = ((far(x), halves[0]), (far(x), halves[1]), (up(x), range(n_sub)), (down(x), range(n_sub)), (x, range(n_sub)))
    cross = [w.send(dq.at[pl.ds(js[0], len(js)), xx * 2 + 1 - c], sq.at[xx, pl.ds(js[0], len(js))], sib) for xx, js in order]
    hy = (pl.ds(0, 2), pl.ds(2, 2))
    kone = Ring(w, z, zu, zd, lambda b, h: sp.keys_of(dk, b, hy[h]), lambda h: k1v.at[h], lambda s, h: k1g.at[s, hy[h]])
    vone = Ring(w, y, yu, yd, lambda b, h: sp.values_of(dv, b, h), lambda h: v1v.at[h], lambda s, h: v1g.at[s, h])
    kone.start()
    vone.start()
    hj = (pl.ds(0, hn), pl.ds(hn, n_sub - hn))
    qring = Ring(w, x, xu, xd, lambda b, h: sq.at[b, hj[h]], lambda h: sv.at[h], lambda s, h: sg.at[s, hj[h]])
    steps = (qring.first_up, qring.first_down, qring.direct_up, qring.direct_down, None)
    for cp, (xx, js), then in zip(cross, order, steps):
        cp.wait_recv()
        for j in js:
            sq[xx, j] = sq[xx, j] + dq[j, xx * 2 + c]
        if then is not None:
            then()
    kone.middle()
    vone.middle()
    qring.middle()
    nr = (sp.low, sp.rows - sp.low)
    hr = (pl.ds(0, nr[0]), pl.ds(nr[0], nr[1]))
    ktwo = Ring(w, y, yu, yd, lambda b, h: ks.at[b, hr[h]], lambda h: k2v.at[h, pl.ds(0, nr[h])], lambda s, h: k2g.at[s, hr[h]])
    vtwo = Ring(w, z, zu, zd, lambda b, h: sp.value_slot(vs, b).at[hr[h]], lambda h: v2v.at[h, pl.ds(0, nr[h])],
                lambda s, h: v2g.at[s, hr[h]])
    kone.wait()
    for b in range(4):
        ks[b] = sp.keys_of(dk, z, b)[...] + k1g[0, b] + k1g[1, b]
    ktwo.start()
    vone.wait()
    for h in range(2):
        vs[h] = sp.values_of(dv, y, h)[...] + v1g[0, h] + v1g[1, h]
    vtwo.start()
    ktwo.middle()
    vtwo.middle()
    ktwo.wait()
    kr[0] = (ks[y] + k2g[0] + k2g[1]) * scale
    home = []

    def go_home(buf, out):
        for owner, h, taker in sp.shares():
            cp = w.copy(buf.at[0], buf.at[h], at(owner, y, x, c))
            home.append((owner, h, taker, buf, out, cp))
            pl.when(z == taker)(cp.start)

    go_home(kr, ok)
    vtwo.wait()
    vr[0] = sp.value_slot(vs, z)[...] + v2g[0] + v2g[1]
    go_home(vr, ov)
    qring.wait()
    for j in range(n_sub):
        oq[j] = ((sq[x, j] + sg[0, j] + sg[1, j]).T * scale).astype(BF16)
    if sp.planes == 4:
        ok[...] = kr[0]
        ov[...] = vr[0]
    else:
        @pl.when(z < 4 - sp.planes)
        def _():
            ok[...] = jnp.zeros_like(ok)
            ov[...] = jnp.zeros_like(ov)

        @pl.when(z >= 4 - sp.planes)
        def _():
            ok[0:sp.rows, :] = kr[0]
            ov[0:sp.rows, :] = vr[0]

        for owner, h, taker, buf, out, cp in home:
            first = min(h * sp.rows, sp.last)

            @pl.when(z == owner)
            def _():
                cp.wait_recv()
                out[first:first + sp.rows, :] = buf[h]

            pl.when(z == taker)(cp.wait_send)
    w.finish()


def scatter(planes, dq, dk, dv):
    n_sub = dq.shape[0]
    sp = Split(planes, dk.shape[2])
    rows = sp.rows
    vm = pl.BlockSpec(memory_space=pltpu.VMEM)
    two = [
        pltpu.VMEM((2, sp.low + sp.low % 16, LANES), F32),
        pltpu.VMEM((2, rows, LANES), F32),
        pltpu.VMEM((sp.parts, rows, LANES), F32),
    ]
    return pl.pallas_call(
        functools.partial(scatter_body, LANES ** -0.5, sp),
        in_specs=[vm] * 3,
        out_specs=[vm] * 3,
        out_shape=[
            jax.ShapeDtypeStruct((n_sub, LANES, LANES), BF16),
            jax.ShapeDtypeStruct((sp.keys, LANES), F32),
            jax.ShapeDtypeStruct((sp.keys, LANES), F32),
        ],
        scratch_shapes=[
            pltpu.VMEM((4, n_sub, LANES, LANES), F32),
            pltpu.VMEM((2, n_sub // 2, LANES, LANES), F32),
            pltpu.VMEM((2, n_sub, LANES, LANES), F32),
            pltpu.VMEM((2, 2, rows, LANES), F32), pltpu.VMEM((2, 4, rows, LANES), F32), pltpu.VMEM((4, rows, LANES), F32), *two,
            pltpu.VMEM((2,) + sp.half, F32), pltpu.VMEM((2, 2) + sp.half, F32), pltpu.VMEM((2,) + sp.half, F32), *two,
            pltpu.SemaphoreType.DMA((44,)), pltpu.SemaphoreType.DMA((44,))],
        compiler_params=pltpu.CompilerParams(collective_id=planes, has_side_effects=True, vmem_limit_bytes=20 * 2**20),
        name='scatter',
    )(dq, dk, dv)


def store_body(a, b, c, oa, ob, oc, sem):
    copies = [pltpu.make_async_copy(src, dst, sem.at[i]) for i, (src, dst) in enumerate(((a, oa), (b, ob), (c, oc)))]
    for cp in copies:
        cp.start()
    for cp in copies:
        cp.wait()


def store(*arrays):
    return pl.pallas_call(
        store_body,
        in_specs=[pl.BlockSpec(memory_space=pltpu.VMEM)] * 3,
        out_specs=[pl.BlockSpec(memory_space=pltpu.HBM)] * 3,
        out_shape=[jax.ShapeDtypeStruct(a.shape, a.dtype) for a in arrays],
        scratch_shapes=[pltpu.SemaphoreType.DMA((3,))],
        name='store',
    )(*arrays)


def solution(mesh):
    q_spec = P(None, 'cp', 'tp', None)
    lse_spec = P(None, 'cp', 'tp')
    kv_spec = P('cp', 'tp', None)

    def local_backward(query, out_act, out_grad, row_lse, key_act, value_act, doc_ids):
        n_sub, local_len, n_heads, head_dim = query.shape
        keys_local = key_act.shape[0]
        rows = local_len * n_heads
        q = query.reshape(n_sub, rows, head_dim)
        do = out_grad.reshape(n_sub, rows, head_dim)
        o = out_act.reshape(n_sub, rows, head_dim)
        doc = doc_ids.reshape(-1, LANES)
        k, v = key_act.reshape(keys_local, head_dim), value_act.reshape(keys_local, head_dim)
        qg, dg, sg, kg, vg, lim, bnd, zq, zk, zv = gather(local_len * LANES, q, do, o, row_lse, doc, k, v)
        flat = (16 * keys_local, head_dim)
        dq, dk, dv, which = attend(bnd, kg.reshape(flat), vg.reshape(flat), qg, dg, sg, lim, zq, zk, zv)
        blocks = (4, 4, keys_local, head_dim)
        oq, ok, ov = lax.switch(which[0], [functools.partial(scatter, n) for n in (1, 2, 4)], dq, dk.reshape(blocks), dv.reshape(blocks))
        oq, ok, ov = store(oq, ok, ov)
        return (oq.reshape(query.shape), ok.reshape(keys_local, 1, head_dim), ov.reshape(keys_local, 1, head_dim))

    return jax.shard_map(local_backward, mesh=mesh, in_specs=(q_spec, q_spec, q_spec, lse_spec, kv_spec, kv_spec, P()), out_specs=(q_spec, kv_spec, kv_spec), check_vma=False)
```

```python
import functools

import jax
import jax.numpy as jnp
from jax import lax
from jax.experimental import pallas as pl
from jax.experimental.pallas import tpu as pltpu
from jax.sharding import PartitionSpec as P

MESH = pl.DeviceIdType.MESH
TK = 256
LANES = 128
LOG2E = 1.4426950408889634
F32, BF16 = jnp.float32, jnp.bfloat16


def place():
    me = lax.axis_index('cp')
    return me // 32, lax.rem(me // 8, 4), lax.rem(me // 2, 4), lax.rem(me, 2)


def at(z, y, x, c):
    return ((z * 4 + y) * 4 + x) * 2 + c


def up(v):
    return lax.rem(v + 1, 4)


def down(v):
    return lax.rem(v + 3, 4)


def far(v):
    return lax.rem(v + 2, 4)


class Wire:
    def __init__(self, ssem, rsem):
        self.ssem, self.rsem, self.n, self.sent = ssem, rsem, 0, []

    def copy(self, src, dst, dev):
        cp = pltpu.make_async_remote_copy(
            src_ref=src, dst_ref=dst, send_sem=self.ssem, recv_sem=self.rsem.at[self.n],
            device_id={'cp': dev}, device_id_type=MESH)
        self.n += 1
        return cp

    def send(self, src, dst, dev):
        cp = self.copy(src, dst, dev)
        cp.start()
        self.sent.append(cp)
        return cp

    def finish(self):
        for cp in self.sent:
            cp.wait_send()


def greet(partners):
    barrier = pltpu.get_barrier_semaphore()
    for dev in partners:
        pl.semaphore_signal(barrier, inc=1, device_id={'cp': dev}, device_id_type=MESH)
    pl.semaphore_wait(barrier, len(partners))


def row_stats(do, o, lse, st):
    st[...] = jnp.zeros_like(st)
    tok = lax.broadcasted_iota(jnp.int32, (8, LANES), 0)
    lane = lax.broadcasted_iota(jnp.int32, (8, LANES), 1)
    for j in range(do.shape[0]):
        wide = jnp.concatenate([lse[j]] * 8, axis=1)
        st[j:j + 1, :] = jnp.sum(jnp.where((lane >> 4) == tok, wide, 0.0), axis=0, keepdims=True) * LOG2E
        prod = do[j].astype(F32) * o[j].astype(F32)
        st[8 + j:9 + j, :] = jnp.sum(prod.T, axis=0, keepdims=True)


def limits(doc, n_sub, sub_len, keys_local, lim, bnd):
    z, y, x, c = place()
    grp, lane = z * 4 + y, x * 2 + c
    n_pos = doc.shape[0] * LANES
    sub_start = n_pos - n_sub * sub_len
    period = 8 * keys_local

    def flat(pos):
        b = jnp.zeros_like(pos)
        for i in range(1, n_pos // period):
            b += jnp.where(pos >= i * period, 1, 0)
        return b * keys_local + jnp.clip(pos - b * period - lane * keys_local, 0, keys_local)

    sub = lax.broadcasted_iota(jnp.int32, (8, LANES), 0)
    tok = lax.broadcasted_iota(jnp.int32, (8, LANES), 1)
    docs = jnp.zeros((8, LANES), jnp.int32)
    for j in range(n_sub):
        row = doc[pl.ds((sub_start + j * sub_len) // LANES + grp // 2, 1), :]
        docs = jnp.where(sub == j, row, docs)
    docs = jnp.where(lax.rem(grp, 2) == 1, pltpu.roll(docs, 64, 1), docs)
    before = jnp.zeros((8, LANES), jnp.int32)
    for j in range(n_sub):
        head = docs[j:j + 1, 0:1]
        count = jnp.zeros((8, LANES), jnp.int32)
        for r in range(0, doc.shape[0], 8):
            count += jnp.where(doc[r:r + 8, :] < head, 1, 0)
        count = jnp.sum(jnp.sum(count.astype(F32), axis=0, keepdims=True), axis=1, keepdims=True)
        before = jnp.where(sub == j, count.astype(jnp.int32), before)
    base = sub_start + sub * sub_len + grp * 64
    pos = base + tok
    begin = jnp.where((tok > 0) & (docs != pltpu.roll(docs, 1, 1)), pos, before)
    for shift in (1, 2, 4, 8, 16, 32):
        begin = jnp.maximum(begin, jnp.where(tok >= shift, pltpu.roll(begin, shift, 1), 0))
    pick = jnp.where(
        lax.broadcasted_iota(jnp.int32, (LANES, 1024), 0) == lax.broadcasted_iota(jnp.int32, (LANES, 1024), 1) >> 4, 1.0, 0.0)
    for first, value in ((0, flat(begin)), (8, flat(pos + 1))):
        wide = jnp.dot(value.astype(F32), pick, precision=lax.Precision.HIGHEST, preferred_element_type=F32)
        for l in range(8):
            lim[l, first:first + 8, :] = wide[:, LANES * l:LANES * l + LANES].astype(jnp.int32)
    start = flat(before) & -16
    tiles = jnp.maximum((flat(base + 64) - start + (TK - 1)) // TK, jnp.where(sub == 0, 1, 0))
    first = doc[pl.ds(sub_start // LANES, 1), :][:, 0:1]
    edge = lambda planes: doc[pl.ds((n_pos - planes * n_pos // 4 - 1) // LANES, 1), :][:, 127:LANES] >= first
    which = jnp.where(edge(1), jnp.where(edge(2), 2, 1), 0)
    bnd[...] = jnp.where(tok == 0, start, jnp.where(tok == 1, tiles, which))


def clear(zq, zk, zv):
    def rows(i, _):
        for r in range(4):
            at_ = pl.ds(pl.multiple_of((i * 4 + r) * 16, 16), 16)
            zk[at_, :] = jnp.zeros((16, LANES), F32)
            zv[at_, :] = jnp.zeros((16, LANES), F32)
        return 0

    lax.fori_loop(0, zk.shape[0] // 64, rows, 0)

    def block(i, _):
        zq[i // 8, lax.rem(i, 8)] = jnp.zeros((LANES, LANES), F32)
        return 0

    lax.fori_loop(0, zq.shape[0] * 8, block, 0)


def gather_body(sub_len, q, do, o, lse, doc, k, v, qg, dg, sg, kg, vg, lim, bnd, zq, zk, zv, st, ov, lv, cv, lsem, ssem, rsem):
    z, y, x, c = place()
    xu, xd, sib = at(z, y, up(x), c), at(z, y, down(x), c), at(z, y, x, 1 - c)
    yu, yd = at(z, up(y), x, c), at(z, down(y), x, c)
    zu, zd = at(up(z), y, x, c), at(down(z), y, x, c)
    lane = lambda xx: xx * 2 + c
    own = lane(x)
    loads = []
    for i, (src, dst) in enumerate((
            (k, kg.at[z, y]), (v, vg.at[z, y]), (q, qg.at[:, own]), (do, dg.at[:, own]), (o, ov), (lse, lv), (doc, cv))):
        loads.append(pltpu.make_async_copy(src, dst, lsem.at[i]))
        loads[i].start()
    greet([xu, xd, sib, yu, yd, zu, zd])
    w = Wire(ssem, rsem)
    ha, hb = slice(0, 3), slice(3, 6)
    pairs = (qg, dg)
    k, v = kg.at[z, y], vg.at[z, y]
    ru_a, rd_b, ru_b, rd_a = [], [], [], []
    loads[0].wait()
    k_u = w.send(k, k, yu)
    k_d = w.send(k, k, yd)
    loads[1].wait()
    v_u = w.send(v, v, zu)
    v_d = w.send(v, v, zd)
    for i, g in enumerate(pairs):
        loads[2 + i].wait()
        ru_a.append(w.send(g.at[ha, own], g.at[ha, own], xu))
        rd_b.append(w.send(g.at[hb, own], g.at[hb, own], xd))
    for g in pairs:
        ru_b.append(w.send(g.at[hb, own], g.at[hb, own], xu))
        rd_a.append(w.send(g.at[ha, own], g.at[ha, own], xd))
    sibs = [w.send(g.at[:, own], g.at[:, own], sib) for g in pairs]
    kz, vy = {}, {}
    kz['u', 0] = w.send(k, k, zu)
    kz['d', 0] = w.send(k, k, zd)
    vy['u', 0] = w.send(v, v, yu)
    vy['d', 0] = w.send(v, v, yd)
    for cp in loads[4:]:
        cp.wait()
    row_stats(dg.at[:, own], ov, lv, st)
    sg[own] = st[...]
    limits(cv, qg.shape[0], sub_len, kg.shape[2], lim, bnd)
    su = w.send(st, sg.at[own], xu)
    sd = w.send(st, sg.at[own], xd)
    sibs.append(w.send(st, sg.at[own], sib))
    lo_rows, hi_rows = pl.ds(0, 160), pl.ds(160, 144)
    clear(zq, zk, zv)
    k_u.wait_recv()
    kf_a = w.send(kg.at[z, down(y), lo_rows], kg.at[z, down(y), lo_rows], yu)
    k_d.wait_recv()
    kf_b = w.send(kg.at[z, up(y), hi_rows], kg.at[z, up(y), hi_rows], yd)
    v_u.wait_recv()
    vf_a = w.send(vg.at[down(z), y, lo_rows], vg.at[down(z), y, lo_rows], zu)
    v_d.wait_recv()
    vf_b = w.send(vg.at[up(z), y, hi_rows], vg.at[up(z), y, hi_rows], zd)
    for r, yy, zz in ((3, down(y), down(z)), (1, up(y), up(z))):
        for name, dev in (('u', zu), ('d', zd)):
            kz[name, r] = w.send(kg.at[z, yy], kg.at[z, yy], dev)
        for name, dev in (('u', yu), ('d', yd)):
            vy[name, r] = w.send(vg.at[zz, y], vg.at[zz, y], dev)
    kf_a.wait_recv()
    kf_b.wait_recv()
    for name, dev in (('u', zu), ('d', zd)):
        kz[name, 2] = w.send(kg.at[z, far(y)], kg.at[z, far(y)], dev)
    vf_a.wait_recv()
    vf_b.wait_recv()
    for name, dev in (('u', yu), ('d', yd)):
        vy[name, 2] = w.send(vg.at[far(z), y], vg.at[far(z), y], dev)
    ld, lu, lf = lane(down(x)), lane(up(x)), lane(far(x))
    fu, fd = [], []
    for i, g in enumerate(pairs):
        ru_a[i].wait_recv()
        fu.append(w.send(g.at[ha, ld], g.at[ha, ld], xu))
        rd_b[i].wait_recv()
        fd.append(w.send(g.at[hb, lu], g.at[hb, lu], xd))
    su.wait_recv()
    sf = w.send(sg.at[ld], sg.at[ld], xu)
    sd.wait_recv()
    for i, g in enumerate(pairs):
        sibs.append(w.send(g.at[ha, ld], g.at[ha, ld], sib))
        sibs.append(w.send(g.at[hb, lu], g.at[hb, lu], sib))
    sibs.append(w.send(sg.at[ld], sg.at[ld], sib))
    sibs.append(w.send(sg.at[lu], sg.at[lu], sib))
    slot = lambda r, v_: lax.rem(v_ + r, 4)
    kzf, vyf = [], []
    for r in (0, 3, 1, 2):
        if r == 2:
            for i, g in enumerate(pairs):
                ru_b[i].wait_recv()
                sibs.append(w.send(g.at[hb, ld], g.at[hb, ld], sib))
                rd_a[i].wait_recv()
                sibs.append(w.send(g.at[ha, lu], g.at[ha, lu], sib))
        yy, zz = slot(r, y), slot(r, z)
        kz['u', r].wait_recv()
        if r in (0, 1):
            kzf.append(w.send(kg.at[down(z), yy], kg.at[down(z), yy], zu))
        kz['d', r].wait_recv()
        if r in (2, 3):
            kzf.append(w.send(kg.at[up(z), yy], kg.at[up(z), yy], zd))
        vy['u', r].wait_recv()
        if r in (0, 1):
            vyf.append(w.send(vg.at[zz, down(y)], vg.at[zz, down(y)], yu))
        vy['d', r].wait_recv()
        if r in (2, 3):
            vyf.append(w.send(vg.at[zz, up(y)], vg.at[zz, up(y)], yd))
    sf.wait_recv()
    sibs.append(w.send(sg.at[lf], sg.at[lf], sib))
    for i, g in enumerate(pairs):
        fu[i].wait_recv()
        sibs.append(w.send(g.at[ha, lf], g.at[ha, lf], sib))
        fd[i].wait_recv()
        sibs.append(w.send(g.at[hb, lf], g.at[hb, lf], sib))
    for cp in kzf + vyf + sibs:
        cp.wait_recv()
    w.finish()


def gather(sub_len, q, do, o, lse, doc, k, v):
    n_sub = q.shape[0]
    vm = pl.BlockSpec(memory_space=pltpu.VMEM)
    return pl.pallas_call(
        functools.partial(gather_body, sub_len),
        in_specs=[pl.BlockSpec(memory_space=pltpu.HBM)] * 7,
        out_specs=[vm] * 10,
        out_shape=[
            jax.ShapeDtypeStruct((n_sub, 8, LANES, LANES), BF16),
            jax.ShapeDtypeStruct((n_sub, 8, LANES, LANES), BF16),
            jax.ShapeDtypeStruct((8, 16, LANES), F32),
            jax.ShapeDtypeStruct((4, 4) + k.shape, BF16),
            jax.ShapeDtypeStruct((4, 4) + k.shape, BF16),
            jax.ShapeDtypeStruct((8, 16, LANES), jnp.int32),
            jax.ShapeDtypeStruct((8, LANES), jnp.int32),
            jax.ShapeDtypeStruct((n_sub, 8, LANES, LANES), F32),
            jax.ShapeDtypeStruct((16 * k.shape[0], LANES), F32),
            jax.ShapeDtypeStruct((16 * k.shape[0], LANES), F32),
        ],
        scratch_shapes=[
            pltpu.VMEM((16, LANES), F32), pltpu.VMEM(o.shape, BF16), pltpu.VMEM(lse.shape, F32), pltpu.VMEM(doc.shape, jnp.int32),
            pltpu.SemaphoreType.DMA((7,)), pltpu.SemaphoreType.DMA(()), pltpu.SemaphoreType.DMA((65,))],
        compiler_params=pltpu.CompilerParams(collective_id=0, has_side_effects=True, vmem_limit_bytes=8 * 2**20),
        name='gather',
    )(*[pltpu.with_memory_space_constraint(a, pltpu.HBM) for a in (q, do, o, lse, doc, k, v)])


def attend_body(scale, bnd, kg, vg, q, do, st, lim, zq, zk, zv, dq, dk, dv, which, p0, d0, p1, d1):
    n_keys, n_sub, n_lane = kg.shape[0], q.shape[0], q.shape[1]

    which[0] = bnd[0, 2]
    total = bnd[0, 1]
    for j in range(1, n_sub):
        total = total + bnd[j, 1]

    def tile_of(j, i):
        nominal = bnd[j, 0] + i * TK
        return nominal, pl.multiple_of(jnp.minimum(nominal, n_keys - TK), 16)

    def front(j, i, pr, dr):
        nominal, first = tile_of(j, i)
        rows = pl.ds(first, TK)
        kt, vt = kg[rows, :], vg[rows, :]
        index = lax.broadcasted_iota(jnp.int32, (TK, LANES), 0) + first

        def chunk(m):
            qc = q[j, 2 * m:2 * m + 2].reshape(256, LANES)
            dc = do[j, 2 * m:2 * m + 2].reshape(256, LANES)
            s = lax.dot_general(kt, qc, (((1,), (1,)), ((), ())), preferred_element_type=F32)
            dp = lax.dot_general(vt, dc, (((1,), (1,)), ((), ())), preferred_element_type=F32)
            for h in range(2):
                l = 2 * m + h
                cols = slice(LANES * h, LANES * h + LANES)
                lse, delta = st[l, pl.ds(j, 1), :], st[l, pl.ds(j + 8, 1), :]
                low, high = lim[l, pl.ds(j, 1), :], lim[l, pl.ds(j + 8, 1), :]
                e = jnp.exp2(s[:, cols] * (scale * LOG2E) - lse)
                p = jnp.where((index >= jnp.maximum(low, nominal)) & (index < high), e, 0.0)
                pr[l] = p.astype(BF16)
                dr[l] = (p * (dp[:, cols] - delta)).astype(BF16)

        return [functools.partial(chunk, m) for m in range(n_lane // 2)]

    def back(j, i, pr, dr):
        rows = pl.ds(tile_of(j, i)[1], TK)
        wide = lambda ref, ls: jnp.concatenate([ref[l] for l in ls], axis=1)

        def values():
            dv[rows, :] += jnp.dot(wide(pr, range(n_lane)), do[j].reshape(n_lane * LANES, LANES), preferred_element_type=F32)

        def keys():
            t = lax.dot_general(q[j].reshape(n_lane * LANES, LANES).T, wide(dr, range(n_lane)), (((1,), (1,)), ((), ())), preferred_element_type=F32)
            dk[rows, :] += t.T

        def queries():
            ktt = kg[rows, :].T
            for m in range(n_lane // 2):
                t = jnp.dot(ktt, wide(dr, (2 * m, 2 * m + 1)), preferred_element_type=F32)
                dq[j, 2 * m] += t[:, :LANES]
                dq[j, 2 * m + 1] += t[:, LANES:]

        return [values, keys, queries]

    def do_all(*parts):
        for part in parts:
            part()

    def beyond(j):
        nxt = n_sub - 1
        for jj in reversed(range(n_sub - 1)):
            nxt = jnp.where((jj > j) & (bnd[jj, 1] > 0), jj, nxt)
        return nxt

    def after(j, i):
        turn = i + 1 >= bnd[j, 1]
        return jnp.where(turn, beyond(j), j), jnp.where(turn, 0, i + 1)

    def step(now, have, want):
        nxt = after(*now)
        b, f = back(*now, *have), front(*nxt, *want)
        do_all(b[0], f[0], f[1], b[1], f[2], f[3], b[2])
        return nxt

    def four(_, now):
        for _ in range(2):
            now = step(step(now, (p0, d0), (p1, d1)), (p1, d1), (p0, d0))
        return now

    def one(_, now):
        nxt = after(*now)
        do_all(*back(*now, p0, d0), *front(*nxt, p0, d0))
        return nxt

    first = (beyond(jnp.int32(-1)), jnp.int32(0))
    do_all(*front(*first, p0, d0))
    more = total - 1
    now = lax.fori_loop(0, more // 4, four, first)
    now = lax.fori_loop(0, lax.rem(more, 4), one, now)
    do_all(*back(*now, p0, d0))


def attend(bnd, kg, vg, q, do, st, lim, zq, zk, zv):
    n_lane = q.shape[1]
    vm = pl.BlockSpec(memory_space=pltpu.VMEM)
    return pl.pallas_call(
        functools.partial(attend_body, LANES ** -0.5),
        in_specs=[pl.BlockSpec(memory_space=pltpu.SMEM)] + [vm] * 9,
        out_specs=[vm] * 3 + [pl.BlockSpec(memory_space=pltpu.SMEM)],
        out_shape=[jax.ShapeDtypeStruct(q.shape, F32), jax.ShapeDtypeStruct(kg.shape, F32),
                   jax.ShapeDtypeStruct(kg.shape, F32), jax.ShapeDtypeStruct((1,), jnp.int32)],
        input_output_aliases={7: 0, 8: 1, 9: 2},
        scratch_shapes=[pltpu.VMEM((n_lane, TK, LANES), BF16)] * 4,
        compiler_params=pltpu.CompilerParams(vmem_limit_bytes=16 * 2**20),
        name='attend',
    )(bnd, kg, vg, q, do, st, lim, zq, zk, zv)


class Split:
    def __init__(self, planes, keys):
        self.planes, self.keys, self.parts = planes, keys, 4 // planes
        self.rows = -(-keys // self.parts // 16) * 16 if planes == 1 else keys // self.parts
        self.low = self.rows // 2 if self.rows % 16 == 0 else self.rows // 16 * 8
        self.last = keys - self.rows
        self.half = {4: (2, keys, LANES), 2: (keys, LANES), 1: (2 * self.rows, LANES)}[planes]

    def slot(self, z):
        if self.planes == 4:
            return z, 0
        if self.planes == 2:
            return jnp.where(lax.rem(z, 3) == 0, 3, 2), jnp.where(z < 2, self.rows, 0)
        return 3, jnp.minimum(lax.rem(z + 1, 4) * self.rows, self.last)

    def rows_at(self, first):
        return pl.ds(first if isinstance(first, int) else pl.multiple_of(first, 8), self.rows)

    def keys_of(self, dk, z, ys):
        owner, first = self.slot(z)
        return dk.at[owner, ys, self.rows_at(first)]

    def values_of(self, dv, y, h):
        if self.planes == 4:
            return dv.at[pl.ds(2 * h, 2), y]
        if self.planes == 2:
            return dv.at[2 + h, y]
        return dv.at[3, y, pl.ds(h * (self.keys - 2 * self.rows), 2 * self.rows)]

    def value_slot(self, vs, z):
        owner, first = self.slot(z)
        if self.planes == 4:
            return vs.at[z // 2, lax.rem(z, 2)]
        if self.planes == 2:
            return vs.at[owner - 2, self.rows_at(first)]
        h = jnp.where(first >= 2 * self.rows, 1, 0)
        return vs.at[h, self.rows_at(first - h * (self.keys - 2 * self.rows))]

    def shares(self):
        if self.planes == 4:
            return []
        if self.planes == 2:
            return [(3, 1, 0), (2, 1, 1)]
        return [(3, h, (3 + h) % 4) for h in (1, 2, 3)]


class Ring:
    def __init__(self, w, place_, dev_up, dev_down, block, via, got):
        self.w, self.p, self.up, self.dn = w, place_, dev_up, dev_down
        self.block, self.via, self.got = block, via, got

    def first_up(self):
        self.fu = self.w.send(self.block(far(self.p), 0), self.via(0), self.up)

    def first_down(self):
        self.fd = self.w.send(self.block(far(self.p), 1), self.via(1), self.dn)

    def direct_up(self):
        self.du = self.w.send(self.block(up(self.p), 1), self.got(0, 1), self.up)

    def direct_down(self):
        self.dd = self.w.send(self.block(down(self.p), 0), self.got(1, 0), self.dn)

    def start(self):
        self.first_up()
        self.first_down()
        self.direct_up()
        self.direct_down()

    def middle(self):
        w, p = self.w, self.p
        self.fu.wait_recv()
        add(self.via(0), self.block(up(p), 0))
        self.mu = w.send(self.via(0), self.got(0, 0), self.up)
        self.fd.wait_recv()
        add(self.via(1), self.block(down(p), 1))
        self.md = w.send(self.via(1), self.got(1, 1), self.dn)

    def wait(self):
        for cp in (self.du, self.dd, self.mu, self.md):
            cp.wait_recv()


def add(dst, src):
    dst[...] = dst[...] + src[...]


def scatter_body(scale, sp, dq, dk, dv, oq, ok, ov, sq, sv, sg, k1v, k1g, ks, k2v, k2g, kr, v1v, v1g, vs, v2v, v2g, vr, ssem, rsem):
    z, y, x, c = place()
    xu, xd, sib = at(z, y, up(x), c), at(z, y, down(x), c), at(z, y, x, 1 - c)
    yu, yd = at(z, up(y), x, c), at(z, down(y), x, c)
    zu, zd = at(up(z), y, x, c), at(down(z), y, x, c)
    greet([xu, xd, sib, yu, yd, zu, zd] + ([at(far(z), y, x, c)] if sp.planes == 1 else []))
    w = Wire(ssem, rsem)
    n_sub = dq.shape[0]
    hn = n_sub // 2
    halves = (range(hn), range(hn, n_sub))
    order = ((far(x), halves[0]), (far(x), halves[1]), (up(x), range(n_sub)), (down(x), range(n_sub)), (x, range(n_sub)))
    cross = [w.send(dq.at[pl.ds(js[0], len(js)), xx * 2 + 1 - c], sq.at[xx, pl.ds(js[0], len(js))], sib) for xx, js in order]
    hy = (pl.ds(0, 2), pl.ds(2, 2))
    kone = Ring(w, z, zu, zd, lambda b, h: sp.keys_of(dk, b, hy[h]), lambda h: k1v.at[h], lambda s, h: k1g.at[s, hy[h]])
    vone = Ring(w, y, yu, yd, lambda b, h: sp.values_of(dv, b, h), lambda h: v1v.at[h], lambda s, h: v1g.at[s, h])
    kone.start()
    vone.start()
    hj = (pl.ds(0, hn), pl.ds(hn, n_sub - hn))
    qring = Ring(w, x, xu, xd, lambda b, h: sq.at[b, hj[h]], lambda h: sv.at[h], lambda s, h: sg.at[s, hj[h]])
    steps = (qring.first_up, qring.first_down, qring.direct_up, qring.direct_down, None)
    for cp, (xx, js), then in zip(cross, order, steps):
        cp.wait_recv()
        for j in js:
            sq[xx, j] = sq[xx, j] + dq[j, xx * 2 + c]
        if then is not None:
            then()
    kone.middle()
    vone.middle()
    qring.middle()
    nr = (sp.low, sp.rows - sp.low)
    hr = (pl.ds(0, nr[0]), pl.ds(nr[0], nr[1]))
    ktwo = Ring(w, y, yu, yd, lambda b, h: ks.at[b, hr[h]], lambda h: k2v.at[h, pl.ds(0, nr[h])], lambda s, h: k2g.at[s, hr[h]])
    vtwo = Ring(w, z, zu, zd, lambda b, h: sp.value_slot(vs, b).at[hr[h]], lambda h: v2v.at[h, pl.ds(0, nr[h])],
                lambda s, h: v2g.at[s, hr[h]])
    kone.wait()
    for b in range(4):
        ks[b] = sp.keys_of(dk, z, b)[...] + k1g[0, b] + k1g[1, b]
    ktwo.start()
    vone.wait()
    for h in range(2):
        vs[h] = sp.values_of(dv, y, h)[...] + v1g[0, h] + v1g[1, h]
    vtwo.start()
    ktwo.middle()
    vtwo.middle()
    ktwo.wait()
    kr[0] = (ks[y] + k2g[0] + k2g[1]) * scale
    home = []

    def go_home(buf, out):
        for owner, h, taker in sp.shares():
            cp = w.copy(buf.at[0], buf.at[h], at(owner, y, x, c))
            home.append((owner, h, taker, buf, out, cp))
            pl.when(z == taker)(cp.start)

    go_home(kr, ok)
    vtwo.wait()
    vr[0] = sp.value_slot(vs, z)[...] + v2g[0] + v2g[1]
    go_home(vr, ov)
    qring.wait()
    for j in range(n_sub):
        oq[j] = ((sq[x, j] + sg[0, j] + sg[1, j]).T * scale).astype(BF16)
    if sp.planes == 4:
        ok[...] = kr[0]
        ov[...] = vr[0]
    else:
        @pl.when(z < 4 - sp.planes)
        def _():
            ok[...] = jnp.zeros_like(ok)
            ov[...] = jnp.zeros_like(ov)

        @pl.when(z >= 4 - sp.planes)
        def _():
            ok[0:sp.rows, :] = kr[0]
            ov[0:sp.rows, :] = vr[0]

        for owner, h, taker, buf, out, cp in home:
            first = min(h * sp.rows, sp.last)

            @pl.when(z == owner)
            def _():
                cp.wait_recv()
                out[first:first + sp.rows, :] = buf[h]

            pl.when(z == taker)(cp.wait_send)
    w.finish()


def scatter(planes, dq, dk, dv):
    n_sub = dq.shape[0]
    sp = Split(planes, dk.shape[2])
    rows = sp.rows
    vm = pl.BlockSpec(memory_space=pltpu.VMEM)
    two = [
        pltpu.VMEM((2, sp.low + sp.low % 16, LANES), F32),
        pltpu.VMEM((2, rows, LANES), F32),
        pltpu.VMEM((sp.parts, rows, LANES), F32),
    ]
    return pl.pallas_call(
        functools.partial(scatter_body, LANES ** -0.5, sp),
        in_specs=[vm] * 3,
        out_specs=[vm] * 3,
        out_shape=[
            jax.ShapeDtypeStruct((n_sub, LANES, LANES), BF16),
            jax.ShapeDtypeStruct((sp.keys, LANES), F32),
            jax.ShapeDtypeStruct((sp.keys, LANES), F32),
        ],
        scratch_shapes=[
            pltpu.VMEM((4, n_sub, LANES, LANES), F32),
            pltpu.VMEM((2, n_sub // 2, LANES, LANES), F32),
            pltpu.VMEM((2, n_sub, LANES, LANES), F32),
            pltpu.VMEM((2, 2, rows, LANES), F32), pltpu.VMEM((2, 4, rows, LANES), F32), pltpu.VMEM((4, rows, LANES), F32), *two,
            pltpu.VMEM((2,) + sp.half, F32), pltpu.VMEM((2, 2) + sp.half, F32), pltpu.VMEM((2,) + sp.half, F32), *two,
            pltpu.SemaphoreType.DMA(()), pltpu.SemaphoreType.DMA(({1: 41, 2: 39, 4: 35}[planes],))],
        compiler_params=pltpu.CompilerParams(collective_id=planes, has_side_effects=True, vmem_limit_bytes=20 * 2**20),
        name='scatter',
    )(dq, dk, dv)


def store_body(a, b, c, oa, ob, oc, sem):
    copies = [pltpu.make_async_copy(src, dst, sem.at[i]) for i, (src, dst) in enumerate(((a, oa), (b, ob), (c, oc)))]
    for cp in copies:
        cp.start()
    for cp in copies:
        cp.wait()


def store(*arrays):
    return pl.pallas_call(
        store_body,
        in_specs=[pl.BlockSpec(memory_space=pltpu.VMEM)] * 3,
        out_specs=[pl.BlockSpec(memory_space=pltpu.HBM)] * 3,
        out_shape=[jax.ShapeDtypeStruct(a.shape, a.dtype) for a in arrays],
        scratch_shapes=[pltpu.SemaphoreType.DMA((3,))],
        name='store',
    )(*arrays)


def solution(mesh):
    q_spec = P(None, 'cp', 'tp', None)
    lse_spec = P(None, 'cp', 'tp')
    kv_spec = P('cp', 'tp', None)

    def local_backward(query, out_act, out_grad, row_lse, key_act, value_act, doc_ids):
        n_sub, local_len, n_heads, head_dim = query.shape
        keys_local = key_act.shape[0]
        rows = local_len * n_heads
        q = query.reshape(n_sub, rows, head_dim)
        do = out_grad.reshape(n_sub, rows, head_dim)
        o = out_act.reshape(n_sub, rows, head_dim)
        doc = doc_ids.reshape(-1, LANES)
        k, v = key_act.reshape(keys_local, head_dim), value_act.reshape(keys_local, head_dim)
        qg, dg, sg, kg, vg, lim, bnd, zq, zk, zv = gather(local_len * LANES, q, do, o, row_lse, doc, k, v)
        flat = (16 * keys_local, head_dim)
        dq, dk, dv, which = attend(bnd, kg.reshape(flat), vg.reshape(flat), qg, dg, sg, lim, zq, zk, zv)
        blocks = (4, 4, keys_local, head_dim)
        oq, ok, ov = lax.switch(which[0], [functools.partial(scatter, n) for n in (1, 2, 4)], dq, dk.reshape(blocks), dv.reshape(blocks))
        oq, ok, ov = store(oq, ok, ov)
        return (oq.reshape(query.shape), ok.reshape(keys_local, 1, head_dim), ov.reshape(keys_local, 1, head_dim))

    return jax.shard_map(local_backward, mesh=mesh, in_specs=(q_spec, q_spec, q_spec, lse_spec, kv_spec, kv_spec, P()), out_specs=(q_spec, kv_spec, kv_spec), check_vma=False)
```

```python
import functools

import jax
import jax.numpy as jnp
from jax import lax
from jax.experimental import pallas as pl
from jax.experimental.pallas import tpu as pltpu
from jax.sharding import PartitionSpec as P

MESH = pl.DeviceIdType.MESH
TK = 256
LANES = 128
GROUP = 8
MIB = 2 ** 20
LOG2E = 1.4426950408889634
F32, BF16 = jnp.float32, jnp.bfloat16


def place():
    me = lax.axis_index('cp')
    return me // 32, lax.rem(me // GROUP, 4), lax.rem(me // 2, 4), lax.rem(me, 2)


def at(z, y, x, c):
    return ((z * 4 + y) * 4 + x) * 2 + c


def up(v):
    return lax.rem(v + 1, 4)


def down(v):
    return lax.rem(v + 3, 4)


def far(v):
    return lax.rem(v + 2, 4)


class Wire:
    def __init__(self, ssem, rsem):
        self.ssem, self.rsem, self.n, self.sent, self.groups = ssem, rsem, 0, [], {}

    def copy(self, src, dst, dev, group=None):
        i = self.groups.get(group, self.n)
        if i == self.n:
            self.n += 1
            if group is not None:
                self.groups[group] = i
        return pltpu.make_async_remote_copy(
            src_ref=src, dst_ref=dst, send_sem=self.ssem, recv_sem=self.rsem.at[i], device_id={'cp': dev}, device_id_type=MESH)

    def send(self, src, dst, dev, group=None):
        cp = self.copy(src, dst, dev, group)
        cp.start()
        self.sent.append(cp)
        return cp

    def same(self, ref, dev, group=None):
        return self.send(ref, ref, dev, group)

    def wait_all(self, group, ref):
        pltpu.make_async_copy(ref, ref, self.rsem.at[self.groups[group]]).wait()

    def finish(self):
        for cp in self.sent:
            cp.wait_send()


def greet(partners):
    barrier = pltpu.get_barrier_semaphore()
    for dev in partners:
        pl.semaphore_signal(barrier, inc=1, device_id={'cp': dev}, device_id_type=MESH)
    pl.semaphore_wait(barrier, len(partners))


def row_stats(do, o, lse, st):
    st[...] = jnp.zeros_like(st)
    tok = lax.broadcasted_iota(jnp.int32, (GROUP, LANES), 0)
    lane = lax.broadcasted_iota(jnp.int32, (GROUP, LANES), 1)
    for j in range(do.shape[0]):
        wide = jnp.concatenate([lse[j]] * GROUP, axis=1)
        st[j:j + 1, :] = jnp.sum(jnp.where((lane >> 4) == tok, wide, 0.0), axis=0, keepdims=True) * LOG2E
        prod = do[j].astype(F32) * o[j].astype(F32)
        st[GROUP + j:9 + j, :] = jnp.sum(prod.T, axis=0, keepdims=True)


def limits(doc, n_sub, sub_len, keys_local, lim, bnd):
    z, y, x, c = place()
    grp, lane = z * 4 + y, x * 2 + c
    n_pos = doc.shape[0] * LANES
    sub_start = n_pos - n_sub * sub_len
    period = GROUP * keys_local

    def flat(pos):
        b = jnp.zeros_like(pos)
        for i in range(1, n_pos // period):
            b += jnp.where(pos >= i * period, 1, 0)
        return b * keys_local + jnp.clip(pos - b * period - lane * keys_local, 0, keys_local)

    sub = lax.broadcasted_iota(jnp.int32, (GROUP, LANES), 0)
    tok = lax.broadcasted_iota(jnp.int32, (GROUP, LANES), 1)
    docs = jnp.zeros((GROUP, LANES), jnp.int32)
    for j in range(n_sub):
        row = doc[pl.ds((sub_start + j * sub_len) // LANES + grp // 2, 1), :]
        docs = jnp.where(sub == j, row, docs)
    docs = jnp.where(lax.rem(grp, 2) == 1, pltpu.roll(docs, 64, 1), docs)
    before = jnp.zeros((GROUP, LANES), jnp.int32)
    for j in range(n_sub):
        head = docs[j:j + 1, 0:1]
        count = jnp.zeros((GROUP, LANES), jnp.int32)
        for r in range(0, doc.shape[0], GROUP):
            count += jnp.where(doc[r:r + GROUP, :] < head, 1, 0)
        count = jnp.sum(jnp.sum(count.astype(F32), axis=0, keepdims=True), axis=1, keepdims=True)
        before = jnp.where(sub == j, count.astype(jnp.int32), before)
    base = sub_start + sub * sub_len + grp * 64
    pos = base + tok
    begin = jnp.where((tok > 0) & (docs != pltpu.roll(docs, 1, 1)), pos, before)
    for shift in (1, 2, 4, GROUP, 16, 32):
        begin = jnp.maximum(begin, jnp.where(tok >= shift, pltpu.roll(begin, shift, 1), 0))
    pick = jnp.where(
        lax.broadcasted_iota(jnp.int32, (LANES, 1024), 0) == lax.broadcasted_iota(jnp.int32, (LANES, 1024), 1) >> 4, 1.0, 0.0)
    for first, value in ((0, flat(begin)), (GROUP, flat(pos + 1))):
        wide = jnp.dot(value.astype(F32), pick, precision=lax.Precision.HIGHEST, preferred_element_type=F32)
        for l in range(GROUP):
            lim[l, first:first + GROUP, :] = wide[:, LANES * l:LANES * l + LANES].astype(jnp.int32)
    start = flat(before) & -16
    tiles = jnp.maximum((flat(base + 64) - start + (TK - 1)) // TK, jnp.where(sub == 0, 1, 0))
    first = doc[pl.ds(sub_start // LANES, 1), :][:, 0:1]
    edge = lambda planes: doc[pl.ds((n_pos - planes * n_pos // 4 - 1) // LANES, 1), :][:, 127:LANES] >= first
    which = jnp.where(edge(1), jnp.where(edge(2), 2, 1), 0)
    bnd[...] = jnp.where(tok == 0, start, jnp.where(tok == 1, tiles, which))


def clear(zq, zk, zv):
    def rows(i, _):
        for r in range(4):
            at_ = pl.ds(pl.multiple_of((i * 4 + r) * 16, 16), 16)
            zk[at_, :] = jnp.zeros((16, LANES), F32)
            zv[at_, :] = jnp.zeros((16, LANES), F32)
        return 0

    lax.fori_loop(0, zk.shape[0] // 64, rows, 0)

    def block(i, _):
        zq[i // GROUP, lax.rem(i, GROUP)] = jnp.zeros((LANES, LANES), F32)
        return 0

    lax.fori_loop(0, zq.shape[0] * GROUP, block, 0)


def gather_body(sub_len, q, do, o, lse, doc, k, v, rg, sg, kg, vg, lim, bnd, zq, zk, zv, st, ov, lv, cv, lsem, ssem, rsem):
    z, y, x, c = place()
    xu, xd, sib = at(z, y, up(x), c), at(z, y, down(x), c), at(z, y, x, 1 - c)
    yu, yd = at(z, up(y), x, c), at(z, down(y), x, c)
    zu, zd = at(up(z), y, x, c), at(down(z), y, x, c)
    lane = lambda xx: xx * 2 + c
    own, n_sub, n_own = lane(x), q.shape[0], k.shape[0]
    loads = []
    for i, (src, dst) in enumerate((
            (q, rg.at[0, :, own]), (do, rg.at[1, :, own]), (k, kg.at[z, y]), (v, vg.at[z, y]), (o, ov), (lse, lv), (doc, cv))):
        loads.append(pltpu.make_async_copy(src, dst, lsem.at[max(i // 2, i - 2)]))
        loads[i].start()
    greet([xu, xd, sib, yu, yd, zu, zd])
    w = Wire(ssem, rsem)
    same = w.same
    rows = lambda half, l: rg.at[:, pl.ds(half * (n_sub // 2), n_sub // 2), l]
    k_own, v_own = kg.at[z, y], vg.at[z, y]

    def load(i, ref):
        pltpu.make_async_copy(ref, ref, lsem.at[i]).wait()

    def end(ref, dev, group='keys'):
        same(ref, dev, group)

    load(0, rg.at[:, :, own])
    ru_a, rd_b = same(rows(0, own), xu), same(rows(1, own), xd)
    load(1, kg.at[0, pl.ds(0, 2)])
    k_u, k_d = same(k_own, yu), same(k_own, yd)
    v_u, v_d = same(v_own, zu), same(v_own, zd)
    ru_b, rd_a = same(rows(1, own), xu), same(rows(0, own), xd)
    end(rg.at[:, :, own], sib, 'rows')
    kz, vy = {}, {}
    slot = lambda r, v_: lax.rem(v_ + r, 4)

    def second(kind, r):
        ref = kg.at[z, slot(r, y)] if kind is kz else vg.at[slot(r, z), y]
        for way, dev in (('u', zu if kind is kz else yu), ('d', zd if kind is kz else yd)):
            goes_on = (r < 2) == (way == 'u')
            kind[way, r] = same(ref, dev, None if goes_on else 'keys')

    second(kz, 0)
    second(vy, 0)
    for cp in loads[4:]:
        cp.wait()
    row_stats(rg.at[1, :, own], ov, lv, st)
    sg[own] = st[...]
    limits(cv, n_sub, sub_len, n_own, lim, bnd)
    su, sd = w.send(st, sg.at[own], xu), w.send(st, sg.at[own], xd)
    w.send(st, sg.at[own], sib, 'stats')
    clear(zq, zk, zv)
    low = n_own // 32 * 16 + 16
    lo_rows, hi_rows = pl.ds(0, low), pl.ds(low, n_own - low)
    k_u.wait_recv()
    same(kg.at[z, down(y), lo_rows], yu, 'k')
    k_d.wait_recv()
    same(kg.at[z, up(y), hi_rows], yd, 'k')
    v_u.wait_recv()
    same(vg.at[down(z), y, lo_rows], zu, 'v')
    v_d.wait_recv()
    same(vg.at[up(z), y, hi_rows], zd, 'v')
    for r in (3, 1):
        second(kz, r)
        second(vy, r)
    w.wait_all('k', kg.at[z, far(y)])
    second(kz, 2)
    w.wait_all('v', vg.at[far(z), y])
    second(vy, 2)
    ld, lu, lf = lane(down(x)), lane(up(x)), lane(far(x))
    ru_a.wait_recv()
    fu = same(rows(0, ld), xu)
    rd_b.wait_recv()
    fd = same(rows(1, lu), xd)
    su.wait_recv()
    sf = same(sg.at[ld], xu)
    sd.wait_recv()
    end(rows(0, ld), sib, 'rows')
    end(rows(1, lu), sib, 'rows')
    end(sg.at[ld], sib, 'stats')
    end(sg.at[lu], sib, 'stats')
    for r in (0, 3, 1, 2):
        if r == 2:
            ru_b.wait_recv()
            end(rows(1, ld), sib, 'rows')
            rd_a.wait_recv()
            end(rows(0, lu), sib, 'rows')
        yy, zz = slot(r, y), slot(r, z)
        way, zn, yn, zdev, ydev = ('u', down(z), down(y), zu, yu) if r < 2 else ('d', up(z), up(y), zd, yd)
        kz[way, r].wait_recv()
        end(kg.at[zn, yy], zdev)
        vy[way, r].wait_recv()
        end(vg.at[zz, yn], ydev)
    sf.wait_recv()
    end(sg.at[lf], sib, 'stats')
    fu.wait_recv()
    end(rows(0, lf), sib, 'rows')
    fd.wait_recv()
    end(rows(1, lf), sib, 'rows')
    w.wait_all('rows', rg.at[0])
    w.wait_all('stats', sg.at[pl.ds(0, 4)])
    w.wait_all('keys', kg)
    w.finish()


def gather(sub_len, q, do, o, lse, doc, k, v):
    n_sub = q.shape[0]
    vm = pl.BlockSpec(memory_space=pltpu.VMEM)
    return pl.pallas_call(
        functools.partial(gather_body, sub_len),
        in_specs=[pl.BlockSpec(memory_space=pltpu.HBM)] * 7,
        out_specs=[vm] * 9,
        out_shape=[
            jax.ShapeDtypeStruct((2, n_sub, GROUP, LANES, LANES), BF16),
            jax.ShapeDtypeStruct((GROUP, 16, LANES), F32),
            jax.ShapeDtypeStruct((4, 4) + k.shape, BF16),
            jax.ShapeDtypeStruct((4, 4) + k.shape, BF16),
            jax.ShapeDtypeStruct((GROUP, 16, LANES), jnp.int32),
            jax.ShapeDtypeStruct((GROUP, LANES), jnp.int32),
            jax.ShapeDtypeStruct((n_sub, GROUP, LANES, LANES), F32),
            jax.ShapeDtypeStruct((16 * k.shape[0], LANES), F32),
            jax.ShapeDtypeStruct((16 * k.shape[0], LANES), F32),
        ],
        scratch_shapes=[
            pltpu.VMEM((16, LANES), F32), pltpu.VMEM(o.shape, BF16), pltpu.VMEM(lse.shape, F32), pltpu.VMEM(doc.shape, jnp.int32),
            pltpu.SemaphoreType.DMA((5,)), pltpu.SemaphoreType.DMA(()), pltpu.SemaphoreType.DMA((26,))],
        compiler_params=pltpu.CompilerParams(collective_id=0, has_side_effects=True, vmem_limit_bytes=GROUP * MIB),
        name='gather',
    )(*[pltpu.with_memory_space_constraint(a, pltpu.HBM) for a in (q, do, o, lse, doc, k, v)])


def attend_body(scale, bnd, kg, vg, rg, st, lim, zq, zk, zv, dq, dk, dv, which, p0, d0, p1, d1):
    q, do = rg.at[0], rg.at[1]
    n_keys, n_sub, n_lane = kg.shape[0], rg.shape[1], rg.shape[2]

    which[0] = bnd[0, 2]
    total = bnd[0, 1]
    for j in range(1, n_sub):
        total = total + bnd[j, 1]

    def tile_of(j, i):
        nominal = bnd[j, 0] + i * TK
        return nominal, pl.multiple_of(jnp.minimum(nominal, n_keys - TK), 16)

    def front(j, i, pr, dr):
        nominal, first = tile_of(j, i)
        rows = pl.ds(first, TK)
        kt, vt = kg[rows, :], vg[rows, :]
        index = lax.broadcasted_iota(jnp.int32, (TK, LANES), 0) + first

        def chunk(m):
            qc = q[j, 2 * m:2 * m + 2].reshape(256, LANES)
            dc = do[j, 2 * m:2 * m + 2].reshape(256, LANES)
            s = lax.dot_general(kt, qc, (((1,), (1,)), ((), ())), preferred_element_type=F32)
            dp = lax.dot_general(vt, dc, (((1,), (1,)), ((), ())), preferred_element_type=F32)
            for h in range(2):
                l = 2 * m + h
                cols = slice(LANES * h, LANES * h + LANES)
                lse, delta = st[l, pl.ds(j, 1), :], st[l, pl.ds(j + GROUP, 1), :]
                low, high = lim[l, pl.ds(j, 1), :], lim[l, pl.ds(j + GROUP, 1), :]
                e = jnp.exp2(s[:, cols] * (scale * LOG2E) - lse)
                p = jnp.where((index >= jnp.maximum(low, nominal)) & (index < high), e, 0.0)
                pr[l] = p.astype(BF16)
                dr[l] = (p * (dp[:, cols] - delta)).astype(BF16)

        return [functools.partial(chunk, m) for m in range(n_lane // 2)]

    def back(j, i, pr, dr):
        rows = pl.ds(tile_of(j, i)[1], TK)
        wide = lambda ref, ls: jnp.concatenate([ref[l] for l in ls], axis=1)

        def values():
            dv[rows, :] += jnp.dot(wide(pr, range(n_lane)), do[j].reshape(n_lane * LANES, LANES), preferred_element_type=F32)

        def keys():
            t = lax.dot_general(q[j].reshape(n_lane * LANES, LANES).T, wide(dr, range(n_lane)), (((1,), (1,)), ((), ())), preferred_element_type=F32)
            dk[rows, :] += t.T

        def queries():
            ktt = kg[rows, :].T
            for m in range(n_lane // 2):
                t = jnp.dot(ktt, wide(dr, (2 * m, 2 * m + 1)), preferred_element_type=F32)
                dq[j, 2 * m] += t[:, :LANES]
                dq[j, 2 * m + 1] += t[:, LANES:]

        return [values, keys, queries]

    def do_all(*parts):
        for part in parts:
            part()

    def beyond(j):
        nxt = n_sub - 1
        for jj in reversed(range(n_sub - 1)):
            nxt = jnp.where((jj > j) & (bnd[jj, 1] > 0), jj, nxt)
        return nxt

    def after(j, i):
        turn = i + 1 >= bnd[j, 1]
        return jnp.where(turn, beyond(j), j), jnp.where(turn, 0, i + 1)

    def step(now, have, want):
        nxt = after(*now)
        b, f = back(*now, *have), front(*nxt, *want)
        do_all(b[0], f[0], f[1], b[1], f[2], f[3], b[2])
        return nxt

    def four(_, now):
        for _ in range(2):
            now = step(step(now, (p0, d0), (p1, d1)), (p1, d1), (p0, d0))
        return now

    def one(_, now):
        nxt = after(*now)
        do_all(*back(*now, p0, d0), *front(*nxt, p0, d0))
        return nxt

    first = (beyond(jnp.int32(-1)), jnp.int32(0))
    do_all(*front(*first, p0, d0))
    more = total - 1
    now = lax.fori_loop(0, more // 4, four, first)
    now = lax.fori_loop(0, lax.rem(more, 4), one, now)
    do_all(*back(*now, p0, d0))


def attend(bnd, kg, vg, rg, st, lim, zq, zk, zv):
    n_lane = rg.shape[2]
    vm = pl.BlockSpec(memory_space=pltpu.VMEM)
    return pl.pallas_call(
        functools.partial(attend_body, LANES ** -0.5),
        in_specs=[pl.BlockSpec(memory_space=pltpu.SMEM)] + [vm] * GROUP,
        out_specs=[vm] * 3 + [pl.BlockSpec(memory_space=pltpu.SMEM)],
        out_shape=[jax.ShapeDtypeStruct(rg.shape[1:], F32), jax.ShapeDtypeStruct(kg.shape, F32),
                   jax.ShapeDtypeStruct(kg.shape, F32), jax.ShapeDtypeStruct((1,), jnp.int32)],
        input_output_aliases={6: 0, 7: 1, GROUP: 2},
        scratch_shapes=[pltpu.VMEM((n_lane, TK, LANES), BF16)] * 4,
        compiler_params=pltpu.CompilerParams(vmem_limit_bytes=16 * MIB),
        name='attend',
    )(bnd, kg, vg, rg, st, lim, zq, zk, zv)


class Split:
    def __init__(self, planes, keys):
        self.planes, self.keys, self.parts = planes, keys, 4 // planes
        self.rows = -(-keys // self.parts // 16) * 16 if planes == 1 else keys // self.parts
        self.last = keys - self.rows
        cut = -(-self.rows // 16) * GROUP
        self.chunks = [(0, self.rows)] if planes == 1 else [(0, cut), (cut, self.rows - cut)]
        self.half = (2 * self.rows, LANES) if planes == 1 else (2, self.rows, LANES)

    def slot(self, z):
        if self.planes == 4:
            return z, 0
        if self.planes == 2:
            return jnp.where(lax.rem(z, 3) == 0, 3, 2), jnp.where(z < 2, self.rows, 0)
        return 3, jnp.minimum(lax.rem(z + 1, 4) * self.rows, self.last)

    def rows_at(self, first, chunk):
        return pl.ds(pl.multiple_of(first + chunk[0], GROUP), chunk[1])

    def keys_of(self, dk, z, ys, chunk):
        owner, first = self.slot(z)
        return dk.at[owner, ys, self.rows_at(first, chunk)]

    def cut(self, ref, chunk):
        return ref if self.planes == 1 else ref.at[:, pl.ds(*chunk)]

    def values_of(self, dv, y, h, chunk):
        if self.planes == 4:
            return dv.at[pl.ds(2 * h, 2), y, pl.ds(*chunk)]
        if self.planes == 2:
            return dv.at[2 + h, y, :, pl.ds(*chunk)]
        return dv.at[3, y, pl.ds(h * (self.keys - 2 * self.rows), 2 * self.rows)]

    def value_slot(self, vs, z, chunk):
        owner, first = self.slot(z)
        if self.planes == 4:
            return vs.at[z // 2, lax.rem(z, 2), pl.ds(*chunk)]
        if self.planes == 2:
            return vs.at[owner - 2, jnp.where(z < 2, 1, 0), pl.ds(*chunk)]
        h = jnp.where(first >= 2 * self.rows, 1, 0)
        return vs.at[h, self.rows_at(first - h * (self.keys - 2 * self.rows), chunk)]

    def shares(self):
        if self.planes == 4:
            return []
        if self.planes == 2:
            return [(3, 1, 0), (2, 1, 1)]
        return [(3, h, (3 + h) % 4) for h in (1, 2, 3)]


class Ring:
    def __init__(self, w, place_, dev_up, dev_down, block, via, got, both):
        self.w, self.p, self.up, self.dn = w, place_, dev_up, dev_down
        self.block, self.via, self.got, self.both = block, via, got, both

    def first_up(self):
        self.fu = self.w.send(self.block(far(self.p), 0), self.via(0), self.up)

    def first_down(self):
        self.fd = self.w.send(self.block(far(self.p), 1), self.via(1), self.dn)

    def direct_up(self):
        self.du = self.w.send(self.block(up(self.p), 1), self.got(0, 1), self.up, self)

    def direct_down(self):
        self.dd = self.w.send(self.block(down(self.p), 0), self.got(1, 0), self.dn, self)

    def start(self):
        self.first_up()
        self.first_down()
        self.direct_up()
        self.direct_down()

    def middle(self):
        w, p = self.w, self.p
        self.fu.wait_recv()
        add(self.via(0), self.block(up(p), 0))
        self.mu = w.send(self.via(0), self.got(0, 0), self.up, self)
        self.fd.wait_recv()
        add(self.via(1), self.block(down(p), 1))
        self.md = w.send(self.via(1), self.got(1, 1), self.dn, self)

    def wait(self):
        self.w.wait_all(self, self.both)


def add(dst, src):
    dst[...] = dst[...] + src[...]


def scatter_body(scale, sp, dq, dk, dv, oq, ok, ov, sq, sv, sg, k1v, k1g, ks, k2v, k2g, kr, v1v, v1g, vs, v2v, v2g, vr, ssem, rsem):
    z, y, x, c = place()
    xu, xd, sib = at(z, y, up(x), c), at(z, y, down(x), c), at(z, y, x, 1 - c)
    yu, yd = at(z, up(y), x, c), at(z, down(y), x, c)
    zu, zd = at(up(z), y, x, c), at(down(z), y, x, c)
    greet([xu, xd, sib, yu, yd, zu, zd] + ([at(far(z), y, x, c)] if sp.planes == 1 else []))
    w = Wire(ssem, rsem)
    n_sub = dq.shape[0]
    hn = n_sub // 2
    halves = (range(hn), range(hn, n_sub))
    order = ((far(x), halves[0]), (far(x), halves[1]), (up(x), range(n_sub)), (down(x), range(n_sub)), (x, range(n_sub)))
    cross = [w.send(dq.at[pl.ds(js[0], len(js)), xx * 2 + 1 - c], sq.at[xx, pl.ds(js[0], len(js))], sib) for xx, js in order]
    hy = (pl.ds(0, 2), pl.ds(2, 2))

    class Chunk:
        def __init__(self, chunk):
            low = -(-chunk[1] // 16) * GROUP
            hr = ((chunk[0], low), (chunk[0] + low, chunk[1] - low))
            part = lambda ref: ref.at[pl.ds(*chunk)]
            self.kone = Ring(w, z, zu, zd, lambda b, h: sp.keys_of(dk, b, hy[h], chunk),
                             lambda h: k1v.at[h, :, pl.ds(*chunk)], lambda s, h: k1g.at[s, hy[h], pl.ds(*chunk)],
                             k1g.at[:, :, pl.ds(*chunk)])
            self.vone = Ring(w, y, yu, yd, lambda b, h: sp.values_of(dv, b, h, chunk),
                             lambda h: sp.cut(v1v.at[h], chunk), lambda s, h: sp.cut(v1g.at[s, h], chunk),
                             v1g if sp.planes == 1 else v1g.at[:, :, :, pl.ds(*chunk)])
            self.ktwo = Ring(w, y, yu, yd, lambda b, h: ks.at[b, pl.ds(*hr[h])],
                             lambda h: k2v.at[h, pl.ds(*hr[h])], lambda s, h: k2g.at[s, pl.ds(*hr[h])],
                             k2g.at[:, pl.ds(*chunk)])
            self.vtwo = Ring(w, z, zu, zd, lambda b, h: sp.value_slot(vs, b, hr[h]),
                             lambda h: v2v.at[h, pl.ds(*hr[h])], lambda s, h: v2g.at[s, pl.ds(*hr[h])],
                             v2g.at[:, pl.ds(*chunk)])
            self.chunk, self.part = chunk, part

        def turn(self):
            self.kone.wait()
            for b in range(4):
                self.part(ks.at[b])[...] = (sp.keys_of(dk, z, b, self.chunk)[...] + self.part(k1g.at[0, b])[...]
                                            + self.part(k1g.at[1, b])[...])
            self.ktwo.start()
            self.vone.wait()
            for h in range(2):
                sp.cut(vs.at[h], self.chunk)[...] = (sp.values_of(dv, y, h, self.chunk)[...] + sp.cut(v1g.at[0, h], self.chunk)[...]
                                                     + sp.cut(v1g.at[1, h], self.chunk)[...])
            self.vtwo.start()

        def end(self):
            self.ktwo.wait()
            self.part(kr.at[0])[...] = (self.part(ks.at[y])[...] + self.part(k2g.at[0])[...] + self.part(k2g.at[1])[...]) * scale
            self.go_home(kr, ok)
            self.vtwo.wait()
            self.part(vr.at[0])[...] = sp.value_slot(vs, z, self.chunk)[...] + self.part(v2g.at[0])[...] + self.part(v2g.at[1])[...]
            self.go_home(vr, ov)

        def go_home(self, buf, out):
            for owner, h, taker in sp.shares():
                cp = w.copy(self.part(buf.at[0]), self.part(buf.at[h]), at(owner, y, x, c), ('home', buf is kr))
                home.append((owner, h, taker, buf, out, self.chunk, cp))
                pl.when(z == taker)(cp.start)

    home = []
    chunks = [Chunk(chunk) for chunk in sp.chunks]
    for ch in chunks:
        ch.kone.start()
        ch.vone.start()
    hj = (pl.ds(0, hn), pl.ds(hn, n_sub - hn))
    qring = Ring(w, x, xu, xd, lambda b, h: sq.at[b, hj[h]], lambda h: sv.at[h], lambda s, h: sg.at[s, hj[h]], sg)
    steps = (qring.first_up, qring.first_down, qring.direct_up, qring.direct_down, None)
    for cp, (xx, js), then in zip(cross, order, steps):
        cp.wait_recv()
        for j in js:
            sq[xx, j] = sq[xx, j] + dq[j, xx * 2 + c]
        if then is not None:
            then()
    for ch in chunks:
        ch.kone.middle()
        ch.vone.middle()
    qring.middle()
    for ch in chunks:
        ch.turn()
    for ch in chunks:
        ch.ktwo.middle()
        ch.vtwo.middle()
    for ch in chunks:
        ch.end()
    qring.wait()
    for j in range(n_sub):
        oq[j] = ((sq[x, j] + sg[0, j] + sg[1, j]).T * scale).astype(BF16)
    if sp.planes == 4:
        ok[...] = kr[0]
        ov[...] = vr[0]
    else:
        @pl.when(z < 4 - sp.planes)
        def _():
            ok[...] = jnp.zeros_like(ok)
            ov[...] = jnp.zeros_like(ov)

        @pl.when(z >= 4 - sp.planes)
        def _():
            ok[0:sp.rows, :] = kr[0]
            ov[0:sp.rows, :] = vr[0]

        for buf in (kr, vr):
            pl.when(z >= 4 - sp.planes)(functools.partial(w.wait_all, ('home', buf is kr), buf.at[pl.ds(1, sp.parts - 1)]))
        for _, _, taker, _, _, _, cp in home:
            pl.when(z == taker)(cp.wait_send)
        for owner, h, taker, buf, out, chunk, cp in home:
            first = min(h * sp.rows, sp.last) + chunk[0]

            @pl.when(z == owner)
            def _():
                out[first:first + chunk[1], :] = buf[h, chunk[0]:chunk[0] + chunk[1], :]

    w.finish()


def scatter(planes, dq, dk, dv):
    n_sub = dq.shape[0]
    sp = Split(planes, dk.shape[2])
    if planes == 2:
        dv = dv.reshape(4, 4, 2, sp.rows, LANES)
    rows = sp.rows
    vm = pl.BlockSpec(memory_space=pltpu.VMEM)
    two = [
        pltpu.VMEM((2, rows, LANES), F32),
        pltpu.VMEM((2, rows, LANES), F32),
        pltpu.VMEM((sp.parts, rows, LANES), F32),
    ]
    return pl.pallas_call(
        functools.partial(scatter_body, LANES ** -0.5, sp),
        in_specs=[vm] * 3,
        out_specs=[vm] * 3,
        out_shape=[
            jax.ShapeDtypeStruct((n_sub, LANES, LANES), BF16),
            jax.ShapeDtypeStruct((sp.keys, LANES), F32),
            jax.ShapeDtypeStruct((sp.keys, LANES), F32),
        ],
        scratch_shapes=[
            pltpu.VMEM((4, n_sub, LANES, LANES), F32),
            pltpu.VMEM((2, n_sub // 2, LANES, LANES), F32),
            pltpu.VMEM((2, n_sub, LANES, LANES), F32),
            pltpu.VMEM((2, 2, rows, LANES), F32), pltpu.VMEM((2, 4, rows, LANES), F32), pltpu.VMEM((4, rows, LANES), F32), *two,
            pltpu.VMEM((2,) + sp.half, F32), pltpu.VMEM((2, 2) + sp.half, F32), pltpu.VMEM((2,) + sp.half, F32), *two,
            pltpu.SemaphoreType.DMA(()), pltpu.SemaphoreType.DMA((10 + 12 * len(sp.chunks),))],
        compiler_params=pltpu.CompilerParams(collective_id=planes, has_side_effects=True, vmem_limit_bytes=20 * MIB),
        name='scatter',
    )(dq, dk, dv)


def store_body(a, b, c, oa, ob, oc, sem):
    copies = [pltpu.make_async_copy(src, dst, sem.at[i]) for i, (src, dst) in enumerate(((a, oa), (b, ob), (c, oc)))]
    for cp in copies:
        cp.start()
    for cp in copies:
        cp.wait()


def store(*arrays):
    return pl.pallas_call(
        store_body,
        in_specs=[pl.BlockSpec(memory_space=pltpu.VMEM)] * 3,
        out_specs=[pl.BlockSpec(memory_space=pltpu.HBM)] * 3,
        out_shape=[jax.ShapeDtypeStruct(a.shape, a.dtype) for a in arrays],
        scratch_shapes=[pltpu.SemaphoreType.DMA((3,))],
        name='store',
    )(*arrays)


def solution(mesh):
    q_spec = P(None, 'cp', 'tp', None)
    lse_spec = P(None, 'cp', 'tp')
    kv_spec = P('cp', 'tp', None)

    def local_backward(query, out_act, out_grad, row_lse, key_act, value_act, doc_ids):
        n_sub, local_len, n_heads, head_dim = query.shape
        keys_local = key_act.shape[0]
        rows = local_len * n_heads
        q = query.reshape(n_sub, rows, head_dim)
        do = out_grad.reshape(n_sub, rows, head_dim)
        o = out_act.reshape(n_sub, rows, head_dim)
        doc = doc_ids.reshape(-1, LANES)
        k, v = key_act.reshape(keys_local, head_dim), value_act.reshape(keys_local, head_dim)
        rg, sg, kg, vg, lim, bnd, zq, zk, zv = gather(local_len * LANES, q, do, o, row_lse, doc, k, v)
        flat = (16 * keys_local, head_dim)
        dq, dk, dv, which = attend(bnd, kg.reshape(flat), vg.reshape(flat), rg, sg, lim, zq, zk, zv)
        blocks = (4, 4, keys_local, head_dim)
        oq, ok, ov = lax.switch(which[0], [functools.partial(scatter, n) for n in (1, 2, 4)], dq, dk.reshape(blocks), dv.reshape(blocks))
        oq, ok, ov = store(oq, ok, ov)
        return (oq.reshape(query.shape), ok.reshape(keys_local, 1, head_dim), ov.reshape(keys_local, 1, head_dim))

    return jax.shard_map(local_backward, mesh=mesh, in_specs=(q_spec, q_spec, q_spec, lse_spec, kv_spec, kv_spec, P()), out_specs=(q_spec, kv_spec, kv_spec), check_vma=False)
```

```python
import functools

import jax
import jax.numpy as jnp
from jax import lax
from jax.experimental import pallas as pl
from jax.experimental.pallas import tpu as pltpu
from jax.sharding import PartitionSpec as P

MESH = pl.DeviceIdType.MESH
TK = 256
LANES = 128
GROUP = 8
MIB = 2 ** 20
LOG2E = 1.4426950408889634
F32, BF16 = jnp.float32, jnp.bfloat16


def place():
    me = lax.axis_index('cp')
    return me // 32, lax.rem(me // GROUP, 4), lax.rem(me // 2, 4), lax.rem(me, 2)


def at(z, y, x, c):
    return ((z * 4 + y) * 4 + x) * 2 + c


def up(v):
    return lax.rem(v + 1, 4)


def down(v):
    return lax.rem(v + 3, 4)


def far(v):
    return lax.rem(v + 2, 4)


class Wire:
    def __init__(self, ssem, rsem):
        self.ssem, self.rsem, self.n, self.sent, self.groups = ssem, rsem, 0, [], {}

    def copy(self, src, dst, dev, group=None):
        i = self.groups.get(group, self.n)
        if i == self.n:
            self.n += 1
            if group is not None:
                self.groups[group] = i
        return pltpu.make_async_remote_copy(
            src_ref=src, dst_ref=dst, send_sem=self.ssem, recv_sem=self.rsem.at[i], device_id={'cp': dev}, device_id_type=MESH)

    def send(self, src, dst, dev, group=None):
        cp = self.copy(src, dst, dev, group)
        cp.start()
        self.sent.append(cp)
        return cp

    def same(self, ref, dev, group=None):
        return self.send(ref, ref, dev, group)

    def wait_all(self, group, ref):
        pltpu.make_async_copy(ref, ref, self.rsem.at[self.groups[group]]).wait()

    def finish(self):
        for cp in self.sent:
            cp.wait_send()


def greet(partners):
    barrier = pltpu.get_barrier_semaphore()
    for dev in partners:
        pl.semaphore_signal(barrier, inc=1, device_id={'cp': dev}, device_id_type=MESH)
    pl.semaphore_wait(barrier, len(partners))


def row_stats(do, o, lse, st):
    st[...] = jnp.zeros_like(st)
    tok = lax.broadcasted_iota(jnp.int32, (GROUP, LANES), 0)
    lane = lax.broadcasted_iota(jnp.int32, (GROUP, LANES), 1)
    for j in range(do.shape[0]):
        wide = jnp.concatenate([lse[j]] * GROUP, axis=1)
        st[j:j + 1, :] = jnp.sum(jnp.where((lane >> 4) == tok, wide, 0.0), axis=0, keepdims=True) * LOG2E
        prod = do[j].astype(F32) * o[j].astype(F32)
        st[GROUP + j:9 + j, :] = jnp.sum(prod.T, axis=0, keepdims=True)


def limits(doc, n_sub, sub_len, keys_local, lim, bnd):
    z, y, x, c = place()
    grp, lane = z * 4 + y, x * 2 + c
    n_pos = doc.shape[0] * LANES
    sub_start = n_pos - n_sub * sub_len
    period = GROUP * keys_local

    def flat(pos):
        b = jnp.zeros_like(pos)
        for i in range(1, n_pos // period):
            b += jnp.where(pos >= i * period, 1, 0)
        return b * keys_local + jnp.clip(pos - b * period - lane * keys_local, 0, keys_local)

    sub = lax.broadcasted_iota(jnp.int32, (GROUP, LANES), 0)
    tok = lax.broadcasted_iota(jnp.int32, (GROUP, LANES), 1)
    docs = jnp.zeros((GROUP, LANES), jnp.int32)
    for j in range(n_sub):
        row = doc[pl.ds((sub_start + j * sub_len) // LANES + grp // 2, 1), :]
        docs = jnp.where(sub == j, row, docs)
    docs = jnp.where(lax.rem(grp, 2) == 1, pltpu.roll(docs, 64, 1), docs)
    before = jnp.zeros((GROUP, LANES), jnp.int32)
    for j in range(n_sub):
        head = docs[j:j + 1, 0:1]
        count = jnp.zeros((GROUP, LANES), jnp.int32)
        for r in range(0, doc.shape[0], GROUP):
            count += jnp.where(doc[r:r + GROUP, :] < head, 1, 0)
        count = jnp.sum(jnp.sum(count.astype(F32), axis=0, keepdims=True), axis=1, keepdims=True)
        before = jnp.where(sub == j, count.astype(jnp.int32), before)
    base = sub_start + sub * sub_len + grp * 64
    pos = base + tok
    begin = jnp.where((tok > 0) & (docs != pltpu.roll(docs, 1, 1)), pos, before)
    for shift in (1, 2, 4, GROUP, 16, 32):
        begin = jnp.maximum(begin, jnp.where(tok >= shift, pltpu.roll(begin, shift, 1), 0))
    pick = jnp.where(
        lax.broadcasted_iota(jnp.int32, (LANES, 1024), 0) == lax.broadcasted_iota(jnp.int32, (LANES, 1024), 1) >> 4, 1.0, 0.0)
    for first, value in ((0, flat(begin)), (GROUP, flat(pos + 1))):
        wide = jnp.dot(value.astype(F32), pick, precision=lax.Precision.HIGHEST, preferred_element_type=F32)
        for l in range(GROUP):
            lim[l, first:first + GROUP, :] = wide[:, LANES * l:LANES * l + LANES].astype(jnp.int32)
    start = flat(before) & -16
    tiles = jnp.maximum((flat(base + 64) - start + (TK - 1)) // TK, jnp.where(sub == 0, 1, 0))
    first = doc[pl.ds(sub_start // LANES, 1), :][:, 0:1]
    edge = lambda planes: doc[pl.ds((n_pos - planes * n_pos // 4 - 1) // LANES, 1), :][:, 127:LANES] >= first
    which = jnp.where(edge(1), jnp.where(edge(2), 2, 1), 0)
    bnd[...] = jnp.where(tok == 0, start, jnp.where(tok == 1, tiles, which))


def clear(zq, zk, zv):
    def rows(i, _):
        for r in range(4):
            at_ = pl.ds(pl.multiple_of((i * 4 + r) * 16, 16), 16)
            zk[at_, :] = jnp.zeros((16, LANES), F32)
            zv[at_, :] = jnp.zeros((16, LANES), F32)
        return 0

    lax.fori_loop(0, zk.shape[0] // 64, rows, 0)

    def block(i, _):
        zq[i // GROUP, lax.rem(i, GROUP)] = jnp.zeros((LANES, LANES), F32)
        return 0

    lax.fori_loop(0, zq.shape[0] * GROUP, block, 0)


def gather_body(sub_len, q, do, o, lse, doc, k, v, rg, sg, kg, vg, lim, bnd, zq, zk, zv, st, ov, lv, cv, lsem, ssem, rsem):
    z, y, x, c = place()
    xu, xd, sib = at(z, y, up(x), c), at(z, y, down(x), c), at(z, y, x, 1 - c)
    yu, yd = at(z, up(y), x, c), at(z, down(y), x, c)
    zu, zd = at(up(z), y, x, c), at(down(z), y, x, c)
    lane = lambda xx: xx * 2 + c
    own, n_sub, n_own = lane(x), q.shape[0], k.shape[0]
    loads = []
    for i, (src, dst) in enumerate((
            (q, rg.at[0, :, own]), (do, rg.at[1, :, own]), (k, kg.at[z, y]), (v, vg.at[z, y]), (o, ov), (lse, lv), (doc, cv))):
        loads.append(pltpu.make_async_copy(src, dst, lsem.at[max(i // 2, i - 2)]))
        loads[i].start()
    greet([xu, xd, sib, yu, yd, zu, zd])
    w = Wire(ssem, rsem)
    same = w.same
    rows = lambda half, l: rg.at[:, pl.ds(half * (n_sub // 2), n_sub // 2), l]
    k_own, v_own = kg.at[z, y], vg.at[z, y]

    def load(i, ref):
        pltpu.make_async_copy(ref, ref, lsem.at[i]).wait()

    def end(ref, dev, group='keys'):
        same(ref, dev, group)

    load(0, rg.at[:, :, own])
    ru_a, rd_b = same(rows(0, own), xu), same(rows(1, own), xd)
    load(1, kg.at[0, pl.ds(0, 2)])
    k_u, k_d = same(k_own, yu), same(k_own, yd)
    v_u, v_d = same(v_own, zu), same(v_own, zd)
    ru_b, rd_a = same(rows(1, own), xu), same(rows(0, own), xd)
    end(rg.at[:, :, own], sib, 'rows')
    kz, vy = {}, {}
    slot = lambda r, v_: lax.rem(v_ + r, 4)

    def second(kind, r):
        ref = kg.at[z, slot(r, y)] if kind is kz else vg.at[slot(r, z), y]
        for way, dev in (('u', zu if kind is kz else yu), ('d', zd if kind is kz else yd)):
            goes_on = (r < 2) == (way == 'u')
            kind[way, r] = same(ref, dev, None if goes_on else 'keys')

    second(kz, 0)
    second(vy, 0)
    for cp in loads[4:]:
        cp.wait()
    row_stats(rg.at[1, :, own], ov, lv, st)
    sg[own] = st[...]
    limits(cv, n_sub, sub_len, n_own, lim, bnd)
    su, sd = w.send(st, sg.at[own], xu), w.send(st, sg.at[own], xd)
    w.send(st, sg.at[own], sib, 'stats')
    clear(zq, zk, zv)
    low = n_own // 32 * 16 + 16
    lo_rows, hi_rows = pl.ds(0, low), pl.ds(low, n_own - low)
    k_u.wait_recv()
    same(kg.at[z, down(y), lo_rows], yu, 'k')
    k_d.wait_recv()
    same(kg.at[z, up(y), hi_rows], yd, 'k')
    v_u.wait_recv()
    same(vg.at[down(z), y, lo_rows], zu, 'v')
    v_d.wait_recv()
    same(vg.at[up(z), y, hi_rows], zd, 'v')
    for r in (3, 1):
        second(kz, r)
        second(vy, r)
    w.wait_all('k', kg.at[z, far(y)])
    second(kz, 2)
    w.wait_all('v', vg.at[far(z), y])
    second(vy, 2)
    ld, lu, lf = lane(down(x)), lane(up(x)), lane(far(x))
    ru_a.wait_recv()
    fu = same(rows(0, ld), xu)
    rd_b.wait_recv()
    fd = same(rows(1, lu), xd)
    su.wait_recv()
    sf = same(sg.at[ld], xu)
    sd.wait_recv()
    end(rows(0, ld), sib, 'rows')
    end(rows(1, lu), sib, 'rows')
    end(sg.at[ld], sib, 'stats')
    end(sg.at[lu], sib, 'stats')
    for r in (0, 3, 1, 2):
        if r == 2:
            ru_b.wait_recv()
            end(rows(1, ld), sib, 'rows')
            rd_a.wait_recv()
            end(rows(0, lu), sib, 'rows')
        yy, zz = slot(r, y), slot(r, z)
        way, zn, yn, zdev, ydev = ('u', down(z), down(y), zu, yu) if r < 2 else ('d', up(z), up(y), zd, yd)
        kz[way, r].wait_recv()
        end(kg.at[zn, yy], zdev)
        vy[way, r].wait_recv()
        end(vg.at[zz, yn], ydev)
    sf.wait_recv()
    end(sg.at[lf], sib, 'stats')
    fu.wait_recv()
    end(rows(0, lf), sib, 'rows')
    fd.wait_recv()
    end(rows(1, lf), sib, 'rows')
    w.wait_all('rows', rg.at[0])
    w.wait_all('stats', sg.at[pl.ds(0, 4)])
    w.wait_all('keys', kg)
    w.finish()


def gather(sub_len, q, do, o, lse, doc, k, v):
    n_sub = q.shape[0]
    vm = pl.BlockSpec(memory_space=pltpu.VMEM)
    return pl.pallas_call(
        functools.partial(gather_body, sub_len),
        in_specs=[pl.BlockSpec(memory_space=pltpu.HBM)] * 7,
        out_specs=[vm] * 9,
        out_shape=[
            jax.ShapeDtypeStruct((2, n_sub, GROUP, LANES, LANES), BF16),
            jax.ShapeDtypeStruct((GROUP, 16, LANES), F32),
            jax.ShapeDtypeStruct((4, 4) + k.shape, BF16),
            jax.ShapeDtypeStruct((4, 4) + k.shape, BF16),
            jax.ShapeDtypeStruct((GROUP, 16, LANES), jnp.int32),
            jax.ShapeDtypeStruct((GROUP, LANES), jnp.int32),
            jax.ShapeDtypeStruct((n_sub, GROUP, LANES, LANES), F32),
            jax.ShapeDtypeStruct((16 * k.shape[0], LANES), F32),
            jax.ShapeDtypeStruct((16 * k.shape[0], LANES), F32),
        ],
        scratch_shapes=[
            pltpu.VMEM((16, LANES), F32), pltpu.VMEM(o.shape, BF16), pltpu.VMEM(lse.shape, F32), pltpu.VMEM(doc.shape, jnp.int32),
            pltpu.SemaphoreType.DMA((5,)), pltpu.SemaphoreType.DMA(()), pltpu.SemaphoreType.DMA((26,))],
        compiler_params=pltpu.CompilerParams(collective_id=0, has_side_effects=True, vmem_limit_bytes=GROUP * MIB),
        name='gather',
    )(*[pltpu.with_memory_space_constraint(a, pltpu.HBM) for a in (q, do, o, lse, doc, k, v)])


def attend_body(scale, bnd, kg, vg, rg, st, lim, zq, zk, zv, dq, dk, dv, which, p0, d0, p1, d1):
    q, do = rg.at[0], rg.at[1]
    n_keys, n_sub, n_lane = kg.shape[0], rg.shape[1], rg.shape[2]

    which[0] = bnd[0, 2]
    total = bnd[0, 1]
    for j in range(1, n_sub):
        total = total + bnd[j, 1]

    def tile_of(j, i):
        nominal = bnd[j, 0] + i * TK
        return nominal, pl.multiple_of(jnp.minimum(nominal, n_keys - TK), 16)

    def front(j, i, pr, dr):
        nominal, first = tile_of(j, i)
        rows = pl.ds(first, TK)
        kt, vt = kg[rows, :], vg[rows, :]
        index = lax.broadcasted_iota(jnp.int32, (TK, LANES), 0) + first

        def chunk(m):
            qc = q[j, 2 * m:2 * m + 2].reshape(256, LANES)
            dc = do[j, 2 * m:2 * m + 2].reshape(256, LANES)
            s = lax.dot_general(kt, qc, (((1,), (1,)), ((), ())), preferred_element_type=F32)
            dp = lax.dot_general(vt, dc, (((1,), (1,)), ((), ())), preferred_element_type=F32)
            for h in range(2):
                l = 2 * m + h
                cols = slice(LANES * h, LANES * h + LANES)
                lse, delta = st[l, pl.ds(j, 1), :], st[l, pl.ds(j + GROUP, 1), :]
                low, high = lim[l, pl.ds(j, 1), :], lim[l, pl.ds(j + GROUP, 1), :]
                e = jnp.exp2(s[:, cols] * (scale * LOG2E) - lse)
                low = jnp.maximum(low, nominal)
                p = jnp.where((index - low).astype(jnp.uint32) < jnp.maximum(high - low, 0).astype(jnp.uint32), e, 0.0)
                pr[l] = p.astype(BF16)
                dr[l] = (p * (dp[:, cols] - delta)).astype(BF16)

        return [functools.partial(chunk, m) for m in range(n_lane // 2)]

    def back(j, i, pr, dr):
        rows = pl.ds(tile_of(j, i)[1], TK)
        wide = lambda ref, ls: jnp.concatenate([ref[l] for l in ls], axis=1)

        def values():
            dv[rows, :] += jnp.dot(wide(pr, range(n_lane)), do[j].reshape(n_lane * LANES, LANES), preferred_element_type=F32)

        def keys():
            t = lax.dot_general(q[j].reshape(n_lane * LANES, LANES).T, wide(dr, range(n_lane)), (((1,), (1,)), ((), ())), preferred_element_type=F32)
            dk[rows, :] += t.T

        def queries():
            ktt = kg[rows, :].T
            for m in range(n_lane // 2):
                t = jnp.dot(ktt, wide(dr, (2 * m, 2 * m + 1)), preferred_element_type=F32)
                dq[j, 2 * m] += t[:, :LANES]
                dq[j, 2 * m + 1] += t[:, LANES:]

        return [values, keys, queries]

    def do_all(*parts):
        for part in parts:
            part()

    def beyond(j):
        nxt = n_sub - 1
        for jj in reversed(range(n_sub - 1)):
            nxt = jnp.where((jj > j) & (bnd[jj, 1] > 0), jj, nxt)
        return nxt

    def after(j, i):
        turn = i + 1 >= bnd[j, 1]
        return jnp.where(turn, beyond(j), j), jnp.where(turn, 0, i + 1)

    def step(now, have, want):
        nxt = after(*now)
        b, f = back(*now, *have), front(*nxt, *want)
        do_all(b[0], f[0], f[1], b[1], f[2], f[3], b[2])
        return nxt

    def two(_, now):
        return step(step(now, (p0, d0), (p1, d1)), (p1, d1), (p0, d0))

    def four(_, now):
        return two(0, two(0, now))

    def one(_, now):
        nxt = after(*now)
        do_all(*back(*now, p0, d0), *front(*nxt, p0, d0))
        return nxt

    first = (beyond(jnp.int32(-1)), jnp.int32(0))
    do_all(*front(*first, p0, d0))
    more = total - 1
    now = lax.fori_loop(0, more // 4, four, first)
    now = lax.fori_loop(0, lax.rem(more, 4) // 2, two, now)
    now = lax.fori_loop(0, lax.rem(more, 2), one, now)
    do_all(*back(*now, p0, d0))


def attend(bnd, kg, vg, rg, st, lim, zq, zk, zv):
    n_lane = rg.shape[2]
    vm = pl.BlockSpec(memory_space=pltpu.VMEM)
    return pl.pallas_call(
        functools.partial(attend_body, LANES ** -0.5),
        in_specs=[pl.BlockSpec(memory_space=pltpu.SMEM)] + [vm] * GROUP,
        out_specs=[vm] * 3 + [pl.BlockSpec(memory_space=pltpu.SMEM)],
        out_shape=[jax.ShapeDtypeStruct(rg.shape[1:], F32), jax.ShapeDtypeStruct(kg.shape, F32),
                   jax.ShapeDtypeStruct(kg.shape, F32), jax.ShapeDtypeStruct((1,), jnp.int32)],
        input_output_aliases={6: 0, 7: 1, GROUP: 2},
        scratch_shapes=[pltpu.VMEM((n_lane, TK, LANES), BF16)] * 4,
        compiler_params=pltpu.CompilerParams(vmem_limit_bytes=16 * MIB),
        name='attend',
    )(bnd, kg, vg, rg, st, lim, zq, zk, zv)


class Split:
    def __init__(self, planes, keys):
        self.planes, self.keys, self.parts = planes, keys, 4 // planes
        self.rows = -(-keys // self.parts // 16) * 16 if planes == 1 else keys // self.parts
        self.last = keys - self.rows
        cut = -(-self.rows // 16) * GROUP
        self.chunks = [(0, self.rows)] if planes == 1 else [(0, cut), (cut, self.rows - cut)]
        self.half = (2 * self.rows, LANES) if planes == 1 else (2, self.rows, LANES)

    def slot(self, z):
        if self.planes == 4:
            return z, 0
        if self.planes == 2:
            return jnp.where(lax.rem(z, 3) == 0, 3, 2), jnp.where(z < 2, self.rows, 0)
        return 3, jnp.minimum(lax.rem(z + 1, 4) * self.rows, self.last)

    def rows_at(self, first, chunk):
        return pl.ds(pl.multiple_of(first + chunk[0], GROUP), chunk[1])

    def keys_of(self, dk, z, ys, chunk):
        owner, first = self.slot(z)
        return dk.at[owner, ys, self.rows_at(first, chunk)]

    def cut(self, ref, chunk):
        return ref if self.planes == 1 else ref.at[:, pl.ds(*chunk)]

    def values_of(self, dv, y, h, chunk):
        if self.planes == 4:
            return dv.at[pl.ds(2 * h, 2), y, pl.ds(*chunk)]
        if self.planes == 2:
            return dv.at[2 + h, y, :, pl.ds(*chunk)]
        return dv.at[3, y, pl.ds(h * (self.keys - 2 * self.rows), 2 * self.rows)]

    def value_slot(self, vs, z, chunk):
        owner, first = self.slot(z)
        if self.planes == 4:
            return vs.at[z // 2, lax.rem(z, 2), pl.ds(*chunk)]
        if self.planes == 2:
            return vs.at[owner - 2, jnp.where(z < 2, 1, 0), pl.ds(*chunk)]
        h = jnp.where(first >= 2 * self.rows, 1, 0)
        return vs.at[h, self.rows_at(first - h * (self.keys - 2 * self.rows), chunk)]

    def shares(self):
        if self.planes == 4:
            return []
        if self.planes == 2:
            return [(3, 1, 0), (2, 1, 1)]
        return [(3, h, (3 + h) % 4) for h in (1, 2, 3)]


class Ring:
    def __init__(self, w, place_, dev_up, dev_down, block, via, got, both):
        self.w, self.p, self.up, self.dn = w, place_, dev_up, dev_down
        self.block, self.via, self.got, self.both = block, via, got, both

    def first_up(self):
        self.fu = self.w.send(self.block(far(self.p), 0), self.via(0), self.up)

    def first_down(self):
        self.fd = self.w.send(self.block(far(self.p), 1), self.via(1), self.dn)

    def direct_up(self):
        self.du = self.w.send(self.block(up(self.p), 1), self.got(0, 1), self.up, self)

    def direct_down(self):
        self.dd = self.w.send(self.block(down(self.p), 0), self.got(1, 0), self.dn, self)

    def start(self):
        self.first_up()
        self.first_down()
        self.direct_up()
        self.direct_down()

    def middle(self):
        w, p = self.w, self.p
        self.fu.wait_recv()
        add(self.via(0), self.block(up(p), 0))
        self.mu = w.send(self.via(0), self.got(0, 0), self.up, self)
        self.fd.wait_recv()
        add(self.via(1), self.block(down(p), 1))
        self.md = w.send(self.via(1), self.got(1, 1), self.dn, self)

    def wait(self):
        self.w.wait_all(self, self.both)


def add(dst, src):
    dst[...] = dst[...] + src[...]


def scatter_body(scale, sp, dq, dk, dv, oq, ok, ov, sq, sv, sg, k1v, k1g, ks, k2v, k2g, kr, v1v, v1g, vs, v2v, v2g, vr, ssem, rsem):
    z, y, x, c = place()
    xu, xd, sib = at(z, y, up(x), c), at(z, y, down(x), c), at(z, y, x, 1 - c)
    yu, yd = at(z, up(y), x, c), at(z, down(y), x, c)
    zu, zd = at(up(z), y, x, c), at(down(z), y, x, c)
    greet([xu, xd, sib, yu, yd, zu, zd] + ([at(far(z), y, x, c)] if sp.planes == 1 else []))
    w = Wire(ssem, rsem)
    n_sub = dq.shape[0]
    hn = n_sub // 2
    halves = (range(hn), range(hn, n_sub))
    order = ((far(x), halves[0]), (far(x), halves[1]), (up(x), range(n_sub)), (down(x), range(n_sub)), (x, range(n_sub)))
    cross = [w.send(dq.at[pl.ds(js[0], len(js)), xx * 2 + 1 - c], sq.at[xx, pl.ds(js[0], len(js))], sib) for xx, js in order]
    hy = (pl.ds(0, 2), pl.ds(2, 2))

    class Chunk:
        def __init__(self, chunk):
            low = -(-chunk[1] // 16) * GROUP
            hr = ((chunk[0], low), (chunk[0] + low, chunk[1] - low))
            part = lambda ref: ref.at[pl.ds(*chunk)]
            self.kone = Ring(w, z, zu, zd, lambda b, h: sp.keys_of(dk, b, hy[h], chunk),
                             lambda h: k1v.at[h, :, pl.ds(*chunk)], lambda s, h: k1g.at[s, hy[h], pl.ds(*chunk)],
                             k1g.at[:, :, pl.ds(*chunk)])
            self.vone = Ring(w, y, yu, yd, lambda b, h: sp.values_of(dv, b, h, chunk),
                             lambda h: sp.cut(v1v.at[h], chunk), lambda s, h: sp.cut(v1g.at[s, h], chunk),
                             v1g if sp.planes == 1 else v1g.at[:, :, :, pl.ds(*chunk)])
            self.ktwo = Ring(w, y, yu, yd, lambda b, h: ks.at[b, pl.ds(*hr[h])],
                             lambda h: k2v.at[h, pl.ds(*hr[h])], lambda s, h: k2g.at[s, pl.ds(*hr[h])],
                             k2g.at[:, pl.ds(*chunk)])
            self.vtwo = Ring(w, z, zu, zd, lambda b, h: sp.value_slot(vs, b, hr[h]),
                             lambda h: v2v.at[h, pl.ds(*hr[h])], lambda s, h: v2g.at[s, pl.ds(*hr[h])],
                             v2g.at[:, pl.ds(*chunk)])
            self.chunk, self.part = chunk, part

        def turn(self):
            self.kone.wait()
            for b in range(4):
                self.part(ks.at[b])[...] = (sp.keys_of(dk, z, b, self.chunk)[...] + self.part(k1g.at[0, b])[...]
                                            + self.part(k1g.at[1, b])[...])
            self.ktwo.start()
            self.vone.wait()
            for h in range(2):
                sp.cut(vs.at[h], self.chunk)[...] = (sp.values_of(dv, y, h, self.chunk)[...] + sp.cut(v1g.at[0, h], self.chunk)[...]
                                                     + sp.cut(v1g.at[1, h], self.chunk)[...])
            self.vtwo.start()

        def end(self):
            self.ktwo.wait()
            self.part(kr.at[0])[...] = (self.part(ks.at[y])[...] + self.part(k2g.at[0])[...] + self.part(k2g.at[1])[...]) * scale
            self.go_home(kr, ok)
            self.vtwo.wait()
            self.part(vr.at[0])[...] = sp.value_slot(vs, z, self.chunk)[...] + self.part(v2g.at[0])[...] + self.part(v2g.at[1])[...]
            self.go_home(vr, ov)

        def go_home(self, buf, out):
            for owner, h, taker in sp.shares():
                cp = w.copy(self.part(buf.at[0]), self.part(buf.at[h]), at(owner, y, x, c), ('home', buf is kr))
                home.append((owner, h, taker, buf, out, self.chunk, cp))
                pl.when(z == taker)(cp.start)

    home = []
    chunks = [Chunk(chunk) for chunk in sp.chunks]
    for ch in chunks:
        ch.kone.start()
        ch.vone.start()
    hj = (pl.ds(0, hn), pl.ds(hn, n_sub - hn))
    qring = Ring(w, x, xu, xd, lambda b, h: sq.at[b, hj[h]], lambda h: sv.at[h], lambda s, h: sg.at[s, hj[h]], sg)
    steps = (qring.first_up, qring.first_down, qring.direct_up, qring.direct_down, None)
    for cp, (xx, js), then in zip(cross, order, steps):
        cp.wait_recv()
        for j in js:
            sq[xx, j] = sq[xx, j] + dq[j, xx * 2 + c]
        if then is not None:
            then()
    for ch in chunks:
        ch.kone.middle()
        ch.vone.middle()
    qring.middle()
    for ch in chunks:
        ch.turn()
    for ch in chunks:
        ch.ktwo.middle()
        ch.vtwo.middle()
    for ch in chunks:
        ch.end()
    qring.wait()
    for j in range(n_sub):
        oq[j] = ((sq[x, j] + sg[0, j] + sg[1, j]).T * scale).astype(BF16)
    if sp.planes == 4:
        ok[...] = kr[0]
        ov[...] = vr[0]
    else:
        @pl.when(z < 4 - sp.planes)
        def _():
            ok[...] = jnp.zeros_like(ok)
            ov[...] = jnp.zeros_like(ov)

        @pl.when(z >= 4 - sp.planes)
        def _():
            ok[0:sp.rows, :] = kr[0]
            ov[0:sp.rows, :] = vr[0]

        for buf in (kr, vr):
            pl.when(z >= 4 - sp.planes)(functools.partial(w.wait_all, ('home', buf is kr), buf.at[pl.ds(1, sp.parts - 1)]))
        for _, _, taker, _, _, _, cp in home:
            pl.when(z == taker)(cp.wait_send)
        for owner, h, taker, buf, out, chunk, cp in home:
            first = min(h * sp.rows, sp.last) + chunk[0]

            @pl.when(z == owner)
            def _():
                out[first:first + chunk[1], :] = buf[h, chunk[0]:chunk[0] + chunk[1], :]

    w.finish()


def scatter(planes, dq, dk, dv):
    n_sub = dq.shape[0]
    sp = Split(planes, dk.shape[2])
    if planes == 2:
        dv = dv.reshape(4, 4, 2, sp.rows, LANES)
    rows = sp.rows
    vm = pl.BlockSpec(memory_space=pltpu.VMEM)
    two = [
        pltpu.VMEM((2, rows, LANES), F32),
        pltpu.VMEM((2, rows, LANES), F32),
        pltpu.VMEM((sp.parts, rows, LANES), F32),
    ]
    return pl.pallas_call(
        functools.partial(scatter_body, LANES ** -0.5, sp),
        in_specs=[vm] * 3,
        out_specs=[vm] * 3,
        out_shape=[
            jax.ShapeDtypeStruct((n_sub, LANES, LANES), BF16),
            jax.ShapeDtypeStruct((sp.keys, LANES), F32),
            jax.ShapeDtypeStruct((sp.keys, LANES), F32),
        ],
        scratch_shapes=[
            pltpu.VMEM((4, n_sub, LANES, LANES), F32),
            pltpu.VMEM((2, n_sub // 2, LANES, LANES), F32),
            pltpu.VMEM((2, n_sub, LANES, LANES), F32),
            pltpu.VMEM((2, 2, rows, LANES), F32), pltpu.VMEM((2, 4, rows, LANES), F32), pltpu.VMEM((4, rows, LANES), F32), *two,
            pltpu.VMEM((2,) + sp.half, F32), pltpu.VMEM((2, 2) + sp.half, F32), pltpu.VMEM((2,) + sp.half, F32), *two,
            pltpu.SemaphoreType.DMA(()), pltpu.SemaphoreType.DMA((10 + 12 * len(sp.chunks),))],
        compiler_params=pltpu.CompilerParams(collective_id=planes, has_side_effects=True, vmem_limit_bytes=20 * MIB),
        name='scatter',
    )(dq, dk, dv)


def store_body(a, b, c, oa, ob, oc, sem):
    copies = [pltpu.make_async_copy(src, dst, sem.at[i]) for i, (src, dst) in enumerate(((a, oa), (b, ob), (c, oc)))]
    for cp in copies:
        cp.start()
    for cp in copies:
        cp.wait()


def store(*arrays):
    return pl.pallas_call(
        store_body,
        in_specs=[pl.BlockSpec(memory_space=pltpu.VMEM)] * 3,
        out_specs=[pl.BlockSpec(memory_space=pltpu.HBM)] * 3,
        out_shape=[jax.ShapeDtypeStruct(a.shape, a.dtype) for a in arrays],
        scratch_shapes=[pltpu.SemaphoreType.DMA((3,))],
        name='store',
    )(*arrays)


def solution(mesh):
    q_spec = P(None, 'cp', 'tp', None)
    lse_spec = P(None, 'cp', 'tp')
    kv_spec = P('cp', 'tp', None)

    def local_backward(query, out_act, out_grad, row_lse, key_act, value_act, doc_ids):
        n_sub, local_len, n_heads, head_dim = query.shape
        keys_local = key_act.shape[0]
        rows = local_len * n_heads
        q = query.reshape(n_sub, rows, head_dim)
        do = out_grad.reshape(n_sub, rows, head_dim)
        o = out_act.reshape(n_sub, rows, head_dim)
        doc = doc_ids.reshape(-1, LANES)
        k, v = key_act.reshape(keys_local, head_dim), value_act.reshape(keys_local, head_dim)
        rg, sg, kg, vg, lim, bnd, zq, zk, zv = gather(local_len * LANES, q, do, o, row_lse, doc, k, v)
        flat = (16 * keys_local, head_dim)
        dq, dk, dv, which = attend(bnd, kg.reshape(flat), vg.reshape(flat), rg, sg, lim, zq, zk, zv)
        blocks = (4, 4, keys_local, head_dim)
        oq, ok, ov = lax.switch(which[0], [functools.partial(scatter, n) for n in (1, 2, 4)], dq, dk.reshape(blocks), dv.reshape(blocks))
        oq, ok, ov = store(oq, ok, ov)
        return (oq.reshape(query.shape), ok.reshape(keys_local, 1, head_dim), ov.reshape(keys_local, 1, head_dim))

    return jax.shard_map(local_backward, mesh=mesh, in_specs=(q_spec, q_spec, q_spec, lse_spec, kv_spec, kv_spec, P()), out_specs=(q_spec, kv_spec, kv_spec), check_vma=False)
```

```python
import functools

import jax
import jax.numpy as jnp
from jax import lax
from jax.experimental import pallas as pl
from jax.experimental.pallas import tpu as pltpu
from jax.sharding import PartitionSpec as P

MESH = pl.DeviceIdType.MESH
TK = 208
LANES = 128
GROUP = 8
MIB = 2 ** 20
LOG2E = 1.4426950408889634
F32, BF16 = jnp.float32, jnp.bfloat16


def place():
    me = lax.axis_index('cp')
    return me // 32, lax.rem(me // GROUP, 4), lax.rem(me // 2, 4), lax.rem(me, 2)


def at(z, y, x, c):
    return ((z * 4 + y) * 4 + x) * 2 + c


def up(v):
    return lax.rem(v + 1, 4)


def down(v):
    return lax.rem(v + 3, 4)


def far(v):
    return lax.rem(v + 2, 4)


class Wire:
    def __init__(self, ssem, rsem):
        self.ssem, self.rsem, self.n, self.sent, self.groups = ssem, rsem, 0, [], {}

    def copy(self, src, dst, dev, group=None):
        i = self.groups.get(group, self.n)
        if i == self.n:
            self.n += 1
            if group is not None:
                self.groups[group] = i
        return pltpu.make_async_remote_copy(
            src_ref=src, dst_ref=dst, send_sem=self.ssem, recv_sem=self.rsem.at[i], device_id={'cp': dev}, device_id_type=MESH)

    def send(self, src, dst, dev, group=None):
        cp = self.copy(src, dst, dev, group)
        cp.start()
        self.sent.append(cp)
        return cp

    def same(self, ref, dev, group=None):
        return self.send(ref, ref, dev, group)

    def wait_all(self, group, ref):
        pltpu.make_async_copy(ref, ref, self.rsem.at[self.groups[group]]).wait()

    def finish(self):
        for cp in self.sent:
            cp.wait_send()


def greet(partners):
    barrier = pltpu.get_barrier_semaphore()
    for dev in partners:
        pl.semaphore_signal(barrier, inc=1, device_id={'cp': dev}, device_id_type=MESH)
    pl.semaphore_wait(barrier, len(partners))


def row_stats(do, o, lse, st):
    st[...] = jnp.zeros_like(st)
    tok = lax.broadcasted_iota(jnp.int32, (GROUP, LANES), 0)
    lane = lax.broadcasted_iota(jnp.int32, (GROUP, LANES), 1)
    for j in range(do.shape[0]):
        wide = jnp.concatenate([lse[j]] * GROUP, axis=1)
        st[j:j + 1, :] = jnp.sum(jnp.where((lane >> 4) == tok, wide, 0.0), axis=0, keepdims=True) * LOG2E
        prod = do[j].astype(F32) * o[j].astype(F32)
        st[GROUP + j:9 + j, :] = jnp.sum(prod.T, axis=0, keepdims=True)


def limits(doc, n_sub, sub_len, keys_local, lim, bnd):
    z, y, x, c = place()
    grp, lane = z * 4 + y, x * 2 + c
    n_pos = doc.shape[0] * LANES
    sub_start = n_pos - n_sub * sub_len
    period = GROUP * keys_local

    def flat(pos):
        b = jnp.zeros_like(pos)
        for i in range(1, n_pos // period):
            b += jnp.where(pos >= i * period, 1, 0)
        return b * keys_local + jnp.clip(pos - b * period - lane * keys_local, 0, keys_local)

    sub = lax.broadcasted_iota(jnp.int32, (GROUP, LANES), 0)
    tok = lax.broadcasted_iota(jnp.int32, (GROUP, LANES), 1)
    docs = jnp.zeros((GROUP, LANES), jnp.int32)
    for j in range(n_sub):
        row = doc[pl.ds((sub_start + j * sub_len) // LANES + grp // 2, 1), :]
        docs = jnp.where(sub == j, row, docs)
    docs = jnp.where(lax.rem(grp, 2) == 1, pltpu.roll(docs, 64, 1), docs)
    before = jnp.zeros((GROUP, LANES), jnp.int32)
    for j in range(n_sub):
        head = docs[j:j + 1, 0:1]
        count = jnp.zeros((GROUP, LANES), jnp.int32)
        for r in range(0, doc.shape[0], GROUP):
            count += jnp.where(doc[r:r + GROUP, :] < head, 1, 0)
        count = jnp.sum(jnp.sum(count.astype(F32), axis=0, keepdims=True), axis=1, keepdims=True)
        before = jnp.where(sub == j, count.astype(jnp.int32), before)
    base = sub_start + sub * sub_len + grp * 64
    pos = base + tok
    begin = jnp.where((tok > 0) & (docs != pltpu.roll(docs, 1, 1)), pos, before)
    for shift in (1, 2, 4, GROUP, 16, 32):
        begin = jnp.maximum(begin, jnp.where(tok >= shift, pltpu.roll(begin, shift, 1), 0))
    pick = jnp.where(
        lax.broadcasted_iota(jnp.int32, (LANES, 1024), 0) == lax.broadcasted_iota(jnp.int32, (LANES, 1024), 1) >> 4, 1.0, 0.0)
    for first, value in ((0, flat(begin)), (GROUP, flat(pos + 1))):
        wide = jnp.dot(value.astype(F32), pick, precision=lax.Precision.HIGHEST, preferred_element_type=F32)
        for l in range(GROUP):
            lim[l, first:first + GROUP, :] = wide[:, LANES * l:LANES * l + LANES].astype(jnp.int32)
    start = flat(before) & -16
    tiles = jnp.maximum((flat(base + 64) - start + (TK - 1)) // TK, jnp.where(sub == 0, 1, 0))
    first = doc[pl.ds(sub_start // LANES, 1), :][:, 0:1]
    edge = lambda planes: doc[pl.ds((n_pos - planes * n_pos // 4 - 1) // LANES, 1), :][:, 127:LANES] >= first
    which = jnp.where(edge(1), jnp.where(edge(2), 2, 1), 0)
    bnd[...] = jnp.where(tok == 0, start, jnp.where(tok == 1, tiles, which))


def clear(zq, zk, zv):
    def rows(i, _):
        for r in range(4):
            at_ = pl.ds(pl.multiple_of((i * 4 + r) * 16, 16), 16)
            zk[at_, :] = jnp.zeros((16, LANES), F32)
            zv[at_, :] = jnp.zeros((16, LANES), F32)
        return 0

    lax.fori_loop(0, zk.shape[0] // 64, rows, 0)

    def block(i, _):
        zq[i // GROUP, lax.rem(i, GROUP)] = jnp.zeros((LANES, LANES), F32)
        return 0

    lax.fori_loop(0, zq.shape[0] * GROUP, block, 0)


def gather_body(sub_len, q, do, o, lse, doc, k, v, rg, sg, kg, vg, lim, bnd, zq, zk, zv, st, ov, lv, cv, lsem, ssem, rsem):
    z, y, x, c = place()
    xu, xd, sib = at(z, y, up(x), c), at(z, y, down(x), c), at(z, y, x, 1 - c)
    yu, yd = at(z, up(y), x, c), at(z, down(y), x, c)
    zu, zd = at(up(z), y, x, c), at(down(z), y, x, c)
    lane = lambda xx: xx * 2 + c
    own, n_sub, n_own = lane(x), q.shape[0], k.shape[0]
    loads = []
    for i, (src, dst) in enumerate((
            (q, rg.at[0, :, own]), (do, rg.at[1, :, own]), (k, kg.at[z, y]), (v, vg.at[z, y]), (o, ov), (lse, lv), (doc, cv))):
        loads.append(pltpu.make_async_copy(src, dst, lsem.at[max(i // 2, i - 2)]))
        loads[i].start()
    greet([xu, xd, sib, yu, yd, zu, zd])
    w = Wire(ssem, rsem)
    same = w.same
    rows = lambda half, l: rg.at[:, pl.ds(half * (n_sub // 2), n_sub // 2), l]
    k_own, v_own = kg.at[z, y], vg.at[z, y]

    def load(i, ref):
        pltpu.make_async_copy(ref, ref, lsem.at[i]).wait()

    def end(ref, dev, group='keys'):
        same(ref, dev, group)

    load(0, rg.at[:, :, own])
    ru_a, rd_b = same(rows(0, own), xu), same(rows(1, own), xd)
    load(1, kg.at[0, pl.ds(0, 2)])
    k_u, k_d = same(k_own, yu), same(k_own, yd)
    v_u, v_d = same(v_own, zu), same(v_own, zd)
    ru_b, rd_a = same(rows(1, own), xu), same(rows(0, own), xd)
    end(rg.at[:, :, own], sib, 'rows')
    kz, vy = {}, {}
    slot = lambda r, v_: lax.rem(v_ + r, 4)

    def second(kind, r):
        ref = kg.at[z, slot(r, y)] if kind is kz else vg.at[slot(r, z), y]
        for way, dev in (('u', zu if kind is kz else yu), ('d', zd if kind is kz else yd)):
            goes_on = (r < 2) == (way == 'u')
            kind[way, r] = same(ref, dev, None if goes_on else 'keys')

    second(kz, 0)
    second(vy, 0)
    for cp in loads[4:]:
        cp.wait()
    row_stats(rg.at[1, :, own], ov, lv, st)
    sg[own] = st[...]
    limits(cv, n_sub, sub_len, n_own, lim, bnd)
    su, sd = w.send(st, sg.at[own], xu), w.send(st, sg.at[own], xd)
    w.send(st, sg.at[own], sib, 'stats')
    clear(zq, zk, zv)
    low = n_own // 32 * 16 + 16
    lo_rows, hi_rows = pl.ds(0, low), pl.ds(low, n_own - low)
    k_u.wait_recv()
    same(kg.at[z, down(y), lo_rows], yu, 'k')
    k_d.wait_recv()
    same(kg.at[z, up(y), hi_rows], yd, 'k')
    v_u.wait_recv()
    same(vg.at[down(z), y, lo_rows], zu, 'v')
    v_d.wait_recv()
    same(vg.at[up(z), y, hi_rows], zd, 'v')
    for r in (3, 1):
        second(kz, r)
        second(vy, r)
    w.wait_all('k', kg.at[z, far(y)])
    second(kz, 2)
    w.wait_all('v', vg.at[far(z), y])
    second(vy, 2)
    ld, lu, lf = lane(down(x)), lane(up(x)), lane(far(x))
    ru_a.wait_recv()
    fu = same(rows(0, ld), xu)
    rd_b.wait_recv()
    fd = same(rows(1, lu), xd)
    su.wait_recv()
    sf = same(sg.at[ld], xu)
    sd.wait_recv()
    end(rows(0, ld), sib, 'rows')
    end(rows(1, lu), sib, 'rows')
    end(sg.at[ld], sib, 'stats')
    end(sg.at[lu], sib, 'stats')
    for r in (0, 3, 1, 2):
        if r == 2:
            ru_b.wait_recv()
            end(rows(1, ld), sib, 'rows')
            rd_a.wait_recv()
            end(rows(0, lu), sib, 'rows')
        yy, zz = slot(r, y), slot(r, z)
        way, zn, yn, zdev, ydev = ('u', down(z), down(y), zu, yu) if r < 2 else ('d', up(z), up(y), zd, yd)
        kz[way, r].wait_recv()
        end(kg.at[zn, yy], zdev)
        vy[way, r].wait_recv()
        end(vg.at[zz, yn], ydev)
    sf.wait_recv()
    end(sg.at[lf], sib, 'stats')
    fu.wait_recv()
    end(rows(0, lf), sib, 'rows')
    fd.wait_recv()
    end(rows(1, lf), sib, 'rows')
    w.wait_all('rows', rg.at[0])
    w.wait_all('stats', sg.at[pl.ds(0, 4)])
    w.wait_all('keys', kg)
    w.finish()


def gather(sub_len, q, do, o, lse, doc, k, v):
    n_sub = q.shape[0]
    vm = pl.BlockSpec(memory_space=pltpu.VMEM)
    return pl.pallas_call(
        functools.partial(gather_body, sub_len),
        in_specs=[pl.BlockSpec(memory_space=pltpu.HBM)] * 7,
        out_specs=[vm] * 9,
        out_shape=[
            jax.ShapeDtypeStruct((2, n_sub, GROUP, LANES, LANES), BF16),
            jax.ShapeDtypeStruct((GROUP, 16, LANES), F32),
            jax.ShapeDtypeStruct((4, 4) + k.shape, BF16),
            jax.ShapeDtypeStruct((4, 4) + k.shape, BF16),
            jax.ShapeDtypeStruct((GROUP, 16, LANES), jnp.int32),
            jax.ShapeDtypeStruct((GROUP, LANES), jnp.int32),
            jax.ShapeDtypeStruct((n_sub, GROUP, LANES, LANES), F32),
            jax.ShapeDtypeStruct((16 * k.shape[0], LANES), F32),
            jax.ShapeDtypeStruct((16 * k.shape[0], LANES), F32),
        ],
        scratch_shapes=[
            pltpu.VMEM((16, LANES), F32), pltpu.VMEM(o.shape, BF16), pltpu.VMEM(lse.shape, F32), pltpu.VMEM(doc.shape, jnp.int32),
            pltpu.SemaphoreType.DMA((5,)), pltpu.SemaphoreType.DMA(()), pltpu.SemaphoreType.DMA((26,))],
        compiler_params=pltpu.CompilerParams(collective_id=0, has_side_effects=True, vmem_limit_bytes=GROUP * MIB),
        name='gather',
    )(*[pltpu.with_memory_space_constraint(a, pltpu.HBM) for a in (q, do, o, lse, doc, k, v)])


def attend_body(scale, bnd, kg, vg, rg, st, lim, zq, zk, zv, dq, dk, dv, which, p0, d0, p1, d1):
    q, do = rg.at[0], rg.at[1]
    n_keys, n_sub, n_lane = kg.shape[0], rg.shape[1], rg.shape[2]

    which[0] = bnd[0, 2]
    total = bnd[0, 1]
    for j in range(1, n_sub):
        total = total + bnd[j, 1]

    def tile_of(j, i):
        nominal = bnd[j, 0] + i * TK
        return nominal, pl.multiple_of(jnp.minimum(nominal, n_keys - TK), 16)

    def front(j, i, pr, dr):
        nominal, first = tile_of(j, i)
        rows = pl.ds(first, TK)
        kt, vt = kg[rows, :], vg[rows, :]
        index = lax.broadcasted_iota(jnp.int32, (TK, LANES), 0) + first

        def chunk(m):
            qc = q[j, 2 * m:2 * m + 2].reshape(256, LANES)
            dc = do[j, 2 * m:2 * m + 2].reshape(256, LANES)
            s = lax.dot_general(kt, qc, (((1,), (1,)), ((), ())), preferred_element_type=F32)
            dp = lax.dot_general(vt, dc, (((1,), (1,)), ((), ())), preferred_element_type=F32)
            for h in range(2):
                l = 2 * m + h
                cols = slice(LANES * h, LANES * h + LANES)
                lse, delta = st[l, pl.ds(j, 1), :], st[l, pl.ds(j + GROUP, 1), :]
                low, high = lim[l, pl.ds(j, 1), :], lim[l, pl.ds(j + GROUP, 1), :]
                e = jnp.exp2(s[:, cols] * (scale * LOG2E) - lse)
                low = jnp.maximum(low, nominal)
                p = jnp.where((index - low).astype(jnp.uint32) < jnp.maximum(high - low, 0).astype(jnp.uint32), e, 0.0)
                pr[l] = p.astype(BF16)
                dr[l] = (p * (dp[:, cols] - delta)).astype(BF16)

        return [functools.partial(chunk, m) for m in range(n_lane // 2)]

    def back(j, i, pr, dr):
        rows = pl.ds(tile_of(j, i)[1], TK)
        wide = lambda ref, ls: jnp.concatenate([ref[l] for l in ls], axis=1)

        def values():
            dv[rows, :] += jnp.dot(wide(pr, range(n_lane)), do[j].reshape(n_lane * LANES, LANES), preferred_element_type=F32)

        def keys():
            t = lax.dot_general(q[j].reshape(n_lane * LANES, LANES).T, wide(dr, range(n_lane)), (((1,), (1,)), ((), ())), preferred_element_type=F32)
            dk[rows, :] += t.T

        def queries():
            ktt = kg[rows, :].T
            for m in range(n_lane // 2):
                t = jnp.dot(ktt, wide(dr, (2 * m, 2 * m + 1)), preferred_element_type=F32)
                dq[j, 2 * m] += t[:, :LANES]
                dq[j, 2 * m + 1] += t[:, LANES:]

        return [values, keys, queries]

    def do_all(*parts):
        for part in parts:
            part()

    def beyond(j):
        nxt = n_sub - 1
        for jj in reversed(range(n_sub - 1)):
            nxt = jnp.where((jj > j) & (bnd[jj, 1] > 0), jj, nxt)
        return nxt

    def after(j, i):
        turn = i + 1 >= bnd[j, 1]
        return jnp.where(turn, beyond(j), j), jnp.where(turn, 0, i + 1)

    def step(now, have, want):
        nxt = after(*now)
        b, f = back(*now, *have), front(*nxt, *want)
        do_all(b[0], f[0], f[1], b[1], f[2], f[3], b[2])
        return nxt

    def two(_, now):
        return step(step(now, (p0, d0), (p1, d1)), (p1, d1), (p0, d0))

    def four(_, now):
        return two(0, two(0, now))

    def one(_, now):
        nxt = after(*now)
        do_all(*back(*now, p0, d0), *front(*nxt, p0, d0))
        return nxt

    first = (beyond(jnp.int32(-1)), jnp.int32(0))
    do_all(*front(*first, p0, d0))
    more = total - 1
    now = lax.fori_loop(0, more // 4, four, first)
    now = lax.fori_loop(0, lax.rem(more, 4) // 2, two, now)
    now = lax.fori_loop(0, lax.rem(more, 2), one, now)
    do_all(*back(*now, p0, d0))


def attend(bnd, kg, vg, rg, st, lim, zq, zk, zv):
    n_lane = rg.shape[2]
    vm = pl.BlockSpec(memory_space=pltpu.VMEM)
    return pl.pallas_call(
        functools.partial(attend_body, LANES ** -0.5),
        in_specs=[pl.BlockSpec(memory_space=pltpu.SMEM)] + [vm] * GROUP,
        out_specs=[vm] * 3 + [pl.BlockSpec(memory_space=pltpu.SMEM)],
        out_shape=[jax.ShapeDtypeStruct(rg.shape[1:], F32), jax.ShapeDtypeStruct(kg.shape, F32),
                   jax.ShapeDtypeStruct(kg.shape, F32), jax.ShapeDtypeStruct((1,), jnp.int32)],
        input_output_aliases={6: 0, 7: 1, GROUP: 2},
        scratch_shapes=[pltpu.VMEM((n_lane, TK, LANES), BF16)] * 4,
        compiler_params=pltpu.CompilerParams(vmem_limit_bytes=16 * MIB),
        name='attend',
    )(bnd, kg, vg, rg, st, lim, zq, zk, zv)


class Split:
    def __init__(self, planes, keys):
        self.planes, self.keys, self.parts = planes, keys, 4 // planes
        self.rows = -(-keys // self.parts // 16) * 16 if planes == 1 else keys // self.parts
        self.last = keys - self.rows
        cut = -(-self.rows // 16) * GROUP
        self.chunks = [(0, self.rows)] if planes == 1 else [(0, cut), (cut, self.rows - cut)]
        self.half = (2 * self.rows, LANES) if planes == 1 else (2, self.rows, LANES)

    def slot(self, z):
        if self.planes == 4:
            return z, 0
        if self.planes == 2:
            return jnp.where(lax.rem(z, 3) == 0, 3, 2), jnp.where(z < 2, self.rows, 0)
        return 3, jnp.minimum(lax.rem(z + 1, 4) * self.rows, self.last)

    def rows_at(self, first, chunk):
        return pl.ds(pl.multiple_of(first + chunk[0], GROUP), chunk[1])

    def keys_of(self, dk, z, ys, chunk):
        owner, first = self.slot(z)
        return dk.at[owner, ys, self.rows_at(first, chunk)]

    def cut(self, ref, chunk):
        return ref if self.planes == 1 else ref.at[:, pl.ds(*chunk)]

    def values_of(self, dv, y, h, chunk):
        if self.planes == 4:
            return dv.at[pl.ds(2 * h, 2), y, pl.ds(*chunk)]
        if self.planes == 2:
            return dv.at[2 + h, y, :, pl.ds(*chunk)]
        return dv.at[3, y, pl.ds(h * (self.keys - 2 * self.rows), 2 * self.rows)]

    def value_slot(self, vs, z, chunk):
        owner, first = self.slot(z)
        if self.planes == 4:
            return vs.at[z // 2, lax.rem(z, 2), pl.ds(*chunk)]
        if self.planes == 2:
            return vs.at[owner - 2, jnp.where(z < 2, 1, 0), pl.ds(*chunk)]
        h = jnp.where(first >= 2 * self.rows, 1, 0)
        return vs.at[h, self.rows_at(first - h * (self.keys - 2 * self.rows), chunk)]

    def shares(self):
        if self.planes == 4:
            return []
        if self.planes == 2:
            return [(3, 1, 0), (2, 1, 1)]
        return [(3, h, (3 + h) % 4) for h in (1, 2, 3)]


class Ring:
    def __init__(self, w, place_, dev_up, dev_down, block, via, got, both):
        self.w, self.p, self.up, self.dn = w, place_, dev_up, dev_down
        self.block, self.via, self.got, self.both = block, via, got, both

    def first_up(self):
        self.fu = self.w.send(self.block(far(self.p), 0), self.via(0), self.up)

    def first_down(self):
        self.fd = self.w.send(self.block(far(self.p), 1), self.via(1), self.dn)

    def direct_up(self):
        self.du = self.w.send(self.block(up(self.p), 1), self.got(0, 1), self.up, self)

    def direct_down(self):
        self.dd = self.w.send(self.block(down(self.p), 0), self.got(1, 0), self.dn, self)

    def start(self):
        self.first_up()
        self.first_down()
        self.direct_up()
        self.direct_down()

    def middle(self):
        w, p = self.w, self.p
        self.fu.wait_recv()
        add(self.via(0), self.block(up(p), 0))
        self.mu = w.send(self.via(0), self.got(0, 0), self.up, self)
        self.fd.wait_recv()
        add(self.via(1), self.block(down(p), 1))
        self.md = w.send(self.via(1), self.got(1, 1), self.dn, self)

    def wait(self):
        self.w.wait_all(self, self.both)


def add(dst, src):
    dst[...] = dst[...] + src[...]


def scatter_body(scale, sp, dq, dk, dv, oq, ok, ov, sq, sv, sg, k1v, k1g, ks, k2v, k2g, kr, v1v, v1g, vs, v2v, v2g, vr, ssem, rsem):
    z, y, x, c = place()
    xu, xd, sib = at(z, y, up(x), c), at(z, y, down(x), c), at(z, y, x, 1 - c)
    yu, yd = at(z, up(y), x, c), at(z, down(y), x, c)
    zu, zd = at(up(z), y, x, c), at(down(z), y, x, c)
    greet([xu, xd, sib, yu, yd, zu, zd] + ([at(far(z), y, x, c)] if sp.planes == 1 else []))
    w = Wire(ssem, rsem)
    n_sub = dq.shape[0]
    hn = n_sub // 2
    halves = (range(hn), range(hn, n_sub))
    order = ((far(x), halves[0]), (far(x), halves[1]), (up(x), range(n_sub)), (down(x), range(n_sub)), (x, range(n_sub)))
    cross = [w.send(dq.at[pl.ds(js[0], len(js)), xx * 2 + 1 - c], sq.at[xx, pl.ds(js[0], len(js))], sib) for xx, js in order]
    hy = (pl.ds(0, 2), pl.ds(2, 2))

    class Chunk:
        def __init__(self, chunk):
            low = -(-chunk[1] // 16) * GROUP
            hr = ((chunk[0], low), (chunk[0] + low, chunk[1] - low))
            part = lambda ref: ref.at[pl.ds(*chunk)]
            self.kone = Ring(w, z, zu, zd, lambda b, h: sp.keys_of(dk, b, hy[h], chunk),
                             lambda h: k1v.at[h, :, pl.ds(*chunk)], lambda s, h: k1g.at[s, hy[h], pl.ds(*chunk)],
                             k1g.at[:, :, pl.ds(*chunk)])
            self.vone = Ring(w, y, yu, yd, lambda b, h: sp.values_of(dv, b, h, chunk),
                             lambda h: sp.cut(v1v.at[h], chunk), lambda s, h: sp.cut(v1g.at[s, h], chunk),
                             v1g if sp.planes == 1 else v1g.at[:, :, :, pl.ds(*chunk)])
            self.ktwo = Ring(w, y, yu, yd, lambda b, h: ks.at[b, pl.ds(*hr[h])],
                             lambda h: k2v.at[h, pl.ds(*hr[h])], lambda s, h: k2g.at[s, pl.ds(*hr[h])],
                             k2g.at[:, pl.ds(*chunk)])
            self.vtwo = Ring(w, z, zu, zd, lambda b, h: sp.value_slot(vs, b, hr[h]),
                             lambda h: v2v.at[h, pl.ds(*hr[h])], lambda s, h: v2g.at[s, pl.ds(*hr[h])],
                             v2g.at[:, pl.ds(*chunk)])
            self.chunk, self.part = chunk, part

        def turn(self):
            self.kone.wait()
            for b in range(4):
                self.part(ks.at[b])[...] = (sp.keys_of(dk, z, b, self.chunk)[...] + self.part(k1g.at[0, b])[...]
                                            + self.part(k1g.at[1, b])[...])
            self.ktwo.start()
            self.vone.wait()
            for h in range(2):
                sp.cut(vs.at[h], self.chunk)[...] = (sp.values_of(dv, y, h, self.chunk)[...] + sp.cut(v1g.at[0, h], self.chunk)[...]
                                                     + sp.cut(v1g.at[1, h], self.chunk)[...])
            self.vtwo.start()

        def end(self):
            self.ktwo.wait()
            self.part(kr.at[0])[...] = (self.part(ks.at[y])[...] + self.part(k2g.at[0])[...] + self.part(k2g.at[1])[...]) * scale
            self.go_home(kr, ok)
            self.vtwo.wait()
            self.part(vr.at[0])[...] = sp.value_slot(vs, z, self.chunk)[...] + self.part(v2g.at[0])[...] + self.part(v2g.at[1])[...]
            self.go_home(vr, ov)

        def go_home(self, buf, out):
            for owner, h, taker in sp.shares():
                cp = w.copy(self.part(buf.at[0]), self.part(buf.at[h]), at(owner, y, x, c), ('home', buf is kr))
                home.append((owner, h, taker, buf, out, self.chunk, cp))
                pl.when(z == taker)(cp.start)

    home = []
    chunks = [Chunk(chunk) for chunk in sp.chunks]
    for ch in chunks:
        ch.kone.start()
        ch.vone.start()
    hj = (pl.ds(0, hn), pl.ds(hn, n_sub - hn))
    qring = Ring(w, x, xu, xd, lambda b, h: sq.at[b, hj[h]], lambda h: sv.at[h], lambda s, h: sg.at[s, hj[h]], sg)
    steps = (qring.first_up, qring.first_down, qring.direct_up, qring.direct_down, None)
    for cp, (xx, js), then in zip(cross, order, steps):
        cp.wait_recv()
        for j in js:
            sq[xx, j] = sq[xx, j] + dq[j, xx * 2 + c]
        if then is not None:
            then()
    for ch in chunks:
        ch.kone.middle()
        ch.vone.middle()
    qring.middle()
    for ch in chunks:
        ch.turn()
    for ch in chunks:
        ch.ktwo.middle()
        ch.vtwo.middle()
    for ch in chunks:
        ch.end()
    qring.wait()
    for j in range(n_sub):
        oq[j] = ((sq[x, j] + sg[0, j] + sg[1, j]).T * scale).astype(BF16)
    if sp.planes == 4:
        ok[...] = kr[0]
        ov[...] = vr[0]
    else:
        @pl.when(z < 4 - sp.planes)
        def _():
            ok[...] = jnp.zeros_like(ok)
            ov[...] = jnp.zeros_like(ov)

        @pl.when(z >= 4 - sp.planes)
        def _():
            ok[0:sp.rows, :] = kr[0]
            ov[0:sp.rows, :] = vr[0]

        for buf in (kr, vr):
            pl.when(z >= 4 - sp.planes)(functools.partial(w.wait_all, ('home', buf is kr), buf.at[pl.ds(1, sp.parts - 1)]))
        for _, _, taker, _, _, _, cp in home:
            pl.when(z == taker)(cp.wait_send)
        for owner, h, taker, buf, out, chunk, cp in home:
            first = min(h * sp.rows, sp.last) + chunk[0]

            @pl.when(z == owner)
            def _():
                out[first:first + chunk[1], :] = buf[h, chunk[0]:chunk[0] + chunk[1], :]

    w.finish()


def scatter(planes, dq, dk, dv):
    n_sub = dq.shape[0]
    sp = Split(planes, dk.shape[2])
    if planes == 2:
        dv = dv.reshape(4, 4, 2, sp.rows, LANES)
    rows = sp.rows
    vm = pl.BlockSpec(memory_space=pltpu.VMEM)
    two = [
        pltpu.VMEM((2, rows, LANES), F32),
        pltpu.VMEM((2, rows, LANES), F32),
        pltpu.VMEM((sp.parts, rows, LANES), F32),
    ]
    return pl.pallas_call(
        functools.partial(scatter_body, LANES ** -0.5, sp),
        in_specs=[vm] * 3,
        out_specs=[vm] * 3,
        out_shape=[
            jax.ShapeDtypeStruct((n_sub, LANES, LANES), BF16),
            jax.ShapeDtypeStruct((sp.keys, LANES), F32),
            jax.ShapeDtypeStruct((sp.keys, LANES), F32),
        ],
        scratch_shapes=[
            pltpu.VMEM((4, n_sub, LANES, LANES), F32),
            pltpu.VMEM((2, n_sub // 2, LANES, LANES), F32),
            pltpu.VMEM((2, n_sub, LANES, LANES), F32),
            pltpu.VMEM((2, 2, rows, LANES), F32), pltpu.VMEM((2, 4, rows, LANES), F32), pltpu.VMEM((4, rows, LANES), F32), *two,
            pltpu.VMEM((2,) + sp.half, F32), pltpu.VMEM((2, 2) + sp.half, F32), pltpu.VMEM((2,) + sp.half, F32), *two,
            pltpu.SemaphoreType.DMA(()), pltpu.SemaphoreType.DMA((10 + 12 * len(sp.chunks),))],
        compiler_params=pltpu.CompilerParams(collective_id=planes, has_side_effects=True, vmem_limit_bytes=20 * MIB),
        name='scatter',
    )(dq, dk, dv)


def store_body(a, b, c, oa, ob, oc, sem):
    copies = [pltpu.make_async_copy(src, dst, sem.at[i]) for i, (src, dst) in enumerate(((a, oa), (b, ob), (c, oc)))]
    for cp in copies:
        cp.start()
    for cp in copies:
        cp.wait()


def store(*arrays):
    return pl.pallas_call(
        store_body,
        in_specs=[pl.BlockSpec(memory_space=pltpu.VMEM)] * 3,
        out_specs=[pl.BlockSpec(memory_space=pltpu.HBM)] * 3,
        out_shape=[jax.ShapeDtypeStruct(a.shape, a.dtype) for a in arrays],
        scratch_shapes=[pltpu.SemaphoreType.DMA((3,))],
        name='store',
    )(*arrays)


def solution(mesh):
    q_spec = P(None, 'cp', 'tp', None)
    lse_spec = P(None, 'cp', 'tp')
    kv_spec = P('cp', 'tp', None)

    def local_backward(query, out_act, out_grad, row_lse, key_act, value_act, doc_ids):
        n_sub, local_len, n_heads, head_dim = query.shape
        keys_local = key_act.shape[0]
        rows = local_len * n_heads
        q = query.reshape(n_sub, rows, head_dim)
        do = out_grad.reshape(n_sub, rows, head_dim)
        o = out_act.reshape(n_sub, rows, head_dim)
        doc = doc_ids.reshape(-1, LANES)
        k, v = key_act.reshape(keys_local, head_dim), value_act.reshape(keys_local, head_dim)
        rg, sg, kg, vg, lim, bnd, zq, zk, zv = gather(local_len * LANES, q, do, o, row_lse, doc, k, v)
        flat = (16 * keys_local, head_dim)
        dq, dk, dv, which = attend(bnd, kg.reshape(flat), vg.reshape(flat), rg, sg, lim, zq, zk, zv)
        blocks = (4, 4, keys_local, head_dim)
        oq, ok, ov = lax.switch(which[0], [functools.partial(scatter, n) for n in (1, 2, 4)], dq, dk.reshape(blocks), dv.reshape(blocks))
        oq, ok, ov = store(oq, ok, ov)
        return (oq.reshape(query.shape), ok.reshape(keys_local, 1, head_dim), ov.reshape(keys_local, 1, head_dim))

    return jax.shard_map(local_backward, mesh=mesh, in_specs=(q_spec, q_spec, q_spec, lse_spec, kv_spec, kv_spec, P()), out_specs=(q_spec, kv_spec, kv_spec), check_vma=False)
```

```python
import functools

import jax
import jax.numpy as jnp
from jax import lax
from jax.experimental import pallas as pl
from jax.experimental.pallas import tpu as pltpu
from jax.sharding import PartitionSpec as P

MESH = pl.DeviceIdType.MESH
TK = 224
LANES = 128
GROUP = 8
MIB = 2 ** 20
LOG2E = 1.4426950408889634
F32, BF16 = jnp.float32, jnp.bfloat16


def place():
    me = lax.axis_index('cp')
    return me // 32, lax.rem(me // GROUP, 4), lax.rem(me // 2, 4), lax.rem(me, 2)


def at(z, y, x, c):
    return ((z * 4 + y) * 4 + x) * 2 + c


def up(v):
    return lax.rem(v + 1, 4)


def down(v):
    return lax.rem(v + 3, 4)


def far(v):
    return lax.rem(v + 2, 4)


class Wire:
    def __init__(self, ssem, rsem):
        self.ssem, self.rsem, self.n, self.sent, self.groups = ssem, rsem, 0, [], {}

    def copy(self, src, dst, dev, group=None):
        i = self.groups.get(group, self.n)
        if i == self.n:
            self.n += 1
            if group is not None:
                self.groups[group] = i
        return pltpu.make_async_remote_copy(
            src_ref=src, dst_ref=dst, send_sem=self.ssem, recv_sem=self.rsem.at[i], device_id={'cp': dev}, device_id_type=MESH)

    def send(self, src, dst, dev, group=None):
        cp = self.copy(src, dst, dev, group)
        cp.start()
        self.sent.append(cp)
        return cp

    def same(self, ref, dev, group=None):
        return self.send(ref, ref, dev, group)

    def wait_all(self, group, ref):
        pltpu.make_async_copy(ref, ref, self.rsem.at[self.groups[group]]).wait()

    def finish(self):
        for cp in self.sent:
            cp.wait_send()


def greet(partners):
    barrier = pltpu.get_barrier_semaphore()
    for dev in partners:
        pl.semaphore_signal(barrier, inc=1, device_id={'cp': dev}, device_id_type=MESH)
    pl.semaphore_wait(barrier, len(partners))


def row_stats(do, o, lse, st):
    st[...] = jnp.zeros_like(st)
    tok = lax.broadcasted_iota(jnp.int32, (GROUP, LANES), 0)
    lane = lax.broadcasted_iota(jnp.int32, (GROUP, LANES), 1)
    for j in range(do.shape[0]):
        wide = jnp.concatenate([lse[j]] * GROUP, axis=1)
        st[j:j + 1, :] = jnp.sum(jnp.where((lane >> 4) == tok, wide, 0.0), axis=0, keepdims=True) * LOG2E
        prod = do[j].astype(F32) * o[j].astype(F32)
        st[GROUP + j:9 + j, :] = jnp.sum(prod.T, axis=0, keepdims=True)


def limits(doc, n_sub, sub_len, keys_local, lim, bnd):
    z, y, x, c = place()
    grp, lane = z * 4 + y, x * 2 + c
    n_pos = doc.shape[0] * LANES
    sub_start = n_pos - n_sub * sub_len
    period = GROUP * keys_local

    def flat(pos):
        b = jnp.zeros_like(pos)
        for i in range(1, n_pos // period):
            b += jnp.where(pos >= i * period, 1, 0)
        return b * keys_local + jnp.clip(pos - b * period - lane * keys_local, 0, keys_local)

    sub = lax.broadcasted_iota(jnp.int32, (GROUP, LANES), 0)
    tok = lax.broadcasted_iota(jnp.int32, (GROUP, LANES), 1)
    docs = jnp.zeros((GROUP, LANES), jnp.int32)
    for j in range(n_sub):
        row = doc[pl.ds((sub_start + j * sub_len) // LANES + grp // 2, 1), :]
        docs = jnp.where(sub == j, row, docs)
    docs = jnp.where(lax.rem(grp, 2) == 1, pltpu.roll(docs, 64, 1), docs)
    before = jnp.zeros((GROUP, LANES), jnp.int32)
    for j in range(n_sub):
        head = docs[j:j + 1, 0:1]
        count = jnp.zeros((GROUP, LANES), jnp.int32)
        for r in range(0, doc.shape[0], GROUP):
            count += jnp.where(doc[r:r + GROUP, :] < head, 1, 0)
        count = jnp.sum(jnp.sum(count.astype(F32), axis=0, keepdims=True), axis=1, keepdims=True)
        before = jnp.where(sub == j, count.astype(jnp.int32), before)
    base = sub_start + sub * sub_len + grp * 64
    pos = base + tok
    begin = jnp.where((tok > 0) & (docs != pltpu.roll(docs, 1, 1)), pos, before)
    for shift in (1, 2, 4, GROUP, 16, 32):
        begin = jnp.maximum(begin, jnp.where(tok >= shift, pltpu.roll(begin, shift, 1), 0))
    pick = jnp.where(
        lax.broadcasted_iota(jnp.int32, (LANES, 1024), 0) == lax.broadcasted_iota(jnp.int32, (LANES, 1024), 1) >> 4, 1.0, 0.0)
    for first, value in ((0, flat(begin)), (GROUP, flat(pos + 1))):
        wide = jnp.dot(value.astype(F32), pick, precision=lax.Precision.HIGHEST, preferred_element_type=F32)
        for l in range(GROUP):
            lim[l, first:first + GROUP, :] = wide[:, LANES * l:LANES * l + LANES].astype(jnp.int32)
    start = flat(before) & -16
    tiles = jnp.maximum((flat(base + 64) - start + (TK - 1)) // TK, jnp.where(sub == 0, 1, 0))
    first = doc[pl.ds(sub_start // LANES, 1), :][:, 0:1]
    edge = lambda planes: doc[pl.ds((n_pos - planes * n_pos // 4 - 1) // LANES, 1), :][:, 127:LANES] >= first
    which = jnp.where(edge(1), jnp.where(edge(2), 2, 1), 0)
    bnd[...] = jnp.where(tok == 0, start, jnp.where(tok == 1, tiles, which))


def clear(zq, zk, zv):
    def rows(i, _):
        for r in range(4):
            at_ = pl.ds(pl.multiple_of((i * 4 + r) * 16, 16), 16)
            zk[at_, :] = jnp.zeros((16, LANES), F32)
            zv[at_, :] = jnp.zeros((16, LANES), F32)
        return 0

    lax.fori_loop(0, zk.shape[0] // 64, rows, 0)

    def block(i, _):
        zq[i // GROUP, lax.rem(i, GROUP)] = jnp.zeros((LANES, LANES), F32)
        return 0

    lax.fori_loop(0, zq.shape[0] * GROUP, block, 0)


def gather_body(sub_len, q, do, o, lse, doc, k, v, rg, sg, kg, vg, lim, bnd, zq, zk, zv, st, ov, lv, cv, lsem, ssem, rsem):
    z, y, x, c = place()
    xu, xd, sib = at(z, y, up(x), c), at(z, y, down(x), c), at(z, y, x, 1 - c)
    yu, yd = at(z, up(y), x, c), at(z, down(y), x, c)
    zu, zd = at(up(z), y, x, c), at(down(z), y, x, c)
    lane = lambda xx: xx * 2 + c
    own, n_sub, n_own = lane(x), q.shape[0], k.shape[0]
    loads = []
    for i, (src, dst) in enumerate((
            (q, rg.at[0, :, own]), (do, rg.at[1, :, own]), (k, kg.at[z, y]), (v, vg.at[z, y]), (o, ov), (lse, lv), (doc, cv))):
        loads.append(pltpu.make_async_copy(src, dst, lsem.at[max(i // 2, i - 2)]))
        loads[i].start()
    greet([xu, xd, sib, yu, yd, zu, zd])
    w = Wire(ssem, rsem)
    same = w.same
    rows = lambda half, l: rg.at[:, pl.ds(half * (n_sub // 2), n_sub // 2), l]
    k_own, v_own = kg.at[z, y], vg.at[z, y]

    def load(i, ref):
        pltpu.make_async_copy(ref, ref, lsem.at[i]).wait()

    def end(ref, dev, group='keys'):
        same(ref, dev, group)

    load(0, rg.at[:, :, own])
    ru_a, rd_b = same(rows(0, own), xu), same(rows(1, own), xd)
    load(1, kg.at[0, pl.ds(0, 2)])
    k_u, k_d = same(k_own, yu), same(k_own, yd)
    v_u, v_d = same(v_own, zu), same(v_own, zd)
    ru_b, rd_a = same(rows(1, own), xu), same(rows(0, own), xd)
    end(rg.at[:, :, own], sib, 'rows')
    kz, vy = {}, {}
    slot = lambda r, v_: lax.rem(v_ + r, 4)

    def second(kind, r):
        ref = kg.at[z, slot(r, y)] if kind is kz else vg.at[slot(r, z), y]
        for way, dev in (('u', zu if kind is kz else yu), ('d', zd if kind is kz else yd)):
            goes_on = (r < 2) == (way == 'u')
            kind[way, r] = same(ref, dev, None if goes_on else 'keys')

    second(kz, 0)
    second(vy, 0)
    for cp in loads[4:]:
        cp.wait()
    row_stats(rg.at[1, :, own], ov, lv, st)
    sg[own] = st[...]
    limits(cv, n_sub, sub_len, n_own, lim, bnd)
    su, sd = w.send(st, sg.at[own], xu), w.send(st, sg.at[own], xd)
    w.send(st, sg.at[own], sib, 'stats')
    clear(zq, zk, zv)
    low = n_own // 32 * 16 + 16
    lo_rows, hi_rows = pl.ds(0, low), pl.ds(low, n_own - low)
    k_u.wait_recv()
    same(kg.at[z, down(y), lo_rows], yu, 'k')
    k_d.wait_recv()
    same(kg.at[z, up(y), hi_rows], yd, 'k')
    v_u.wait_recv()
    same(vg.at[down(z), y, lo_rows], zu, 'v')
    v_d.wait_recv()
    same(vg.at[up(z), y, hi_rows], zd, 'v')
    for r in (3, 1):
        second(kz, r)
        second(vy, r)
    w.wait_all('k', kg.at[z, far(y)])
    second(kz, 2)
    w.wait_all('v', vg.at[far(z), y])
    second(vy, 2)
    ld, lu, lf = lane(down(x)), lane(up(x)), lane(far(x))
    ru_a.wait_recv()
    fu = same(rows(0, ld), xu)
    rd_b.wait_recv()
    fd = same(rows(1, lu), xd)
    su.wait_recv()
    sf = same(sg.at[ld], xu)
    sd.wait_recv()
    end(rows(0, ld), sib, 'rows')
    end(rows(1, lu), sib, 'rows')
    end(sg.at[ld], sib, 'stats')
    end(sg.at[lu], sib, 'stats')
    for r in (0, 3, 1, 2):
        if r == 2:
            ru_b.wait_recv()
            end(rows(1, ld), sib, 'rows')
            rd_a.wait_recv()
            end(rows(0, lu), sib, 'rows')
        yy, zz = slot(r, y), slot(r, z)
        way, zn, yn, zdev, ydev = ('u', down(z), down(y), zu, yu) if r < 2 else ('d', up(z), up(y), zd, yd)
        kz[way, r].wait_recv()
        end(kg.at[zn, yy], zdev)
        vy[way, r].wait_recv()
        end(vg.at[zz, yn], ydev)
    sf.wait_recv()
    end(sg.at[lf], sib, 'stats')
    fu.wait_recv()
    end(rows(0, lf), sib, 'rows')
    fd.wait_recv()
    end(rows(1, lf), sib, 'rows')
    w.wait_all('rows', rg.at[0])
    w.wait_all('stats', sg.at[pl.ds(0, 4)])
    w.wait_all('keys', kg)
    w.finish()


def gather(sub_len, q, do, o, lse, doc, k, v):
    n_sub = q.shape[0]
    vm = pl.BlockSpec(memory_space=pltpu.VMEM)
    return pl.pallas_call(
        functools.partial(gather_body, sub_len),
        in_specs=[pl.BlockSpec(memory_space=pltpu.HBM)] * 7,
        out_specs=[vm] * 9,
        out_shape=[
            jax.ShapeDtypeStruct((2, n_sub, GROUP, LANES, LANES), BF16),
            jax.ShapeDtypeStruct((GROUP, 16, LANES), F32),
            jax.ShapeDtypeStruct((4, 4) + k.shape, BF16),
            jax.ShapeDtypeStruct((4, 4) + k.shape, BF16),
            jax.ShapeDtypeStruct((GROUP, 16, LANES), jnp.int32),
            jax.ShapeDtypeStruct((GROUP, LANES), jnp.int32),
            jax.ShapeDtypeStruct((n_sub, GROUP, LANES, LANES), F32),
            jax.ShapeDtypeStruct((16 * k.shape[0], LANES), F32),
            jax.ShapeDtypeStruct((16 * k.shape[0], LANES), F32),
        ],
        scratch_shapes=[
            pltpu.VMEM((16, LANES), F32), pltpu.VMEM(o.shape, BF16), pltpu.VMEM(lse.shape, F32), pltpu.VMEM(doc.shape, jnp.int32),
            pltpu.SemaphoreType.DMA((5,)), pltpu.SemaphoreType.DMA(()), pltpu.SemaphoreType.DMA((26,))],
        compiler_params=pltpu.CompilerParams(collective_id=0, has_side_effects=True, vmem_limit_bytes=GROUP * MIB),
        name='gather',
    )(*[pltpu.with_memory_space_constraint(a, pltpu.HBM) for a in (q, do, o, lse, doc, k, v)])


def attend_body(scale, bnd, kg, vg, rg, st, lim, zq, zk, zv, dq, dk, dv, which, p0, d0, p1, d1):
    q, do = rg.at[0], rg.at[1]
    n_keys, n_sub, n_lane = kg.shape[0], rg.shape[1], rg.shape[2]

    which[0] = bnd[0, 2]
    total = bnd[0, 1]
    for j in range(1, n_sub):
        total = total + bnd[j, 1]

    def tile_of(j, i):
        nominal = bnd[j, 0] + i * TK
        return nominal, pl.multiple_of(jnp.minimum(nominal, n_keys - TK), 16)

    def front(j, i, pr, dr):
        nominal, first = tile_of(j, i)
        rows = pl.ds(first, TK)
        kt, vt = kg[rows, :], vg[rows, :]
        index = lax.broadcasted_iota(jnp.int32, (TK, LANES), 0) + first

        def chunk(m):
            qc = q[j, 2 * m:2 * m + 2].reshape(256, LANES)
            dc = do[j, 2 * m:2 * m + 2].reshape(256, LANES)
            s = lax.dot_general(kt, qc, (((1,), (1,)), ((), ())), preferred_element_type=F32)
            dp = lax.dot_general(vt, dc, (((1,), (1,)), ((), ())), preferred_element_type=F32)
            for h in range(2):
                l = 2 * m + h
                cols = slice(LANES * h, LANES * h + LANES)
                lse, delta = st[l, pl.ds(j, 1), :], st[l, pl.ds(j + GROUP, 1), :]
                low, high = lim[l, pl.ds(j, 1), :], lim[l, pl.ds(j + GROUP, 1), :]
                e = jnp.exp2(s[:, cols] * (scale * LOG2E) - lse)
                low = jnp.maximum(low, nominal)
                p = jnp.where((index - low).astype(jnp.uint32) < jnp.maximum(high - low, 0).astype(jnp.uint32), e, 0.0)
                pr[l] = p.astype(BF16)
                dr[l] = (p * (dp[:, cols] - delta)).astype(BF16)

        return [functools.partial(chunk, m) for m in range(n_lane // 2)]

    def back(j, i, pr, dr):
        rows = pl.ds(tile_of(j, i)[1], TK)
        wide = lambda ref, ls: jnp.concatenate([ref[l] for l in ls], axis=1)

        def values():
            dv[rows, :] += jnp.dot(wide(pr, range(n_lane)), do[j].reshape(n_lane * LANES, LANES), preferred_element_type=F32)

        def keys():
            t = lax.dot_general(q[j].reshape(n_lane * LANES, LANES).T, wide(dr, range(n_lane)), (((1,), (1,)), ((), ())), preferred_element_type=F32)
            dk[rows, :] += t.T

        def queries():
            ktt = kg[rows, :].T
            for m in range(n_lane // 2):
                t = jnp.dot(ktt, wide(dr, (2 * m, 2 * m + 1)), preferred_element_type=F32)
                dq[j, 2 * m] += t[:, :LANES]
                dq[j, 2 * m + 1] += t[:, LANES:]

        return [values, keys, queries]

    def do_all(*parts):
        for part in parts:
            part()

    def beyond(j):
        nxt = n_sub - 1
        for jj in reversed(range(n_sub - 1)):
            nxt = jnp.where((jj > j) & (bnd[jj, 1] > 0), jj, nxt)
        return nxt

    def after(j, i):
        turn = i + 1 >= bnd[j, 1]
        return jnp.where(turn, beyond(j), j), jnp.where(turn, 0, i + 1)

    def step(now, have, want):
        nxt = after(*now)
        b, f = back(*now, *have), front(*nxt, *want)
        do_all(b[0], f[0], f[1], b[1], f[2], f[3], b[2])
        return nxt

    def two(_, now):
        return step(step(now, (p0, d0), (p1, d1)), (p1, d1), (p0, d0))

    def four(_, now):
        return two(0, two(0, now))

    def one(_, now):
        nxt = after(*now)
        do_all(*back(*now, p0, d0), *front(*nxt, p0, d0))
        return nxt

    first = (beyond(jnp.int32(-1)), jnp.int32(0))
    do_all(*front(*first, p0, d0))
    more = total - 1
    now = lax.fori_loop(0, more // 4, four, first)
    now = lax.fori_loop(0, lax.rem(more, 4) // 2, two, now)
    now = lax.fori_loop(0, lax.rem(more, 2), one, now)
    do_all(*back(*now, p0, d0))


def attend(bnd, kg, vg, rg, st, lim, zq, zk, zv):
    n_lane = rg.shape[2]
    vm = pl.BlockSpec(memory_space=pltpu.VMEM)
    return pl.pallas_call(
        functools.partial(attend_body, LANES ** -0.5),
        in_specs=[pl.BlockSpec(memory_space=pltpu.SMEM)] + [vm] * GROUP,
        out_specs=[vm] * 3 + [pl.BlockSpec(memory_space=pltpu.SMEM)],
        out_shape=[jax.ShapeDtypeStruct(rg.shape[1:], F32), jax.ShapeDtypeStruct(kg.shape, F32),
                   jax.ShapeDtypeStruct(kg.shape, F32), jax.ShapeDtypeStruct((1,), jnp.int32)],
        input_output_aliases={6: 0, 7: 1, GROUP: 2},
        scratch_shapes=[pltpu.VMEM((n_lane, TK, LANES), BF16)] * 4,
        compiler_params=pltpu.CompilerParams(vmem_limit_bytes=16 * MIB),
        name='attend',
    )(bnd, kg, vg, rg, st, lim, zq, zk, zv)


class Split:
    def __init__(self, planes, keys):
        self.planes, self.keys, self.parts = planes, keys, 4 // planes
        self.rows = -(-keys // self.parts // 16) * 16 if planes == 1 else keys // self.parts
        self.last = keys - self.rows
        cut = -(-self.rows // 16) * GROUP
        self.chunks = [(0, self.rows)] if planes == 1 else [(0, cut), (cut, self.rows - cut)]
        self.half = (2 * self.rows, LANES) if planes == 1 else (2, self.rows, LANES)

    def slot(self, z):
        if self.planes == 4:
            return z, 0
        if self.planes == 2:
            return jnp.where(lax.rem(z, 3) == 0, 3, 2), jnp.where(z < 2, self.rows, 0)
        return 3, jnp.minimum(lax.rem(z + 1, 4) * self.rows, self.last)

    def rows_at(self, first, chunk):
        return pl.ds(pl.multiple_of(first + chunk[0], GROUP), chunk[1])

    def keys_of(self, dk, z, ys, chunk):
        owner, first = self.slot(z)
        return dk.at[owner, ys, self.rows_at(first, chunk)]

    def cut(self, ref, chunk):
        return ref if self.planes == 1 else ref.at[:, pl.ds(*chunk)]

    def values_of(self, dv, y, h, chunk):
        if self.planes == 4:
            return dv.at[pl.ds(2 * h, 2), y, pl.ds(*chunk)]
        if self.planes == 2:
            return dv.at[2 + h, y, :, pl.ds(*chunk)]
        return dv.at[3, y, pl.ds(h * (self.keys - 2 * self.rows), 2 * self.rows)]

    def value_slot(self, vs, z, chunk):
        owner, first = self.slot(z)
        if self.planes == 4:
            return vs.at[z // 2, lax.rem(z, 2), pl.ds(*chunk)]
        if self.planes == 2:
            return vs.at[owner - 2, jnp.where(z < 2, 1, 0), pl.ds(*chunk)]
        h = jnp.where(first >= 2 * self.rows, 1, 0)
        return vs.at[h, self.rows_at(first - h * (self.keys - 2 * self.rows), chunk)]

    def shares(self):
        if self.planes == 4:
            return []
        if self.planes == 2:
            return [(3, 1, 0), (2, 1, 1)]
        return [(3, h, (3 + h) % 4) for h in (1, 2, 3)]


class Ring:
    def __init__(self, w, place_, dev_up, dev_down, block, via, got, both):
        self.w, self.p, self.up, self.dn = w, place_, dev_up, dev_down
        self.block, self.via, self.got, self.both = block, via, got, both

    def first_up(self):
        self.fu = self.w.send(self.block(far(self.p), 0), self.via(0), self.up)

    def first_down(self):
        self.fd = self.w.send(self.block(far(self.p), 1), self.via(1), self.dn)

    def direct_up(self):
        self.du = self.w.send(self.block(up(self.p), 1), self.got(0, 1), self.up, self)

    def direct_down(self):
        self.dd = self.w.send(self.block(down(self.p), 0), self.got(1, 0), self.dn, self)

    def start(self):
        self.first_up()
        self.first_down()
        self.direct_up()
        self.direct_down()

    def middle(self):
        w, p = self.w, self.p
        self.fu.wait_recv()
        add(self.via(0), self.block(up(p), 0))
        self.mu = w.send(self.via(0), self.got(0, 0), self.up, self)
        self.fd.wait_recv()
        add(self.via(1), self.block(down(p), 1))
        self.md = w.send(self.via(1), self.got(1, 1), self.dn, self)

    def wait(self):
        self.w.wait_all(self, self.both)


def add(dst, src):
    dst[...] = dst[...] + src[...]


def scatter_body(scale, sp, dq, dk, dv, oq, ok, ov, sq, sv, sg, k1v, k1g, ks, k2v, k2g, kr, v1v, v1g, vs, v2v, v2g, vr, ssem, rsem):
    z, y, x, c = place()
    xu, xd, sib = at(z, y, up(x), c), at(z, y, down(x), c), at(z, y, x, 1 - c)
    yu, yd = at(z, up(y), x, c), at(z, down(y), x, c)
    zu, zd = at(up(z), y, x, c), at(down(z), y, x, c)
    greet([xu, xd, sib, yu, yd, zu, zd] + ([at(far(z), y, x, c)] if sp.planes == 1 else []))
    w = Wire(ssem, rsem)
    n_sub = dq.shape[0]
    hn = n_sub // 2
    halves = (range(hn), range(hn, n_sub))
    order = ((far(x), halves[0]), (far(x), halves[1]), (up(x), range(n_sub)), (down(x), range(n_sub)), (x, range(n_sub)))
    cross = [w.send(dq.at[pl.ds(js[0], len(js)), xx * 2 + 1 - c], sq.at[xx, pl.ds(js[0], len(js))], sib) for xx, js in order]
    hy = (pl.ds(0, 2), pl.ds(2, 2))

    class Chunk:
        def __init__(self, chunk):
            low = -(-chunk[1] // 16) * GROUP
            hr = ((chunk[0], low), (chunk[0] + low, chunk[1] - low))
            part = lambda ref: ref.at[pl.ds(*chunk)]
            self.kone = Ring(w, z, zu, zd, lambda b, h: sp.keys_of(dk, b, hy[h], chunk),
                             lambda h: k1v.at[h, :, pl.ds(*chunk)], lambda s, h: k1g.at[s, hy[h], pl.ds(*chunk)],
                             k1g.at[:, :, pl.ds(*chunk)])
            self.vone = Ring(w, y, yu, yd, lambda b, h: sp.values_of(dv, b, h, chunk),
                             lambda h: sp.cut(v1v.at[h], chunk), lambda s, h: sp.cut(v1g.at[s, h], chunk),
                             v1g if sp.planes == 1 else v1g.at[:, :, :, pl.ds(*chunk)])
            self.ktwo = Ring(w, y, yu, yd, lambda b, h: ks.at[b, pl.ds(*hr[h])],
                             lambda h: k2v.at[h, pl.ds(*hr[h])], lambda s, h: k2g.at[s, pl.ds(*hr[h])],
                             k2g.at[:, pl.ds(*chunk)])
            self.vtwo = Ring(w, z, zu, zd, lambda b, h: sp.value_slot(vs, b, hr[h]),
                             lambda h: v2v.at[h, pl.ds(*hr[h])], lambda s, h: v2g.at[s, pl.ds(*hr[h])],
                             v2g.at[:, pl.ds(*chunk)])
            self.chunk, self.part = chunk, part

        def turn(self):
            self.kone.wait()
            for b in range(4):
                self.part(ks.at[b])[...] = (sp.keys_of(dk, z, b, self.chunk)[...] + self.part(k1g.at[0, b])[...]
                                            + self.part(k1g.at[1, b])[...])
            self.ktwo.start()
            self.vone.wait()
            for h in range(2):
                sp.cut(vs.at[h], self.chunk)[...] = (sp.values_of(dv, y, h, self.chunk)[...] + sp.cut(v1g.at[0, h], self.chunk)[...]
                                                     + sp.cut(v1g.at[1, h], self.chunk)[...])
            self.vtwo.start()

        def end(self):
            self.ktwo.wait()
            self.part(kr.at[0])[...] = (self.part(ks.at[y])[...] + self.part(k2g.at[0])[...] + self.part(k2g.at[1])[...]) * scale
            self.go_home(kr, ok)
            self.vtwo.wait()
            self.part(vr.at[0])[...] = sp.value_slot(vs, z, self.chunk)[...] + self.part(v2g.at[0])[...] + self.part(v2g.at[1])[...]
            self.go_home(vr, ov)

        def go_home(self, buf, out):
            for owner, h, taker in sp.shares():
                cp = w.copy(self.part(buf.at[0]), self.part(buf.at[h]), at(owner, y, x, c), ('home', buf is kr))
                home.append((owner, h, taker, buf, out, self.chunk, cp))
                pl.when(z == taker)(cp.start)

    home = []
    chunks = [Chunk(chunk) for chunk in sp.chunks]
    for ch in chunks:
        ch.kone.start()
        ch.vone.start()
    hj = (pl.ds(0, hn), pl.ds(hn, n_sub - hn))
    qring = Ring(w, x, xu, xd, lambda b, h: sq.at[b, hj[h]], lambda h: sv.at[h], lambda s, h: sg.at[s, hj[h]], sg)
    steps = (qring.first_up, qring.first_down, qring.direct_up, qring.direct_down, None)
    for cp, (xx, js), then in zip(cross, order, steps):
        cp.wait_recv()
        for j in js:
            sq[xx, j] = sq[xx, j] + dq[j, xx * 2 + c]
        if then is not None:
            then()
    for ch in chunks:
        ch.kone.middle()
        ch.vone.middle()
    qring.middle()
    for ch in chunks:
        ch.turn()
    for ch in chunks:
        ch.ktwo.middle()
        ch.vtwo.middle()
    for ch in chunks:
        ch.end()
    qring.wait()
    for j in range(n_sub):
        oq[j] = ((sq[x, j] + sg[0, j] + sg[1, j]).T * scale).astype(BF16)
    if sp.planes == 4:
        ok[...] = kr[0]
        ov[...] = vr[0]
    else:
        @pl.when(z < 4 - sp.planes)
        def _():
            ok[...] = jnp.zeros_like(ok)
            ov[...] = jnp.zeros_like(ov)

        @pl.when(z >= 4 - sp.planes)
        def _():
            ok[0:sp.rows, :] = kr[0]
            ov[0:sp.rows, :] = vr[0]

        for buf in (kr, vr):
            pl.when(z >= 4 - sp.planes)(functools.partial(w.wait_all, ('home', buf is kr), buf.at[pl.ds(1, sp.parts - 1)]))
        for _, _, taker, _, _, _, cp in home:
            pl.when(z == taker)(cp.wait_send)
        for owner, h, taker, buf, out, chunk, cp in home:
            first = min(h * sp.rows, sp.last) + chunk[0]

            @pl.when(z == owner)
            def _():
                out[first:first + chunk[1], :] = buf[h, chunk[0]:chunk[0] + chunk[1], :]

    w.finish()


def scatter(planes, dq, dk, dv):
    n_sub = dq.shape[0]
    sp = Split(planes, dk.shape[2])
    if planes == 2:
        dv = dv.reshape(4, 4, 2, sp.rows, LANES)
    rows = sp.rows
    vm = pl.BlockSpec(memory_space=pltpu.VMEM)
    two = [
        pltpu.VMEM((2, rows, LANES), F32),
        pltpu.VMEM((2, rows, LANES), F32),
        pltpu.VMEM((sp.parts, rows, LANES), F32),
    ]
    return pl.pallas_call(
        functools.partial(scatter_body, LANES ** -0.5, sp),
        in_specs=[vm] * 3,
        out_specs=[vm] * 3,
        out_shape=[
            jax.ShapeDtypeStruct((n_sub, LANES, LANES), BF16),
            jax.ShapeDtypeStruct((sp.keys, LANES), F32),
            jax.ShapeDtypeStruct((sp.keys, LANES), F32),
        ],
        scratch_shapes=[
            pltpu.VMEM((4, n_sub, LANES, LANES), F32),
            pltpu.VMEM((2, n_sub // 2, LANES, LANES), F32),
            pltpu.VMEM((2, n_sub, LANES, LANES), F32),
            pltpu.VMEM((2, 2, rows, LANES), F32), pltpu.VMEM((2, 4, rows, LANES), F32), pltpu.VMEM((4, rows, LANES), F32), *two,
            pltpu.VMEM((2,) + sp.half, F32), pltpu.VMEM((2, 2) + sp.half, F32), pltpu.VMEM((2,) + sp.half, F32), *two,
            pltpu.SemaphoreType.DMA(()), pltpu.SemaphoreType.DMA((10 + 12 * len(sp.chunks),))],
        compiler_params=pltpu.CompilerParams(collective_id=planes, has_side_effects=True, vmem_limit_bytes=20 * MIB),
        name='scatter',
    )(dq, dk, dv)


def store_body(a, b, c, oa, ob, oc, sem):
    copies = [pltpu.make_async_copy(src, dst, sem.at[i]) for i, (src, dst) in enumerate(((a, oa), (b, ob), (c, oc)))]
    for cp in copies:
        cp.start()
    for cp in copies:
        cp.wait()


def store(*arrays):
    return pl.pallas_call(
        store_body,
        in_specs=[pl.BlockSpec(memory_space=pltpu.VMEM)] * 3,
        out_specs=[pl.BlockSpec(memory_space=pltpu.HBM)] * 3,
        out_shape=[jax.ShapeDtypeStruct(a.shape, a.dtype) for a in arrays],
        scratch_shapes=[pltpu.SemaphoreType.DMA((3,))],
        name='store',
    )(*arrays)


def solution(mesh):
    q_spec = P(None, 'cp', 'tp', None)
    lse_spec = P(None, 'cp', 'tp')
    kv_spec = P('cp', 'tp', None)

    def local_backward(query, out_act, out_grad, row_lse, key_act, value_act, doc_ids):
        n_sub, local_len, n_heads, head_dim = query.shape
        keys_local = key_act.shape[0]
        rows = local_len * n_heads
        q = query.reshape(n_sub, rows, head_dim)
        do = out_grad.reshape(n_sub, rows, head_dim)
        o = out_act.reshape(n_sub, rows, head_dim)
        doc = doc_ids.reshape(-1, LANES)
        k, v = key_act.reshape(keys_local, head_dim), value_act.reshape(keys_local, head_dim)
        rg, sg, kg, vg, lim, bnd, zq, zk, zv = gather(local_len * LANES, q, do, o, row_lse, doc, k, v)
        flat = (16 * keys_local, head_dim)
        dq, dk, dv, which = attend(bnd, kg.reshape(flat), vg.reshape(flat), rg, sg, lim, zq, zk, zv)
        blocks = (4, 4, keys_local, head_dim)
        oq, ok, ov = lax.switch(which[0], [functools.partial(scatter, n) for n in (1, 2, 4)], dq, dk.reshape(blocks), dv.reshape(blocks))
        oq, ok, ov = store(oq, ok, ov)
        return (oq.reshape(query.shape), ok.reshape(keys_local, 1, head_dim), ov.reshape(keys_local, 1, head_dim))

    return jax.shard_map(local_backward, mesh=mesh, in_specs=(q_spec, q_spec, q_spec, lse_spec, kv_spec, kv_spec, P()), out_specs=(q_spec, kv_spec, kv_spec), check_vma=False)
```
